32 devices in a mesh: space: 8 (over y, x, core), tm: 4 (over z).
Axes of the slice: x: 2, y: 2, z: 4, core: 2. Of those that a mesh axis runs over, the one named last changes fastest.
Arguments:
- links: float32 [4, 3, 2, 3, 3, 16, 4096], P('tm', None, None, None, None, 'space'), may hold values from -1 to 1, as said below
- propagator: float32 [2, 144, 16, 4096], P(None, 'tm', 'space'), may hold values from -6 to 6
- sink_time: int32 [1], replicated, may hold values from 0 to 16383
- src_time: int32 [1], replicated, may hold values from 0 to 16383
- src_site: int32 [1], replicated, may hold values from 0 to 65535
Outputs:
- fixed_links: float32 [4, 3, 2, 3, 3, 16, 4096], P('tm', None, None, None, None, 'space')
- wall: float32 [2, 144], replicated
The draws below stay inside these ranges and needn't reach their ends.
Inputs may be any that keep to these rules, and one draw needn't show every extreme that they name: `links`: every link is a special unitary 3 x 3 matrix up to rounding.
All inputs are finite; a program needn't handle non-finite values.
Results may differ from the reference program's by a relative error of at most 0.0001.
Values sent between devices are 32-bit elements; how exact they have to be, the bound alone decides.
No kernel may reach another device: no remote copies, remote signals or barrier semaphores. Data moves between devices by JAX's collectives and lax.ppermute only.
A program may use at most 128 MiB of HBM per device.

```python
import math
import jax
import jax.numpy as jnp
from jax import lax

L = 64
SC = 12
ITERS = 2
NX = 16
NT = 4


def draw_product(left_matrix, right_matrix):
    pattern = 'tdikxn,tdkjxn->tdijxn'
    real_part = jnp.einsum(pattern, left_matrix[:, :, 0], right_matrix[:, :, 0]) - jnp.einsum(pattern, left_matrix[:, :, 1], right_matrix[:, :, 1])
    imag_part = jnp.einsum(pattern, left_matrix[:, :, 0], right_matrix[:, :, 1]) + jnp.einsum(pattern, left_matrix[:, :, 1], right_matrix[:, :, 0])
    return jnp.stack([real_part, imag_part], axis=2)


def draw_links(key, part):
    normal_draw = jax.random.normal(key, (NT, 3, 2, 3, 3, NX, L * L), jnp.float32)
    real_part = normal_draw[:, :, 0]
    imag_part = normal_draw[:, :, 1]
    real_anti = 0.5 * (real_part - jnp.swapaxes(real_part, 2, 3))
    imag_sym = 0.5 * (imag_part + jnp.swapaxes(imag_part, 2, 3))
    trace_third = (imag_sym[:, :, 0, 0] + imag_sym[:, :, 1, 1] + imag_sym[:, :, 2, 2]) / 3.0
    unit_matrix = jnp.eye(3, dtype=jnp.float32)[None, None, :, :, None, None]
    imag_sym = imag_sym - unit_matrix * trace_third[:, :, None, None]
    algebra = jnp.stack([real_anti, imag_sym], axis=2) / 16.0
    identity = jnp.stack([jnp.broadcast_to(unit_matrix, real_anti.shape), jnp.zeros(real_anti.shape, jnp.float32)], axis=2)
    result = identity
    for degree in range(8, 0, -1):
        result = identity + draw_product(algebra, result) / degree
    for square_index in range(4):
        result = draw_product(result, result)
    return result


def level_of(rng, extent, shards, least, largest):
    def one(axis_at, shards_of):
        heights = jax.random.uniform(jax.random.fold_in(jax.random.fold_in(rng, 6), axis_at), (shards_of,), jnp.float32, least / len(shards), largest / len(shards))
        return jnp.repeat(jnp.exp(heights), extent[axis_at] // shards_of).reshape((-1,) + (1,) * (len(extent) - axis_at - 1))

    level = one(*shards[0])
    for cut in shards[1:]:
        level = level * one(*cut)
    return level


def noise(key, shape, scale, reach, cuts=(), kind=jnp.bfloat16):
    entries = scale * jax.random.normal(key, shape, jnp.float32)
    if cuts:
        entries = entries * level_of(key, shape, cuts, -0.22, 0.18)
    return jnp.clip(entries, -reach, reach).astype(kind)


def setup_inputs(seed: int = 0) -> dict:
    arg_keys = jax.random.split(jax.random.key(seed), 6)
    links = draw_links(jax.random.fold_in(arg_keys[5], 71), 0)
    propagator = noise(arg_keys[1], (2, SC * SC, NX, L * L), 1.0, 6.0, ((1, 4), (2, 8)), jnp.float32)
    sink_time = jax.random.randint(arg_keys[2], (1,), 0, NT * 4096).astype(jnp.int32)
    src_time = jax.random.randint(arg_keys[3], (1,), 0, NT * 4096).astype(jnp.int32)
    src_site = jax.random.randint(arg_keys[4], (1,), 0, NX * L * L).astype(jnp.int32)
    return dict(links=links, propagator=propagator, sink_time=sink_time, src_time=src_time, src_site=src_site)


STEP_SIZE = 0.08
PEAK_SQUARE = 12.0
ENTRY_PAIRS = ((0, 0), (0, 1), (0, 2), (1, 1), (1, 2), (2, 2))
EXACT = lax.Precision.HIGHEST


def colour_product(left_matrix, right_matrix):
    return jnp.sum(left_matrix[:, :, None] * right_matrix[None, :, :], axis=1)


def complex_product(left_matrix, right_matrix):
    real_part = colour_product(left_matrix[0], right_matrix[0]) - colour_product(left_matrix[1], right_matrix[1])
    imag_part = colour_product(left_matrix[0], right_matrix[1]) + colour_product(left_matrix[1], right_matrix[0])
    return jnp.stack([real_part, imag_part])


def dagger(matrix):
    return jnp.stack([jnp.swapaxes(matrix[0], 0, 1), -jnp.swapaxes(matrix[1], 0, 1)])


def roll_depth(values, amount):
    old_shape = values.shape
    folded = values.reshape(old_shape[:-1] + (L, L))
    return jnp.roll(folded, amount, axis=-1).reshape(old_shape)


def project(divergence):
    real_part = 0.5 * (divergence[0] - jnp.swapaxes(divergence[0], 0, 1))
    imag_part = 0.5 * (divergence[1] + jnp.swapaxes(divergence[1], 0, 1))
    trace_third = (imag_part[0, 0] + imag_part[1, 1] + imag_part[2, 2]) / 3.0
    real_six = jnp.stack([real_part[row_index, column_index] for row_index, column_index in ENTRY_PAIRS])
    imag_six = jnp.stack([imag_part[row_index, column_index] - trace_third if row_index == column_index else imag_part[row_index, column_index] for row_index, column_index in ENTRY_PAIRS])
    return real_six, imag_six


def assemble(real_six, imag_six):
    zero_plane = jnp.zeros_like(real_six[0])
    position = {}
    for entry_index, entry_pair in enumerate(ENTRY_PAIRS):
        position[entry_pair] = entry_index
    real_rows = []
    imag_rows = []
    for row_index in range(3):
        real_line = []
        imag_line = []
        for column_index in range(3):
            if row_index == column_index:
                real_line.append(zero_plane)
                imag_line.append(imag_six[position[(row_index, row_index)]])
            elif row_index < column_index:
                slot_index = position[(row_index, column_index)]
                real_line.append(real_six[slot_index])
                imag_line.append(imag_six[slot_index])
            else:
                slot_index = position[(column_index, row_index)]
                real_line.append(-real_six[slot_index])
                imag_line.append(imag_six[slot_index])
        real_rows.append(jnp.stack(real_line))
        imag_rows.append(jnp.stack(imag_line))
    return jnp.stack([jnp.stack(real_rows), jnp.stack(imag_rows)])


def exponential(algebra):
    unit_matrix = jnp.eye(3, dtype=jnp.float32).reshape((3, 3) + (1,) * (algebra.ndim - 3))
    identity = jnp.stack([jnp.broadcast_to(unit_matrix, algebra.shape[1:]), jnp.zeros(algebra.shape[1:], jnp.float32)])
    result = identity
    for degree in range(6, 0, -1):
        result = identity + complex_product(algebra, result) / degree
    for square_index in range(3):
        result = complex_product(result, result)
    return result


def rotate(lattice, gauge_field, gauge_ahead):
    along_x = complex_product(complex_product(gauge_field, lattice[0]), dagger(gauge_ahead))
    along_y = complex_product(complex_product(gauge_field, lattice[1]), dagger(jnp.roll(gauge_field, -L, axis=4)))
    along_z = complex_product(complex_product(gauge_field, lattice[2]), dagger(roll_depth(gauge_field, -1)))
    return jnp.stack([along_x, along_y, along_z])


def sink_product(gauge_field, propagator):
    pair_count = propagator.shape[1]
    source = propagator.reshape((2, pair_count // 3, 3) + propagator.shape[2:])
    pattern = "acxn,qcxn->qa"
    real_part = jnp.einsum(pattern, gauge_field[0], source[0], precision=EXACT) - jnp.einsum(pattern, gauge_field[1], source[1], precision=EXACT)
    imag_part = jnp.einsum(pattern, gauge_field[0], source[1], precision=EXACT) + jnp.einsum(pattern, gauge_field[1], source[0], precision=EXACT)
    return jnp.stack([real_part.reshape(pair_count), imag_part.reshape(pair_count)])


def source_rotate(wall_total, anchor):
    by_spin = wall_total.reshape(2, 4, 3, SC)
    pattern = "scn,bc->sbn"
    real_part = jnp.einsum(pattern, by_spin[0], anchor[0], precision=EXACT) + jnp.einsum(pattern, by_spin[1], anchor[1], precision=EXACT)
    imag_part = jnp.einsum(pattern, by_spin[1], anchor[0], precision=EXACT) - jnp.einsum(pattern, by_spin[0], anchor[1], precision=EXACT)
    return jnp.stack([real_part.reshape(SC * SC), imag_part.reshape(SC * SC)])


def sine_squares(length):
    wavenumber = jnp.arange(length, dtype=jnp.float32)
    return 4.0 * jnp.sin(math.pi * wavenumber / length) ** 2


def inverse_square():
    across = sine_squares(NX)
    sine_square = sine_squares(L)
    momentum = across[:, None, None] + sine_square[None, :, None] + sine_square[None, None, :]
    guarded = jnp.where(momentum > 0.0, momentum, 1.0)
    return jnp.where(momentum > 0.0, PEAK_SQUARE / guarded, 0.0)


def reference(links, propagator, sink_time, src_time, src_site):
    filter_weight = inverse_square()

    def fix_timeslice(lattice):
        overall = None
        for sweep_index in range(ITERS):
            divergence = jnp.roll(lattice[0], 1, axis=3) - lattice[0] + jnp.roll(lattice[1], L, axis=4) - lattice[1] + roll_depth(lattice[2], 1) - lattice[2]
            real_six, imag_six = project(divergence)
            packed = (real_six + 1j * imag_six).reshape(6, NX, L, L)
            spectrum = jnp.fft.fftn(packed, axes=(1, 2, 3)) * filter_weight[None]
            filtered = jnp.fft.ifftn(spectrum, axes=(1, 2, 3)).reshape(6, NX, L * L)
            algebra = assemble(jnp.real(filtered), jnp.imag(filtered))
            gauge_field = exponential(algebra * (STEP_SIZE / 16.0))
            lattice = rotate(lattice, gauge_field, jnp.roll(gauge_field, -1, axis=3))
            overall = gauge_field if overall is None else complex_product(gauge_field, overall)
        return lattice, overall

    fixed_links, overall_all = lax.map(fix_timeslice, links)
    sink_slice = sink_time[0] % NT
    source_slice = src_time[0] % NT
    wall_total = sink_product(overall_all[sink_slice], propagator)
    site_index = src_site[0]
    anchor = overall_all[source_slice][:, :, :, site_index // (L * L), site_index % (L * L)]
    wall = source_rotate(wall_total, anchor) * float(NX * L * L) ** -0.5
    return fixed_links, wall
```

```python
import functools
import math

import jax
import jax.numpy as jnp
import numpy as np
from jax import lax
from jax.experimental import pallas as pl
from jax.experimental.pallas import tpu as pltpu
from jax.sharding import PartitionSpec as P

SC = 12
STEP_SIZE = 0.08
PEAK_SQUARE = 12.0
F32 = jnp.float32
BF16 = jnp.bfloat16
VMEM = pltpu.VMEM
PAIRS = ((0, 1), (0, 2), (1, 2))


def split_table(table):
    high = table.astype(jnp.bfloat16)
    low = (table - high.astype(np.float64)).astype(jnp.bfloat16)
    return high, low


def as_real(real, imag):
    return np.block([[real, imag], [-imag, real]])


@functools.lru_cache(None)
def transform_tables(side, inverse):
    half = side // 2
    sign = 1.0 if inverse else -1.0
    k = np.arange(half)
    row_phase = sign * 2.0 * np.pi * np.outer(k, k) / half
    rows_left = as_real(np.cos(row_phase), -np.sin(row_phase))
    high, low = split_table(rows_left)
    left = np.concatenate([high, low, high], axis=1)
    z = np.arange(side)
    depth_phase = sign * 2.0 * np.pi * np.outer(z, z) / side
    parity = np.array([[1.0, 1.0], [1.0, -1.0]])
    right = as_real(np.kron(parity, np.cos(depth_phase)), np.kron(parity, np.sin(depth_phase)))
    high, low = split_table(right)
    right = np.stack([high, low])
    twiddle_phase = sign * 2.0 * np.pi * k / side
    lanes = np.arange(2 * side) >= side
    phase = np.where(lanes[None, :], twiddle_phase[:, None], 0.0)
    twiddle = np.stack([np.cos(phase), np.sin(phase)]).astype(np.float32)
    return left, right, twiddle


@functools.lru_cache(None)
def filter_table(side, across, blocks):
    half = side // 2
    squares = 4.0 * np.sin(np.pi * np.arange(side) / side) ** 2
    squares_across = 4.0 * np.sin(np.pi * np.arange(across) / across) ** 2
    column = (squares[:, None] + squares[None, :]).reshape(2, half, side)
    column = np.swapaxes(column, 0, 1).reshape(half, 2 * side)
    momentum = squares_across[:, None, None] + column[None]
    weight = np.where(momentum > 0.0, PEAK_SQUARE / np.where(momentum > 0.0, momentum, 1.0), 0.0)
    offsets = np.arange(across // 2 + 1)
    phase = np.cos(2.0 * np.pi * np.outer(offsets, np.arange(across)) / across)
    table = np.einsum("dk,krl->drl", phase, weight) / (across * side * side)
    table = table * (STEP_SIZE / 16.0)
    table = table.reshape(len(offsets), blocks, half // blocks, 2 * side)
    return np.ascontiguousarray(np.swapaxes(table, 0, 1)).astype(np.float32)


def cmul(x, y):
    return x[0] * y[0] - x[1] * y[1], x[0] * y[1] + x[1] * y[0]


def csquare(x):
    return x[0] * x[0] - x[1] * x[1], 2.0 * (x[0] * x[1])


def row_times(row, matrix):
    out = []
    for b in range(3):
        re = row[0][0] * matrix[0][b][0] - row[0][1] * matrix[0][b][1]
        im = row[0][0] * matrix[0][b][1] + row[0][1] * matrix[0][b][0]
        for k in (1, 2):
            re = re + row[k][0] * matrix[k][b][0] - row[k][1] * matrix[k][b][1]
            im = im + row[k][0] * matrix[k][b][1] + row[k][1] * matrix[k][b][0]
        out.append((re, im))
    return out


def row_times_dagger(row, matrix):
    out = []
    for b in range(3):
        re = row[0][0] * matrix[b][0][0] + row[0][1] * matrix[b][0][1]
        im = row[0][1] * matrix[b][0][0] - row[0][0] * matrix[b][0][1]
        for k in (1, 2):
            re = re + row[k][0] * matrix[b][k][0] + row[k][1] * matrix[b][k][1]
            im = im + row[k][1] * matrix[b][k][0] - row[k][0] * matrix[b][k][1]
        out.append((re, im))
    return out


def exponential(x):
    t0, t1 = x[0], x[1]
    a, b, e = (x[2], x[3]), (x[4], x[5]), (x[6], x[7])
    t2 = -(t0 + t1)
    na = a[0] * a[0] + a[1] * a[1]
    nb = b[0] * b[0] + b[1] * b[1]
    ne = e[0] * e[0] + e[1] * e[1]
    s0, s1, s2 = t0 * t0, t1 * t1, t2 * t2
    ae = cmul(a, e)
    c = -(0.5 * (s0 + s1 + s2) + (na + nb + ne))
    cross = ae[1] * b[0] - ae[0] * b[1]
    d = t0 * ne + t1 * nb + t2 * na - t0 * t1 * t2 - 2.0 * cross
    c30 = c * (1.0 / 30.0)
    q0 = (None, d * (1.0 / 120.0))
    q1 = ((1.0 + c30) * 0.25, None)
    q2r = 1.0 / 20.0
    n0i = d * (q2r / 3.0)
    n1 = ((1.0 + c * q2r) * (1.0 / 3.0), q0[1] * (1.0 / 3.0))
    n2r = q1[0] * (1.0 / 3.0)
    m0 = (None, d * (0.5 * n2r))
    m1 = (0.5 + 0.5 * (c * n2r), 0.5 * n0i)
    m2 = (0.5 * n1[0], 0.5 * n1[1])
    q0 = (1.0 - d * m2[1], d * m2[0])
    q1 = (1.0 + c * m2[0], m0[1] + c * m2[1])
    q2 = m1
    for _ in range(3):
        q12 = cmul(q1, q2)
        q22 = csquare(q2)
        q00 = csquare(q0)
        q11 = csquare(q1)
        q01 = cmul(q0, q1)
        q02 = cmul(q0, q2)
        d2 = 2.0 * d
        q0 = (q00[0] - d2 * q12[1], q00[1] + d2 * q12[0])
        q1 = (
            2.0 * (q01[0] + c * q12[0]) - d * q22[1],
            2.0 * (q01[1] + c * q12[1]) + d * q22[0],
        )
        q2 = (q11[0] + 2.0 * q02[0] + c * q22[0], q11[1] + 2.0 * q02[1] + c * q22[1])
    u, v = q1
    s, t = q2
    result = [[None] * 3 for _ in range(3)]
    for at, (theta, m) in enumerate(
        ((t0, -(s0 + na + nb)), (t1, -(s1 + na + ne)), (t2, -(s2 + nb + ne)))
    ):
        result[at][at] = (q0[0] - v * theta + s * m, q0[1] + u * theta + t * m)
    y01 = (t2 * a[1] - (b[0] * e[0] + b[1] * e[1]), -t2 * a[0] - (b[1] * e[0] - b[0] * e[1]))
    y02 = (t1 * b[1] + ae[0], -t1 * b[0] + ae[1])
    y12 = (t0 * e[1] - (a[0] * b[0] + a[1] * b[1]), -t0 * e[0] - (a[0] * b[1] - a[1] * b[0]))
    for (i, j), xx, yy in zip(PAIRS, (a, b, e), (y01, y02, y12)):
        ur, vi, ui, vr = u * xx[0], v * xx[1], u * xx[1], v * xx[0]
        sr, ti, si, tr = s * yy[0], t * yy[1], s * yy[1], t * yy[0]
        result[i][j] = ((ur - vi) + (sr - ti), (ui + vr) + (si + tr))
        result[j][i] = ((sr + ti) - (ur + vi), (tr - si) + (ui - vr))
    return result


def project(rows):
    third = (rows[0][0][1] + rows[1][1][1] + rows[2][2][1]) * (1.0 / 3.0)
    out = [rows[0][0][1] - third, rows[1][1][1] - third]
    for i, j in PAIRS:
        out.append(0.5 * (rows[i][j][0] - rows[j][i][0]))
        out.append(0.5 * (rows[i][j][1] + rows[j][i][1]))
    return out


def lane_of(shape):
    return lax.broadcasted_iota(jnp.int32, shape, 1)


def ahead_y(v):
    half = v.shape[1] // 2
    r = pltpu.roll(v, half, axis=1)
    return jnp.where(lane_of(v.shape) < half, r, pltpu.roll(r, v.shape[0] - 1, axis=0))


def behind_y(v):
    half = v.shape[1] // 2
    r = pltpu.roll(v, half, axis=1)
    return jnp.where(lane_of(v.shape) >= half, r, pltpu.roll(r, 1, axis=0))


def ahead_z(v):
    lanes = v.shape[1]
    half = lanes // 2
    inner = pltpu.roll(v, lanes - 1, axis=1)
    edge = pltpu.roll(v, half - 1, axis=1)
    return jnp.where(lane_of(v.shape) % half == half - 1, edge, inner)


def behind_z(v):
    lanes = v.shape[1]
    half = lanes // 2
    inner = pltpu.roll(v, 1, axis=1)
    edge = pltpu.roll(v, half + 1, axis=1)
    return jnp.where(lane_of(v.shape) % half == 0, edge, inner)


def halves(x):
    high = x.astype(BF16)
    low = (x - high.astype(F32)).astype(BF16)
    return high, low


def dot(x, y):
    return jnp.dot(x, y, preferred_element_type=F32)


def left_transform(stacked, left_ref):
    high, low = halves(stacked)
    return dot(left_ref[...], jnp.concatenate([high, high, low], axis=0))


def right_transform(high_ref, low_ref, right_ref, out_ref):
    high = high_ref[...]
    out_ref[...] = (
        dot(high, right_ref[0]) + dot(low_ref[...], right_ref[0]) + dot(high, right_ref[1])
    )


def forward_transform(d_ref, left_ref, right_ref, twiddle_ref, high_ref, low_ref, spec_ref, out_ref):
    slots, _, half, lanes = d_ref.shape
    parts = out_ref.shape[0] // 4
    rows = half // parts
    tr, ti = twiddle_ref[0], twiddle_ref[1]
    for slot in range(slots):
        stacked = jnp.concatenate(
            [
                jnp.concatenate([d_ref[slot, 2 * f], d_ref[slot, 2 * f + 1]], axis=0)
                for f in range(4)
            ],
            axis=1,
        )
        y = left_transform(stacked, left_ref)
        for f in range(4):
            re = y[:half, f * lanes : (f + 1) * lanes]
            im = y[half:, f * lanes : (f + 1) * lanes]
            both = jnp.concatenate([re * tr - im * ti, re * ti + im * tr], axis=1)
            high, low = halves(both)
            at = (slot * 4 + f) * half
            high_ref[at : at + half, :] = high
            low_ref[at : at + half, :] = low
    right_transform(high_ref, low_ref, right_ref, spec_ref)
    for slot in range(slots):
        for f in range(4):
            for part in range(parts):
                at = (slot * 4 + f) * half + part * rows
                for c in range(2):
                    to = (slot * 2 + c) * rows
                    out_ref[f * parts + part, to : to + rows, :] = spec_ref[
                        at : at + rows, c * lanes : (c + 1) * lanes
                    ]


def inverse_transform(in_ref, left_ref, right_ref, twiddle_ref, high_ref, low_ref, spec_ref, x_ref):
    _, slots, half, lanes = x_ref.shape
    parts = in_ref.shape[0] // 4
    rows = half // parts
    tr, ti = twiddle_ref[0], twiddle_ref[1]
    for slot in range(slots):
        for f in range(4):
            columns = []
            for c in range(2):
                to = (slot * 2 + c) * rows
                pieces = [in_ref[f * parts + part, to : to + rows, :] for part in range(parts)]
                columns.append(jnp.concatenate(pieces, axis=0))
            high, low = halves(jnp.concatenate(columns, axis=1))
            at = (slot * 4 + f) * half
            high_ref[at : at + half, :] = high
            low_ref[at : at + half, :] = low
    right_transform(high_ref, low_ref, right_ref, spec_ref)
    for slot in range(slots):
        stacks = []
        for f in range(4):
            at = (slot * 4 + f) * half
            re = spec_ref[at : at + half, :lanes]
            im = spec_ref[at : at + half, lanes:]
            stacks.append(jnp.concatenate([re * tr - im * ti, re * ti + im * tr], axis=0))
        y = left_transform(jnp.concatenate(stacks, axis=1), left_ref)
        for f in range(4):
            x_ref[2 * f, slot] = y[:half, f * lanes : (f + 1) * lanes]
            x_ref[2 * f + 1, slot] = y[half:, f * lanes : (f + 1) * lanes]


def site_rows(plane, chunk, planes):
    return pl.ds(chunk * (8 * planes) + plane, 8, stride=planes)


def load_link(links_ref, direction, rows):
    base = direction * 18
    return [
        [(links_ref[base + 3 * i + j, rows, :], links_ref[base + 9 + 3 * i + j, rows, :]) for j in range(3)]
        for i in range(3)
    ]


def load_gauge(ref, plane, rows):
    return [
        [(ref[3 * i + j, plane, rows, :], ref[9 + 3 * i + j, plane, rows, :]) for j in range(3)]
        for i in range(3)
    ]


def store_gauge(ref, plane, rows, matrix):
    for i in range(3):
        for j in range(3):
            ref[3 * i + j, plane, rows, :] = matrix[i][j][0]
            ref[9 + 3 * i + j, plane, rows, :] = matrix[i][j][1]


def chunk_loop(planes, chunks, step):
    def run(index, carry):
        step(index // chunks, index % chunks)
        return carry

    lax.fori_loop(0, planes * chunks, run, 0)


def aligned(chunk):
    return pl.ds(pl.multiple_of(chunk * 8, 8), 8)


def shift_gauge(g_ref, y_ref, z_ref):
    planes = y_ref.shape[1]

    def run(index, carry):
        for plane in range(planes):
            v = g_ref[index, plane]
            y_ref[index, plane] = ahead_y(v)
            z_ref[index, plane] = ahead_z(v)
        return carry

    lax.fori_loop(0, 18, run, 0)


def divergence(v_ref, d_ref):
    planes = v_ref.shape[2]

    def run(comp, carry):
        before = None
        for plane in range(planes):
            vx = v_ref[0, comp, plane]
            vy = v_ref[1, comp, plane]
            vz = v_ref[2, comp, plane]
            total = (behind_y(vy) - vy) + (behind_z(vz) - vz) - vx
            if before is not None:
                total = total + before
            before = vx
            d_ref[plane, comp] = total
        d_ref[planes, comp] = before
        return carry

    lax.fori_loop(0, 8, run, 0)


def start_kernel(links_ref, left_ref, right_ref, twiddle_ref, out_ref, v_ref, d_ref, high_ref, low_ref, spec_ref):
    _, _, planes, half, _ = v_ref.shape

    def step(plane, chunk):
        rows = site_rows(plane, chunk, planes)
        for direction in range(3):
            for comp, value in enumerate(project(load_link(links_ref, direction, rows))):
                v_ref[direction, comp, plane, aligned(chunk), :] = value

    chunk_loop(planes, half // 8, step)
    divergence(v_ref, d_ref)
    forward_transform(d_ref, left_ref, right_ref, twiddle_ref, high_ref, low_ref, spec_ref, out_ref)


def convolve_kernel(planes, in_ref, table_ref, out_ref):
    count = in_ref.shape[0]
    parts, offsets, rows, _ = table_ref.shape
    across = planes * count
    part = lax.axis_index("space") % parts
    step = min(8, rows)

    def run(index, carry):
        c = index // (rows // step)
        chunk = index % (rows // step)

        def at(slot):
            return pl.ds((slot * 2 + c) * rows + chunk * step, step)

        table = [table_ref[part, k, pl.ds(chunk * step, step), :] for k in range(offsets)]
        data = []
        for x in range(across):
            owner, plane = divmod(x, planes)
            value = in_ref[owner, at(plane), :]
            if plane == 0:
                value = value + in_ref[(owner - 1) % count, at(planes), :]
            data.append(value)
        for x in range(across):
            owner, plane = divmod(x, planes)
            total = table[0] * data[x] + table[offsets - 1] * data[(x + across // 2) % across]
            for k in range(1, offsets - 1):
                total = total + table[k] * (data[(x + k) % across] + data[(x - k) % across])
            out_ref[owner, at(plane), :] = total
            if plane == 0:
                out_ref[(owner - 1) % count, at(planes), :] = total
        return carry

    lax.fori_loop(0, 2 * (rows // step), run, 0)


def emit_shares(x_ref, flat_ref, share_refs, planes):
    half = x_ref.shape[2]
    count = len(share_refs)
    per = share_refs[0].shape[1]
    if per * count > planes * half:
        flat_ref[...] = jnp.zeros_like(flat_ref)
    for comp in range(8):
        for plane in range(planes):
            flat_ref[comp, pl.ds(plane, half, stride=planes), :] = x_ref[comp, plane]
    mine = lax.axis_index("tm")
    for shift in range(count):
        start = pl.multiple_of((mine + shift) % count * per, 8)
        for comp in range(8):
            share_refs[shift][comp] = flat_ref[comp, pl.ds(start, per), :]


def middle_kernel(shares, in_ref, links_ref, ileft_ref, iright_ref, itwiddle_ref, left_ref, right_ref, twiddle_ref, *rest):
    out_ref, x_ref = rest[:2]
    share_refs = rest[2 : 2 + shares]
    g_ref, y_ref, z_ref, v_ref, d_ref, high_ref, low_ref, spec_ref, flat_ref = rest[2 + shares :]
    _, slots, half, _ = x_ref.shape
    planes = slots - 1
    inverse_transform(in_ref, ileft_ref, iright_ref, itwiddle_ref, high_ref, low_ref, spec_ref, x_ref)
    emit_shares(x_ref, flat_ref, share_refs, planes)

    def raise_step(plane, chunk):
        rows = aligned(chunk)
        store_gauge(g_ref, plane, rows, exponential([x_ref[k, plane, rows, :] for k in range(8)]))

    chunk_loop(slots, half // 8, raise_step)
    shift_gauge(g_ref, y_ref, z_ref)

    def rotate_step(plane, chunk):
        rows = aligned(chunk)
        gauge = load_gauge(g_ref, plane, rows)
        link_rows = site_rows(plane, chunk, planes)
        for direction in range(3):
            link = load_link(links_ref, direction, link_rows)
            if direction == 0:
                ahead = load_gauge(g_ref, plane + 1, rows)
            else:
                ahead = load_gauge((y_ref, z_ref)[direction - 1], plane, rows)
            turned = [row_times_dagger(row_times(gauge[i], link), ahead) for i in range(3)]
            for comp, value in enumerate(project(turned)):
                v_ref[direction, comp, plane, rows, :] = value

    chunk_loop(planes, half // 8, rotate_step)
    divergence(v_ref, d_ref)
    forward_transform(d_ref, left_ref, right_ref, twiddle_ref, high_ref, low_ref, spec_ref, out_ref)


def last_transform_kernel(shares, in_ref, ileft_ref, iright_ref, itwiddle_ref, *rest):
    x_ref = rest[0]
    share_refs = rest[1 : 1 + shares]
    high_ref, low_ref, spec_ref, flat_ref = rest[1 + shares :]
    inverse_transform(in_ref, ileft_ref, iright_ref, itwiddle_ref, high_ref, low_ref, spec_ref, x_ref)
    emit_shares(x_ref, flat_ref, share_refs, x_ref.shape[1] - 1)


def total_of(first, second):
    earlier = exponential(first)
    later = exponential(second)
    return [row_times(later[i], earlier) for i in range(3)]


def finish_kernel(times, src_time_ref, src_site_ref, links_ref, first_ref, second_ref, out_ref, anchor_ref, g_ref, y_ref, z_ref):
    _, slots, half, lanes = first_ref.shape
    planes = slots - 1

    def raise_step(plane, chunk):
        rows = aligned(chunk)
        store_gauge(
            g_ref,
            plane,
            rows,
            total_of(
                [first_ref[k, plane, rows, :] for k in range(8)],
                [second_ref[k, plane, rows, :] for k in range(8)],
            ),
        )

    chunk_loop(slots, half // 8, raise_step)
    shift_gauge(g_ref, y_ref, z_ref)

    def rotate_step(plane, chunk):
        rows = aligned(chunk)
        gauge = load_gauge(g_ref, plane, rows)
        link_rows = site_rows(plane, chunk, planes)
        for direction in range(3):
            link = load_link(links_ref, direction, link_rows)
            if direction == 0:
                ahead = load_gauge(g_ref, plane + 1, rows)
            else:
                ahead = load_gauge((y_ref, z_ref)[direction - 1], plane, rows)
            for i in range(3):
                row = row_times_dagger(row_times(gauge[i], link), ahead)
                for j in range(3):
                    out_ref[direction * 18 + 3 * i + j, link_rows, :] = row[j][0]
                    out_ref[direction * 18 + 9 + 3 * i + j, link_rows, :] = row[j][1]

    chunk_loop(planes, half // 8, rotate_step)

    site = src_site_ref[0]
    volume = half * lanes
    plane = site // volume - lax.axis_index("space") * planes
    column = site % volume
    present = (src_time_ref[0] % times == lax.axis_index("tm")) & (plane >= 0) & (plane < planes)
    safe = jnp.clip(plane, 0, planes - 1)
    wanted = jnp.where(present, column % lanes, -1)
    keep = lane_of((1, lanes)) == wanted
    anchor_ref[...] = jnp.zeros_like(anchor_ref)
    for k in range(18):
        row = g_ref[k, safe, pl.ds(column // lanes, 1), :]
        anchor_ref[k : k + 1, :] = jnp.where(keep, row, 0.0)


def lane_sums(rows):
    ones = jnp.ones((8, rows.shape[1]), BF16)
    total = None
    rest = rows
    for _ in range(3):
        piece = rest.astype(BF16)
        rest = rest - piece.astype(F32)
        part = lax.dot_general(ones, piece, (((1,), (1,)), ((), ())), preferred_element_type=F32)
        total = part if total is None else total + part
    return total


def sink_kernel(times, sink_ref, anchor_ref, *rest):
    first = rest[:times]
    second = rest[times : 2 * times]
    sources = rest[2 * times : 3 * times]
    out_ref, x_ref, sum_ref = rest[3 * times :]
    per = first[0].shape[1]
    pairs = sources[0].shape[0] // 2
    groups = pairs // 3
    mine = lax.axis_index("tm")
    wanted = (mine - sink_ref[0]) % times
    for shift in range(times):

        @pl.when(wanted == shift)
        def _(shift=shift):
            x_ref[0] = first[shift][...]
            x_ref[1] = second[shift][...]

    for chunk in range(per // 8):
        rows = slice(chunk * 8, chunk * 8 + 8)
        gauge = total_of([x_ref[0, k, rows, :] for k in range(8)], [x_ref[1, k, rows, :] for k in range(8)])
        for shift in range(times):
            base = (mine - shift) % times * pairs

            def run(group, carry, shift=shift, base=base):
                column = [
                    (sources[shift][3 * group + c, rows, :], sources[shift][pairs + 3 * group + c, rows, :])
                    for c in range(3)
                ]
                for a in range(3):
                    re, im = cmul(gauge[a][0], column[0])
                    for c in (1, 2):
                        more = cmul(gauge[a][c], column[c])
                        re = re + more[0]
                        im = im + more[1]
                    to = pl.ds(pl.multiple_of((base + 3 * group + a) * 8, 8), 8)
                    if chunk:
                        re = re + sum_ref[0, to, :]
                        im = im + sum_ref[1, to, :]
                    sum_ref[0, to, :] = re
                    sum_ref[1, to, :] = im
                return carry

            lax.fori_loop(0, groups, run, 0)
    whole = SC * SC
    lanes = anchor_ref.shape[1]
    width = -(-(whole + 24) // lanes) * lanes
    rows = []
    for part in range(2):
        total = sum_ref[part, pl.ds(0, whole, stride=8), :]
        for k in range(1, 8):
            total = total + sum_ref[part, pl.ds(k, whole, stride=8), :]
        fill = jnp.zeros((width - whole - 24, lanes), F32)
        extra = anchor_ref[...] if part == 0 else jnp.zeros((24, lanes), F32)
        sums = lane_sums(jnp.concatenate([total, extra, fill], axis=0))
        for k in range(width // lanes):
            rows.append(sums[0:1, k * lanes : (k + 1) * lanes])
    block = jnp.concatenate(rows, axis=0)

    def spread(index, carry):
        out_ref[index] = block
        return carry

    lax.fori_loop(0, out_ref.shape[0], spread, 0)


def wall_kernel(scale, in_ref, out_ref):
    whole = SC * SC
    total = jnp.sum(in_ref[...], axis=0)
    half = total.shape[0] // 2
    re = jnp.concatenate([total[k : k + 1] for k in range(half)], axis=1)
    im = jnp.concatenate([total[half + k : half + k + 1] for k in range(half)], axis=1)
    width = re.shape[1]
    colour = lane_of((1, width)) // SC % 3
    out_re = jnp.zeros((1, width), F32)
    out_im = jnp.zeros((1, width), F32)
    for b in range(3):
        for c in range(3):
            at = whole + 3 * b + c
            ar = re[:, at : at + 1]
            ai = re[:, at + 9 : at + 10]
            amount = (SC * (b - c)) % width
            wr = pltpu.roll(re, amount, axis=1) if amount else re
            wi = pltpu.roll(im, amount, axis=1) if amount else im
            here = colour == b
            out_re = out_re + jnp.where(here, wr * ar + wi * ai, 0.0)
            out_im = out_im + jnp.where(here, wi * ar - wr * ai, 0.0)
    out_ref[0:1, :] = out_re[:, :whole] * scale
    out_ref[1:2, :] = out_im[:, :whole] * scale


def shape(*dims):
    return jax.ShapeDtypeStruct(dims, F32)


def call(kernel, outs, inputs, scratch, scalars=0):
    smem = pl.BlockSpec(memory_space=pltpu.SMEM)
    vmem = pl.BlockSpec(memory_space=pltpu.VMEM)
    return pl.pallas_call(
        kernel,
        out_shape=outs,
        in_specs=[smem] * scalars + [vmem] * (len(inputs) - scalars),
        out_specs=[vmem] * len(outs),
        scratch_shapes=scratch,
        compiler_params=pltpu.CompilerParams(vmem_limit_bytes=50 * 1024 * 1024),
    )(*inputs)


def body(links, propagator, sink_time, src_time, src_site):
    count = lax.axis_size("space")
    times = lax.axis_size("tm")
    planes = links.shape[5]
    side = math.isqrt(links.shape[6])
    half, lanes = side // 2, 2 * side
    across = planes * count
    slots = planes + 1
    parts = count // 4
    rows = half // parts
    sites = planes * half
    per = 8 * -(-sites // (8 * times))
    pairs = propagator.shape[1]
    mine = lax.axis_index("tm")

    forward = [jnp.asarray(t) for t in transform_tables(side, False)]
    inverse = [jnp.asarray(t) for t in transform_tables(side, True)]
    table = jnp.asarray(filter_table(side, across, parts))

    def interleave(array, lead):
        return array.reshape(lead, planes, half, lanes).transpose(0, 2, 1, 3).reshape(lead, sites, lanes)

    lattice = interleave(links, 54)
    source = interleave(propagator, 2 * pairs)
    if per * times > sites:
        source = jnp.pad(source, ((0, 0), (0, per * times - sites), (0, 0)))

    def forwarded(value, shift):
        if shift == 0:
            return value
        return lax.ppermute(value, "tm", [(i, (i + shift) % times) for i in range(times)])

    sources = []
    for shift in range(times):
        block = lax.dynamic_slice_in_dim(source, (mine + shift) % times * per, per, 1)
        sources.append(forwarded(block, shift))

    spectrum_shape = shape(count, slots * 2 * rows, lanes)
    transform_scratch = [
        VMEM((4 * slots * half, 2 * lanes), BF16),
        VMEM((4 * slots * half, 2 * lanes), BF16),
        VMEM((4 * slots * half, 2 * lanes), F32),
    ]
    divergence_scratch = [
        VMEM((3, 8, planes, half, lanes), F32),
        VMEM((slots, 8, half, lanes), F32),
    ]
    gauge_scratch = [
        VMEM((18, slots, half, lanes), F32),
        VMEM((18, planes, half, lanes), F32),
        VMEM((18, planes, half, lanes), F32),
    ]
    flat_scratch = [VMEM((8, per * times, lanes), F32)]
    algebra_shape = shape(8, slots, half, lanes)
    share_shapes = [shape(8, per, lanes)] * times

    def turn(spectrum):
        return lax.all_to_all(spectrum, "space", 0, 0, tiled=True)

    def filtered(spectrum):
        (out,) = call(
            functools.partial(convolve_kernel, planes), [spectrum_shape], [turn(spectrum), table], []
        )
        return turn(out)

    (spectrum,) = call(
        start_kernel, [spectrum_shape], [lattice] + forward, divergence_scratch + transform_scratch
    )
    spectrum, first, *shares = call(
        functools.partial(middle_kernel, times),
        [spectrum_shape, algebra_shape] + share_shapes,
        [filtered(spectrum), lattice] + inverse + forward,
        gauge_scratch + divergence_scratch + transform_scratch + flat_scratch,
    )
    first_shares = [forwarded(share, shift) for shift, share in enumerate(shares)]
    second, *shares = call(
        functools.partial(last_transform_kernel, times),
        [algebra_shape] + share_shapes,
        [filtered(spectrum)] + inverse,
        transform_scratch + flat_scratch,
    )
    second_shares = [forwarded(share, shift) for shift, share in enumerate(shares)]
    fixed, anchor = call(
        functools.partial(finish_kernel, times),
        [shape(54, sites, lanes), shape(24, lanes)],
        [src_time, src_site, lattice, first, second],
        gauge_scratch,
        scalars=2,
    )
    width = -(-(SC * SC + 24) // lanes)
    devices = count * times
    (payload,) = call(
        functools.partial(sink_kernel, times),
        [shape(devices, 2 * width, lanes)],
        [sink_time, anchor] + first_shares + second_shares + sources,
        [VMEM((2, 8, per, lanes), F32), VMEM((2, SC * SC * 8, lanes), F32)],
        scalars=1,
    )
    gathered = lax.all_to_all(payload, ("space", "tm"), 0, 0, tiled=True)
    scale = float(across * side * side) ** (-0.5)
    (wall,) = call(functools.partial(wall_kernel, scale), [shape(2, SC * SC)], [gathered], [])
    fixed = fixed.reshape(54, half, planes, lanes).transpose(0, 2, 1, 3).reshape(links.shape)
    return fixed, wall


def solution(mesh):
    placed = (
        P("tm", None, None, None, None, "space", None),
        P(None, "tm", "space", None),
        P(),
        P(),
        P(),
    )
    return jax.shard_map(
        body,
        mesh=mesh,
        in_specs=placed,
        out_specs=(P("tm", None, None, None, None, "space", None), P()),
        check_vma=False,
    )
```

```python
import functools
import math

import jax
import jax.numpy as jnp
import numpy as np
from jax import lax
from jax.experimental import pallas as pl
from jax.experimental.pallas import tpu as pltpu
from jax.sharding import PartitionSpec as P


SC = 12
STEP_SIZE = 0.08
PEAK_SQUARE = 12.0
F32 = jnp.float32
BF16 = jnp.bfloat16
VMEM = pltpu.VMEM
PAIRS = ((0, 1), (0, 2), (1, 2))


def split_table(table):
    high = table.astype(jnp.bfloat16)
    low = (table - high.astype(np.float64)).astype(jnp.bfloat16)
    return high, low


def as_real(real, imag):
    return np.block([[real, imag], [-imag, real]])


@functools.lru_cache(None)
def transform_table(side, inverse):
    half = side // 2
    sign = 1.0 if inverse else -1.0
    k = np.arange(half)
    twist = np.exp(1j * sign * 2.0 * np.pi * k / side)
    even = np.exp(1j * sign * 2.0 * np.pi * np.outer(k, k) / half)
    odd = even * (twist[None, :] if inverse else twist[:, None])
    left = np.concatenate([as_real(m.real, -m.imag) for m in (even, odd)], axis=0)
    high, low = split_table(left)
    fill = np.zeros((left.shape[0], 4 * side - 3 * side), high.dtype)
    left = np.concatenate([high, low, high, fill], axis=1)
    z = np.arange(side)
    depth_phase = sign * 2.0 * np.pi * np.outer(z, z) / side
    parity = np.array([[1.0, 1.0], [1.0, -1.0]])
    right = as_real(np.kron(parity, np.cos(depth_phase)), np.kron(parity, np.sin(depth_phase)))
    high, low = split_table(right)
    return np.concatenate([high, low, left], axis=0)


@functools.lru_cache(None)
def filter_table(side, across, blocks):
    half = side // 2
    squares = 4.0 * np.sin(np.pi * np.arange(side) / side) ** 2
    squares_across = 4.0 * np.sin(np.pi * np.arange(across) / across) ** 2
    column = (squares[:, None] + squares[None, :]).reshape(2, half, side)
    column = np.swapaxes(column, 0, 1).reshape(half, 2 * side)
    momentum = squares_across[:, None, None] + column[None]
    weight = np.where(momentum > 0.0, PEAK_SQUARE / np.where(momentum > 0.0, momentum, 1.0), 0.0)
    offsets = np.arange(across // 2 + 1)
    phase = np.cos(2.0 * np.pi * np.outer(offsets, np.arange(across)) / across)
    table = np.einsum("dk,krl->drl", phase, weight) / (across * side * side)
    table = table * (STEP_SIZE / 16.0)
    table = table.reshape(len(offsets), blocks, half // blocks, 2 * side)
    return np.ascontiguousarray(np.swapaxes(table, 0, 1)).astype(np.float32)


def cmul(x, y):
    return x[0] * y[0] - x[1] * y[1], x[0] * y[1] + x[1] * y[0]


def csquare(x):
    return x[0] * x[0] - x[1] * x[1], 2.0 * (x[0] * x[1])


def row_times(row, matrix):
    out = []
    for b in range(3):
        re = row[0][0] * matrix[0][b][0] - row[0][1] * matrix[0][b][1]
        im = row[0][0] * matrix[0][b][1] + row[0][1] * matrix[0][b][0]
        for k in (1, 2):
            re = re + row[k][0] * matrix[k][b][0] - row[k][1] * matrix[k][b][1]
            im = im + row[k][0] * matrix[k][b][1] + row[k][1] * matrix[k][b][0]
        out.append((re, im))
    return out


def row_times_dagger(row, matrix):
    out = []
    for b in range(3):
        re = row[0][0] * matrix[b][0][0] + row[0][1] * matrix[b][0][1]
        im = row[0][1] * matrix[b][0][0] - row[0][0] * matrix[b][0][1]
        for k in (1, 2):
            re = re + row[k][0] * matrix[b][k][0] + row[k][1] * matrix[b][k][1]
            im = im + row[k][1] * matrix[b][k][0] - row[k][0] * matrix[b][k][1]
        out.append((re, im))
    return out


def exponential(x):
    t0, t1 = x[0], x[1]
    a, b, e = (x[2], x[3]), (x[4], x[5]), (x[6], x[7])
    t2 = -(t0 + t1)
    na = a[0] * a[0] + a[1] * a[1]
    nb = b[0] * b[0] + b[1] * b[1]
    ne = e[0] * e[0] + e[1] * e[1]
    s0, s1, s2 = t0 * t0, t1 * t1, t2 * t2
    ae = cmul(a, e)
    c = -(0.5 * (s0 + s1 + s2) + (na + nb + ne))
    cross = ae[1] * b[0] - ae[0] * b[1]
    d = t0 * ne + t1 * nb + t2 * na - t0 * t1 * t2 - 2.0 * cross
    c30 = c * (1.0 / 30.0)
    q0 = (None, d * (1.0 / 120.0))
    q1 = ((1.0 + c30) * 0.25, None)
    q2r = 1.0 / 20.0
    n0i = d * (q2r / 3.0)
    n1 = ((1.0 + c * q2r) * (1.0 / 3.0), q0[1] * (1.0 / 3.0))
    n2r = q1[0] * (1.0 / 3.0)
    m0 = (None, d * (0.5 * n2r))
    m1 = (0.5 + 0.5 * (c * n2r), 0.5 * n0i)
    m2 = (0.5 * n1[0], 0.5 * n1[1])
    q0 = (1.0 - d * m2[1], d * m2[0])
    q1 = (1.0 + c * m2[0], m0[1] + c * m2[1])
    q2 = m1
    for _ in range(3):
        q12 = cmul(q1, q2)
        q22 = csquare(q2)
        q00 = csquare(q0)
        q11 = csquare(q1)
        q01 = cmul(q0, q1)
        q02 = cmul(q0, q2)
        d2 = 2.0 * d
        q0 = (q00[0] - d2 * q12[1], q00[1] + d2 * q12[0])
        q1 = (
            2.0 * (q01[0] + c * q12[0]) - d * q22[1],
            2.0 * (q01[1] + c * q12[1]) + d * q22[0],
        )
        q2 = (q11[0] + 2.0 * q02[0] + c * q22[0], q11[1] + 2.0 * q02[1] + c * q22[1])
    u, v = q1
    s, t = q2
    result = [[None] * 3 for _ in range(3)]
    for at, (theta, m) in enumerate(
        ((t0, -(s0 + na + nb)), (t1, -(s1 + na + ne)), (t2, -(s2 + nb + ne)))
    ):
        result[at][at] = (q0[0] - v * theta + s * m, q0[1] + u * theta + t * m)
    y01 = (t2 * a[1] - (b[0] * e[0] + b[1] * e[1]), -t2 * a[0] - (b[1] * e[0] - b[0] * e[1]))
    y02 = (t1 * b[1] + ae[0], -t1 * b[0] + ae[1])
    y12 = (t0 * e[1] - (a[0] * b[0] + a[1] * b[1]), -t0 * e[0] - (a[0] * b[1] - a[1] * b[0]))
    for (i, j), xx, yy in zip(PAIRS, (a, b, e), (y01, y02, y12)):
        ur, vi, ui, vr = u * xx[0], v * xx[1], u * xx[1], v * xx[0]
        sr, ti, si, tr = s * yy[0], t * yy[1], s * yy[1], t * yy[0]
        result[i][j] = ((ur - vi) + (sr - ti), (ui + vr) + (si + tr))
        result[j][i] = ((sr + ti) - (ur + vi), (tr - si) + (ui - vr))
    return result


def project(rows):
    third = (rows[0][0][1] + rows[1][1][1] + rows[2][2][1]) * (1.0 / 3.0)
    out = [rows[0][0][1] - third, rows[1][1][1] - third]
    for i, j in PAIRS:
        out.append(0.5 * (rows[i][j][0] - rows[j][i][0]))
        out.append(0.5 * (rows[i][j][1] + rows[j][i][1]))
    return out


def lane_of(shape):
    return lax.broadcasted_iota(jnp.int32, shape, 1)


def ahead_y(v):
    half = v.shape[1] // 2
    r = pltpu.roll(v, half, axis=1)
    return jnp.where(lane_of(v.shape) < half, r, pltpu.roll(r, v.shape[0] - 1, axis=0))


def behind_y(v):
    half = v.shape[1] // 2
    r = pltpu.roll(v, half, axis=1)
    return jnp.where(lane_of(v.shape) >= half, r, pltpu.roll(r, 1, axis=0))


def ahead_z(v):
    lanes = v.shape[1]
    half = lanes // 2
    inner = pltpu.roll(v, lanes - 1, axis=1)
    edge = pltpu.roll(v, half - 1, axis=1)
    return jnp.where(lane_of(v.shape) % half == half - 1, edge, inner)


def behind_z(v):
    lanes = v.shape[1]
    half = lanes // 2
    inner = pltpu.roll(v, 1, axis=1)
    edge = pltpu.roll(v, half + 1, axis=1)
    return jnp.where(lane_of(v.shape) % half == 0, edge, inner)


def halves(x):
    high = x.astype(BF16)
    low = (x - high.astype(F32)).astype(BF16)
    return high, low


def dot(x, y):
    return jnp.dot(x, y, preferred_element_type=F32)


def left_transform(stacked, table_ref):
    high, low = halves(stacked)
    depth, width = stacked.shape
    at = 2 * table_ref.shape[1]
    both = dot(
        table_ref[at : at + 2 * depth, : 3 * depth], jnp.concatenate([high, high, low], axis=0)
    )
    even = lane_of((depth, width)) % (2 * depth) < depth
    return jnp.where(even, both[:depth], both[depth:])


def right_transform(high_ref, low_ref, table_ref, out_ref):
    size = table_ref.shape[1]
    high = high_ref[...]
    first = table_ref[:size]
    out_ref[...] = dot(high, first) + dot(low_ref[...], first) + dot(high, table_ref[size : 2 * size])


def forward_transform(d_ref, table_ref, high_ref, low_ref, spec_ref, out_ref):
    slots, _, half, lanes = d_ref.shape
    parts = out_ref.shape[0] // 4
    rows = half // parts
    for slot in range(slots):
        stacked = jnp.concatenate(
            [
                jnp.concatenate([d_ref[slot, 2 * f], d_ref[slot, 2 * f + 1]], axis=0)
                for f in range(4)
            ],
            axis=1,
        )
        y = left_transform(stacked, table_ref)
        for f in range(4):
            re = y[:half, f * lanes : (f + 1) * lanes]
            im = y[half:, f * lanes : (f + 1) * lanes]
            high, low = halves(jnp.concatenate([re, im], axis=1))
            at = (slot * 4 + f) * half
            high_ref[at : at + half, :] = high
            low_ref[at : at + half, :] = low
    right_transform(high_ref, low_ref, table_ref, spec_ref)
    for slot in range(slots):
        for f in range(4):
            for part in range(parts):
                at = (slot * 4 + f) * half + part * rows
                for c in range(2):
                    to = (slot * 2 + c) * rows
                    out_ref[f * parts + part, to : to + rows, :] = spec_ref[
                        at : at + rows, c * lanes : (c + 1) * lanes
                    ]


def inverse_transform(in_ref, table_ref, high_ref, low_ref, spec_ref, x_ref):
    _, slots, half, lanes = x_ref.shape
    parts = in_ref.shape[0] // 4
    rows = half // parts
    for slot in range(slots):
        for f in range(4):
            columns = []
            for c in range(2):
                to = (slot * 2 + c) * rows
                pieces = [in_ref[f * parts + part, to : to + rows, :] for part in range(parts)]
                columns.append(jnp.concatenate(pieces, axis=0))
            high, low = halves(jnp.concatenate(columns, axis=1))
            at = (slot * 4 + f) * half
            high_ref[at : at + half, :] = high
            low_ref[at : at + half, :] = low
    right_transform(high_ref, low_ref, table_ref, spec_ref)
    for slot in range(slots):
        stacks = []
        for f in range(4):
            at = (slot * 4 + f) * half
            stacks.append(
                jnp.concatenate([spec_ref[at : at + half, :lanes], spec_ref[at : at + half, lanes:]], axis=0)
            )
        y = left_transform(jnp.concatenate(stacks, axis=1), table_ref)
        for f in range(4):
            x_ref[2 * f, slot] = y[:half, f * lanes : (f + 1) * lanes]
            x_ref[2 * f + 1, slot] = y[half:, f * lanes : (f + 1) * lanes]


def site_rows(plane, chunk, planes):
    return pl.ds(chunk * (8 * planes) + plane, 8, stride=planes)


def load_link(links_ref, direction, rows):
    base = direction * 18
    return [
        [(links_ref[base + 3 * i + j, rows, :], links_ref[base + 9 + 3 * i + j, rows, :]) for j in range(3)]
        for i in range(3)
    ]


def load_gauge(ref, plane, rows):
    return [
        [(ref[3 * i + j, plane, rows, :], ref[9 + 3 * i + j, plane, rows, :]) for j in range(3)]
        for i in range(3)
    ]


def store_gauge(ref, plane, rows, matrix):
    for i in range(3):
        for j in range(3):
            ref[3 * i + j, plane, rows, :] = matrix[i][j][0]
            ref[9 + 3 * i + j, plane, rows, :] = matrix[i][j][1]


def chunk_loop(planes, chunks, step):
    def run(index, carry):
        step(index // chunks, index % chunks)
        return carry

    lax.fori_loop(0, planes * chunks, run, 0)


def aligned(chunk):
    return pl.ds(pl.multiple_of(chunk * 8, 8), 8)


def shift_gauge(g_ref, y_ref, z_ref):
    planes = y_ref.shape[1]

    def run(index, carry):
        for plane in range(planes):
            v = g_ref[index, plane]
            y_ref[index, plane] = ahead_y(v)
            z_ref[index, plane] = ahead_z(v)
        return carry

    lax.fori_loop(0, 18, run, 0)


def divergence(v_ref, d_ref):
    planes = v_ref.shape[2]

    def run(comp, carry):
        before = None
        for plane in range(planes):
            vx = v_ref[0, comp, plane]
            vy = v_ref[1, comp, plane]
            vz = v_ref[2, comp, plane]
            total = (behind_y(vy) - vy) + (behind_z(vz) - vz) - vx
            if before is not None:
                total = total + before
            before = vx
            d_ref[plane, comp] = total
        d_ref[planes, comp] = before
        return carry

    lax.fori_loop(0, 8, run, 0)


def start_kernel(times, links_any, table_any, source_any, out_ref, *rest):
    cut_refs = rest[: times - 1]
    held_ref, links_ref, table_ref, v_ref, d_ref, high_ref, low_ref, spec_ref, sems, cut_sems = rest[times - 1 :]
    _, _, planes, half, _ = v_ref.shape
    per = held_ref.shape[2]
    reads, writes = [], []
    for shift, cut in enumerate(cut_refs, 1):
        rows = pl.ds(share_start(shift, times, per), per)
        reads.append(
            pltpu.make_async_copy(source_any.at[:, rows, :], held_ref.at[shift - 1], cut_sems.at[0, shift - 1])
        )
        writes.append(pltpu.make_async_copy(held_ref.at[shift - 1], cut, cut_sems.at[1, shift - 1]))
    copies = [
        pltpu.make_async_copy(
            links_any.at[pl.ds(18 * direction, 18)], links_ref.at[pl.ds(18 * direction, 18)], sems.at[direction]
        )
        for direction in range(3)
    ]
    copies.append(pltpu.make_async_copy(table_any, table_ref, sems.at[3]))
    for copy in copies + reads:
        copy.start()
    for direction in range(3):
        copies[direction].wait()

        def step(plane, chunk, direction=direction):
            rows = site_rows(plane, chunk, planes)
            for comp, value in enumerate(project(load_link(links_ref, direction, rows))):
                v_ref[direction, comp, plane, aligned(chunk), :] = value

        chunk_loop(planes, half // 8, step)
    for read, write in zip(reads, writes):
        read.wait()
        write.start()
    divergence(v_ref, d_ref)
    copies[3].wait()
    forward_transform(d_ref, table_ref, high_ref, low_ref, spec_ref, out_ref)
    for write in writes:
        write.wait()


def convolve_kernel(planes, in_ref, table_ref, out_ref):
    count = in_ref.shape[0]
    parts, offsets, rows, _ = table_ref.shape
    across = planes * count
    part = lax.axis_index("space") % parts
    step = min(8, rows)

    def run(index, carry):
        c = index // (rows // step)
        chunk = index % (rows // step)

        def at(slot):
            return pl.ds((slot * 2 + c) * rows + chunk * step, step)

        table = [table_ref[part, k, pl.ds(chunk * step, step), :] for k in range(offsets)]
        data = []
        for x in range(across):
            owner, plane = divmod(x, planes)
            value = in_ref[owner, at(plane), :]
            if plane == 0:
                value = value + in_ref[(owner - 1) % count, at(planes), :]
            data.append(value)
        for x in range(across):
            owner, plane = divmod(x, planes)
            total = table[0] * data[x] + table[offsets - 1] * data[(x + across // 2) % across]
            for k in range(1, offsets - 1):
                total = total + table[k] * (data[(x + k) % across] + data[(x - k) % across])
            out_ref[owner, at(plane), :] = total
            if plane == 0:
                out_ref[(owner - 1) % count, at(planes), :] = total
        return carry

    lax.fori_loop(0, 2 * (rows // step), run, 0)


def flatten_shares(x_ref, flat_ref, planes):
    half = x_ref.shape[2]
    if flat_ref.shape[1] > planes * half:
        flat_ref[...] = jnp.zeros_like(flat_ref)
    for comp in range(8):
        for plane in range(planes):
            flat_ref[comp, pl.ds(plane, half, stride=planes), :] = x_ref[comp, plane]


def share_start(shift, count, per):
    return pl.multiple_of((lax.axis_index("tm") + shift) % count * per, 8)


def middle_kernel(shares, in_ref, links_ref, inverse_ref, forward_ref, *rest):
    out_ref, x_any = rest[:2]
    share_refs = rest[2 : 2 + shares]
    x_ref, g_ref, y_ref, z_ref, v_ref, d_ref, high_ref, low_ref, spec_ref, flat_ref, sems = rest[2 + shares :]
    _, slots, half, _ = x_ref.shape
    planes = slots - 1
    per = share_refs[0].shape[1]
    inverse_transform(in_ref, inverse_ref, high_ref, low_ref, spec_ref, x_ref)
    flatten_shares(x_ref, flat_ref, planes)
    copies = [
        pltpu.make_async_copy(
            flat_ref.at[:, pl.ds(share_start(shift, shares, per), per), :], share_refs[shift], sems.at[shift]
        )
        for shift in range(shares)
    ]
    copies.append(pltpu.make_async_copy(x_ref, x_any, sems.at[shares]))
    for copy in copies:
        copy.start()

    def raise_step(plane, chunk):
        rows = aligned(chunk)
        store_gauge(g_ref, plane, rows, exponential([x_ref[k, plane, rows, :] for k in range(8)]))

    chunk_loop(slots, half // 8, raise_step)
    shift_gauge(g_ref, y_ref, z_ref)

    def rotate_step(plane, chunk):
        rows = aligned(chunk)
        gauge = load_gauge(g_ref, plane, rows)
        link_rows = site_rows(plane, chunk, planes)
        for direction in range(3):
            link = load_link(links_ref, direction, link_rows)
            if direction == 0:
                ahead = load_gauge(g_ref, plane + 1, rows)
            else:
                ahead = load_gauge((y_ref, z_ref)[direction - 1], plane, rows)
            turned = [row_times_dagger(row_times(gauge[i], link), ahead) for i in range(3)]
            for comp, value in enumerate(project(turned)):
                v_ref[direction, comp, plane, rows, :] = value

    chunk_loop(planes, half // 8, rotate_step)
    divergence(v_ref, d_ref)
    forward_transform(d_ref, forward_ref, high_ref, low_ref, spec_ref, out_ref)
    for copy in copies:
        copy.wait()


def last_transform_kernel(in_ref, inverse_ref, x_ref, *rest):
    share_refs = rest[:-4]
    high_ref, low_ref, spec_ref, flat_ref = rest[-4:]
    per = share_refs[0].shape[1]
    inverse_transform(in_ref, inverse_ref, high_ref, low_ref, spec_ref, x_ref)
    flatten_shares(x_ref, flat_ref, x_ref.shape[1] - 1)
    for to, share_ref in enumerate(share_refs):
        share_ref[...] = flat_ref[:, to * per : (to + 1) * per, :]


def total_of(first, second):
    earlier = exponential(first)
    later = exponential(second)
    return [row_times(later[i], earlier) for i in range(3)]


def finish_kernel(links_any, first_any, second_ref, out_any, g_ref, y_ref, z_ref, links_ref, first_ref, out_ref, sems):
    _, slots, half, _ = first_ref.shape
    planes = slots - 1
    chunks = half // 8
    copies = [
        pltpu.make_async_copy(first_any, first_ref, sems.at[0]),
        pltpu.make_async_copy(links_any, links_ref, sems.at[1]),
    ]
    for copy in copies:
        copy.start()
    copies[0].wait()

    def raise_step(plane, chunk):
        rows = aligned(chunk)
        store_gauge(
            g_ref,
            plane,
            rows,
            total_of(
                [first_ref[k, plane, rows, :] for k in range(8)],
                [second_ref[k, plane, rows, :] for k in range(8)],
            ),
        )

    chunk_loop(slots, half // 8, raise_step)
    shift_gauge(g_ref, y_ref, z_ref)
    copies[1].wait()

    def piece(chunk):
        rows = pl.ds(pl.multiple_of(chunk * (8 * planes), 8), 8 * planes)
        return pltpu.make_async_copy(out_ref.at[:, rows, :], out_any.at[:, rows, :], sems.at[2 + chunk])

    def rotate_step(chunk, plane):
        rows = aligned(chunk)
        gauge = load_gauge(g_ref, plane, rows)
        link_rows = site_rows(plane, chunk, planes)
        for direction in range(3):
            link = load_link(links_ref, direction, link_rows)
            if direction == 0:
                ahead = load_gauge(g_ref, plane + 1, rows)
            else:
                ahead = load_gauge((y_ref, z_ref)[direction - 1], plane, rows)
            for i in range(3):
                row = row_times_dagger(row_times(gauge[i], link), ahead)
                for j in range(3):
                    out_ref[direction * 18 + 3 * i + j, link_rows, :] = row[j][0]
                    out_ref[direction * 18 + 9 + 3 * i + j, link_rows, :] = row[j][1]

        @pl.when(plane == planes - 1)
        def _():
            piece(chunk).start()

    chunk_loop(chunks, planes, rotate_step)

    for chunk in range(chunks):
        piece(chunk).wait()


def lane_sums(rows):
    ones = jnp.ones((8, rows.shape[1]), BF16)
    total = None
    rest = rows
    for _ in range(3):
        piece = rest.astype(BF16)
        rest = rest - piece.astype(F32)
        part = lax.dot_general(ones, piece, (((1,), (1,)), ((), ())), preferred_element_type=F32)
        total = part if total is None else total + part
    return total


def sink_kernel(times, split, scalar_ref, first_any, second_ref, own_early_ref, *rest):
    early = (own_early_ref,) + rest[: times - 1]
    own = rest[times - 1 : times - 1 + split]
    late = rest[times - 1 + split : 2 * times - 2 + split]
    sources_any = rest[2 * times - 2 + split : 2 * times - 2 + 2 * split]
    out_ref, source_ref, x_ref, gauge_ref, sum_ref, before_ref, anchor_ref, sems = rest[2 * times - 2 + 2 * split :]
    per = early[0].shape[1]
    pairs = source_ref.shape[1] // 2
    groups = pairs // 3
    _, slots, half, lanes = second_ref.shape
    planes = slots - 1
    mine = lax.axis_index("tm")
    local = sources_any[0].at[:, pl.ds(share_start(0, split, per), per), :]
    sink = scalar_ref[0]
    column = scalar_ref[2] % (half * lanes)
    plane = scalar_ref[2] // (half * lanes) - lax.axis_index("space") * planes
    present = (scalar_ref[1] == mine) & (plane >= 0) & (plane < planes)
    safe = jnp.clip(plane, 0, planes - 1)
    row = column // lanes
    block = pl.ds(pl.multiple_of(row // 8 * 8, 8), 8)
    before = pltpu.make_async_copy(first_any.at[:, safe, block, :], before_ref, sems.at[split])
    copies = [
        pltpu.make_async_copy(sources_any[shift] if shift else local, source_ref.at[shift], sems.at[shift])
        for shift in range(split)
    ]
    before.start()
    for copy in copies:
        copy.start()
    wanted = (mine - sink) % times
    for shift in range(times):

        @pl.when(wanted == shift)
        def _(shift=shift):
            x_ref[0] = early[shift][...]

    for at in range(split):

        @pl.when((mine == sink) & (mine % split == at))
        def _(at=at):
            x_ref[1] = own[at][...]

    for at in range(times - 1):

        @pl.when((mine != sink) & (jnp.where(mine > sink, mine - 1, mine) == at))
        def _(at=at):
            x_ref[1] = late[at][...]

    chunks = per // 8
    for chunk in range(chunks):
        rows = slice(chunk * 8, chunk * 8 + 8)
        gauge = total_of([x_ref[0, k, rows, :] for k in range(8)], [x_ref[1, k, rows, :] for k in range(8)])
        for i in range(3):
            for j in range(3):
                gauge_ref[3 * i + j, rows, :] = gauge[i][j][0]
                gauge_ref[9 + 3 * i + j, rows, :] = gauge[i][j][1]
    sum_ref[...] = jnp.zeros_like(sum_ref)
    for shift in range(split):
        copies[shift].wait()
        base = (mine - mine % split + (mine - shift) % split) * pairs

        def run(group, carry, shift=shift, base=base):
            sums = [None] * 3
            for chunk in range(chunks):
                rows = slice(chunk * 8, chunk * 8 + 8)
                column = [
                    (
                        source_ref[shift, 3 * group + c, rows, :],
                        source_ref[shift, pairs + 3 * group + c, rows, :],
                    )
                    for c in range(3)
                ]
                for a in range(3):
                    for c in range(3):
                        part = cmul(
                            (gauge_ref[3 * a + c, rows, :], gauge_ref[9 + 3 * a + c, rows, :]), column[c]
                        )
                        sums[a] = part if sums[a] is None else (sums[a][0] + part[0], sums[a][1] + part[1])
            for a in range(3):
                to = pl.ds(pl.multiple_of((base + 3 * group + a) * 8, 8), 8)
                sum_ref[0, to, :] = sums[a][0]
                sum_ref[1, to, :] = sums[a][1]
            return carry

        lax.fori_loop(0, groups, run, 0, unroll=2 if groups % 2 == 0 else 1)
    before.wait()
    total = total_of([before_ref[k] for k in range(8)], [second_ref[k, safe, block, :] for k in range(8)])
    wide = (8, lanes)
    keep = (lane_of(wide) == jnp.where(present, column % lanes, -1)) & (
        lax.broadcasted_iota(jnp.int32, wide, 0) == row % 8
    )
    anchor_ref[...] = jnp.zeros_like(anchor_ref)
    for k in range(18):
        value = total[k % 9 // 3][k % 3][k // 9]
        anchor_ref[k : k + 1, :] = jnp.sum(jnp.where(keep, value, 0.0), axis=0, keepdims=True)
    whole = SC * SC
    width = -(-(whole + 24) // lanes) * lanes
    pieces = []
    for part in range(2):
        total = sum_ref[part, pl.ds(0, whole, stride=8), :]
        for k in range(1, 8):
            total = total + sum_ref[part, pl.ds(k, whole, stride=8), :]
        extra = anchor_ref[...] if part == 0 else jnp.zeros((24, lanes), F32)
        pieces += [total, extra, jnp.zeros((width - whole - 24, lanes), F32)]
    sums = lane_sums(jnp.concatenate(pieces, axis=0))
    block = jnp.concatenate(
        [sums[0:1, k * lanes : (k + 1) * lanes] for k in range(2 * width // lanes)], axis=0
    )

    def spread(index, carry):
        out_ref[index] = block
        return carry

    lax.fori_loop(0, out_ref.shape[0], spread, 0)


def wall_kernel(scale, in_ref, out_ref):
    whole = SC * SC
    total = jnp.sum(in_ref[...], axis=0)
    half = total.shape[0] // 2
    re = jnp.concatenate([total[k : k + 1] for k in range(half)], axis=1)
    im = jnp.concatenate([total[half + k : half + k + 1] for k in range(half)], axis=1)
    width = re.shape[1]
    colour = lane_of((1, width)) // SC % 3
    out_re = jnp.zeros((1, width), F32)
    out_im = jnp.zeros((1, width), F32)
    for b in range(3):
        for c in range(3):
            at = whole + 3 * b + c
            ar = re[:, at : at + 1]
            ai = re[:, at + 9 : at + 10]
            amount = (SC * (b - c)) % width
            wr = pltpu.roll(re, amount, axis=1) if amount else re
            wi = pltpu.roll(im, amount, axis=1) if amount else im
            here = colour == b
            out_re = out_re + jnp.where(here, wr * ar + wi * ai, 0.0)
            out_im = out_im + jnp.where(here, wi * ar - wr * ai, 0.0)
    out_ref[0:1, :] = out_re[:, :whole] * scale
    out_ref[1:2, :] = out_im[:, :whole] * scale


def shape(*dims):
    return jax.ShapeDtypeStruct(dims, F32)


SMEM_SPEC = pl.BlockSpec(memory_space=pltpu.SMEM)
VMEM_SPEC = pl.BlockSpec(memory_space=pltpu.VMEM)
ANY_SPEC = pl.BlockSpec(memory_space=pl.ANY)
HBM_SPEC = pl.BlockSpec(memory_space=pltpu.HBM)


def call(kernel, outs, out_specs, inputs, in_specs, scratch):
    inputs = [
        pltpu.with_memory_space_constraint(x, pltpu.HBM) if spec is HBM_SPEC else x
        for x, spec in zip(inputs, in_specs)
    ]
    outs = [
        pltpu.HBM(out.shape, out.dtype) if spec is HBM_SPEC else out
        for out, spec in zip(outs, out_specs)
    ]
    return pl.pallas_call(
        kernel,
        out_shape=outs,
        in_specs=in_specs,
        out_specs=out_specs,
        scratch_shapes=scratch,
        compiler_params=pltpu.CompilerParams(vmem_limit_bytes=20 * 1024 * 1024),
    )(*inputs)


def body(links, propagator, sink_time, src_time, src_site):
    count = lax.axis_size("space")
    times = lax.axis_size("tm")
    planes = links.shape[5]
    side = math.isqrt(links.shape[6])
    half, lanes = side // 2, 2 * side
    across = planes * count
    slots = planes + 1
    parts = count // 4
    rows = half // parts
    sites = planes * half
    split = 2 if times % 2 == 0 else 1
    per = 8 * -(-sites // (8 * split))
    pairs = propagator.shape[1]

    forward = jnp.asarray(transform_table(side, False))
    inverse = jnp.asarray(transform_table(side, True))
    table = jnp.asarray(filter_table(side, across, parts))

    def interleave(array, lead):
        return array.reshape(lead, planes, half, lanes).transpose(0, 2, 1, 3).reshape(lead, sites, lanes)

    lattice = interleave(links, 54)

    def forwarded(value, shift):
        return lax.ppermute(value, "tm", [(i, (i + shift) % times) for i in range(times)])

    def within(i, shift):
        return i - i % split + (i + shift) % split

    spectrum_shape = shape(count, slots * 2 * rows, lanes)
    transform_scratch = [
        VMEM((4 * slots * half, 2 * lanes), BF16),
        VMEM((4 * slots * half, 2 * lanes), BF16),
        VMEM((4 * slots * half, 2 * lanes), F32),
    ]
    divergence_scratch = [
        VMEM((3, 8, planes, half, lanes), F32),
        VMEM((slots, 8, half, lanes), F32),
    ]
    gauge_scratch = [
        VMEM((18, slots, half, lanes), F32),
        VMEM((18, planes, half, lanes), F32),
        VMEM((18, planes, half, lanes), F32),
    ]
    flat_scratch = [VMEM((8, per * split, lanes), F32)]
    algebra_shape = shape(8, slots, half, lanes)
    share_shapes = [shape(8, per, lanes)] * split

    def turn(spectrum):
        return lax.all_to_all(spectrum, "space", 0, 0, tiled=True)

    def convolve(spectrum):
        (out,) = call(
            functools.partial(convolve_kernel, planes),
            [spectrum_shape],
            [VMEM_SPEC],
            [spectrum, table],
            [VMEM_SPEC] * 2,
            [],
        )
        return out

    source = interleave(propagator, 2 * pairs)
    if per * split > sites:
        source = jnp.pad(source, ((0, 0), (0, per * split - sites), (0, 0)))
    scalars = jnp.concatenate([sink_time % times, src_time % times, src_site])
    spectrum, *cuts = call(
        functools.partial(start_kernel, split),
        [spectrum_shape] + [shape(2 * pairs, per, lanes)] * (split - 1),
        [VMEM_SPEC] + [HBM_SPEC] * (split - 1),
        [lattice, forward, source],
        [HBM_SPEC] * 3,
        [
            VMEM((split - 1, 2 * pairs, per, lanes), F32),
            VMEM(lattice.shape, F32),
            VMEM(forward.shape, BF16),
        ]
        + divergence_scratch
        + transform_scratch
        + [pltpu.SemaphoreType.DMA((4,)), pltpu.SemaphoreType.DMA((2, split - 1))],
    )
    sources = [
        lax.ppermute(block, "tm", [(i, within(i, shift)) for i in range(times)])
        for shift, block in enumerate(cuts, 1)
    ]
    spectrum = turn(spectrum)
    spectrum = convolve(spectrum)
    spectrum = turn(spectrum)
    spectrum, first, *early = call(
        functools.partial(middle_kernel, split),
        [spectrum_shape, algebra_shape] + share_shapes,
        [VMEM_SPEC] + [HBM_SPEC] * (1 + split),
        [spectrum, lattice, inverse, forward],
        [VMEM_SPEC] * 4,
        [VMEM(algebra_shape.shape, F32)]
        + gauge_scratch
        + divergence_scratch
        + transform_scratch
        + flat_scratch
        + [pltpu.SemaphoreType.DMA((split + 1,))],
    )
    first_shares = [forwarded(early[shift % split], shift) for shift in range(1, times)]
    spectrum = turn(spectrum)
    spectrum = convolve(spectrum)
    spectrum = turn(spectrum)
    second, *shares = call(
        last_transform_kernel,
        [algebra_shape] + share_shapes,
        [VMEM_SPEC] * (1 + split),
        [spectrum, inverse],
        [VMEM_SPEC] * 2,
        transform_scratch + flat_scratch,
    )

    def sent_from(source_index):
        def send(*blocks):
            return tuple(
                lax.ppermute(blocks[to % split], "tm", [(source_index, to)])
                for to in range(times)
                if to != source_index
            )

        return send

    second_shares = lax.switch(sink_time[0] % times, [sent_from(k) for k in range(times)], *shares)
    (fixed,) = call(
        finish_kernel,
        [shape(54, sites, lanes)],
        [HBM_SPEC],
        [lattice, first, second],
        [HBM_SPEC] * 2 + [VMEM_SPEC],
        gauge_scratch
        + [
            VMEM(lattice.shape, F32),
            VMEM(algebra_shape.shape, F32),
            VMEM(lattice.shape, F32),
            pltpu.SemaphoreType.DMA((2 + half // 8,)),
        ],
    )
    width = -(-(SC * SC + 24) // lanes)
    devices = count * times
    (payload,) = call(
        functools.partial(sink_kernel, times, split),
        [shape(devices, 2 * width, lanes)],
        [VMEM_SPEC],
        [scalars, first, second, early[0]] + first_shares + shares + list(second_shares) + [source] + sources,
        [SMEM_SPEC, HBM_SPEC] + [VMEM_SPEC] * (2 * times + split) + [HBM_SPEC] + [ANY_SPEC] * (split - 1),
        [
            VMEM((split, 2 * pairs, per, lanes), F32),
            VMEM((2, 8, per, lanes), F32),
            VMEM((18, per, lanes), F32),
            VMEM((2, SC * SC * 8, lanes), F32),
            VMEM((8, 8, lanes), F32),
            VMEM((24, lanes), F32),
            pltpu.SemaphoreType.DMA((split + 1,)),
        ],
    )
    gathered = lax.all_to_all(payload, ("space", "tm"), 0, 0, tiled=True)
    scale = float(across * side * side) ** (-0.5)
    (wall,) = call(functools.partial(wall_kernel, scale), [shape(2, SC * SC)], [VMEM_SPEC], [gathered], [VMEM_SPEC], [])
    fixed = fixed.reshape(54, half, planes, lanes).transpose(0, 2, 1, 3).reshape(links.shape)
    return fixed, wall


def solution(mesh):
    placed = (
        P("tm", None, None, None, None, "space", None),
        P(None, "tm", "space", None),
        P(),
        P(),
        P(),
    )
    return jax.shard_map(
        body,
        mesh=mesh,
        in_specs=placed,
        out_specs=(P("tm", None, None, None, None, "space", None), P()),
        check_vma=False,
    )
```

```python
import functools
import math

import jax
import jax.numpy as jnp
import numpy as np
from jax import lax
from jax.experimental import pallas as pl
from jax.experimental.pallas import tpu as pltpu
from jax.sharding import PartitionSpec as P


SC = 12
STEP_SIZE = 0.08
PEAK_SQUARE = 12.0
F32 = jnp.float32
BF16 = jnp.bfloat16
VMEM = pltpu.VMEM
PAIRS = ((0, 1), (0, 2), (1, 2))


def split_table(table):
    high = table.astype(jnp.bfloat16)
    low = (table - high.astype(np.float64)).astype(jnp.bfloat16)
    return high, low


def as_real(real, imag):
    return np.block([[real, imag], [-imag, real]])


@functools.lru_cache(None)
def transform_table(side, inverse):
    half = side // 2
    sign = 1.0 if inverse else -1.0
    k = np.arange(half)
    twist = np.exp(1j * sign * 2.0 * np.pi * k / side)
    even = np.exp(1j * sign * 2.0 * np.pi * np.outer(k, k) / half)
    odd = even * (twist[None, :] if inverse else twist[:, None])
    left = np.concatenate([as_real(m.real, -m.imag) for m in (even, odd)], axis=0)
    high, low = split_table(left)
    fill = np.zeros((left.shape[0], 4 * side - 3 * side), high.dtype)
    left = np.concatenate([high, low, high, fill], axis=1)
    z = np.arange(side)
    depth_phase = sign * 2.0 * np.pi * np.outer(z, z) / side
    parity = np.array([[1.0, 1.0], [1.0, -1.0]])
    right = as_real(np.kron(parity, np.cos(depth_phase)), np.kron(parity, np.sin(depth_phase)))
    high, low = split_table(right)
    lanes = np.arange(2 * side)
    from_depth = lanes - lanes % side + (lanes + (1 if inverse else -1)) % side
    moves = [np.eye(2 * side)[:, (lanes + side) % (2 * side)], np.eye(2 * side)[:, from_depth]]
    shift = np.concatenate(moves, axis=1)
    shift = np.concatenate([shift, shift], axis=0).astype(high.dtype)
    return np.concatenate([high, low, left, shift], axis=0)


@functools.lru_cache(None)
def filter_table(side, across, blocks):
    half = side // 2
    squares = 4.0 * np.sin(np.pi * np.arange(side) / side) ** 2
    squares_across = 4.0 * np.sin(np.pi * np.arange(across) / across) ** 2
    column = (squares[:, None] + squares[None, :]).reshape(2, half, side)
    column = np.swapaxes(column, 0, 1).reshape(half, 2 * side)
    momentum = squares_across[:, None, None] + column[None]
    weight = np.where(momentum > 0.0, PEAK_SQUARE / np.where(momentum > 0.0, momentum, 1.0), 0.0)
    offsets = np.arange(across // 2 + 1)
    phase = np.cos(2.0 * np.pi * np.outer(offsets, np.arange(across)) / across)
    table = np.einsum("dk,krl->drl", phase, weight) / (across * side * side)
    table = table * (STEP_SIZE / 16.0)
    table = table.reshape(len(offsets), blocks, half // blocks, 2 * side)
    return np.ascontiguousarray(np.swapaxes(table, 0, 1)).astype(np.float32)


def cmul(x, y):
    return x[0] * y[0] - x[1] * y[1], x[0] * y[1] + x[1] * y[0]


def csquare(x):
    return x[0] * x[0] - x[1] * x[1], 2.0 * (x[0] * x[1])


def row_times(row, matrix):
    out = []
    for b in range(3):
        re = row[0][0] * matrix[0][b][0] - row[0][1] * matrix[0][b][1]
        im = row[0][0] * matrix[0][b][1] + row[0][1] * matrix[0][b][0]
        for k in (1, 2):
            re = re + row[k][0] * matrix[k][b][0] - row[k][1] * matrix[k][b][1]
            im = im + row[k][0] * matrix[k][b][1] + row[k][1] * matrix[k][b][0]
        out.append((re, im))
    return out


def row_times_dagger(row, matrix):
    out = []
    for b in range(3):
        re = row[0][0] * matrix[b][0][0] + row[0][1] * matrix[b][0][1]
        im = row[0][1] * matrix[b][0][0] - row[0][0] * matrix[b][0][1]
        for k in (1, 2):
            re = re + row[k][0] * matrix[b][k][0] + row[k][1] * matrix[b][k][1]
            im = im + row[k][1] * matrix[b][k][0] - row[k][0] * matrix[b][k][1]
        out.append((re, im))
    return out


def exponential(x):
    t0, t1 = x[0], x[1]
    a, b, e = (x[2], x[3]), (x[4], x[5]), (x[6], x[7])
    t2 = -(t0 + t1)
    na = a[0] * a[0] + a[1] * a[1]
    nb = b[0] * b[0] + b[1] * b[1]
    ne = e[0] * e[0] + e[1] * e[1]
    s0, s1, s2 = t0 * t0, t1 * t1, t2 * t2
    ae = cmul(a, e)
    c = -(0.5 * (s0 + s1 + s2) + (na + nb + ne))
    cross = ae[1] * b[0] - ae[0] * b[1]
    d = t0 * ne + t1 * nb + t2 * na - t0 * t1 * t2 - 2.0 * cross
    c30 = c * (1.0 / 30.0)
    q0 = (None, d * (1.0 / 120.0))
    q1 = ((1.0 + c30) * 0.25, None)
    q2r = 1.0 / 20.0
    n0i = d * (q2r / 3.0)
    n1 = ((1.0 + c * q2r) * (1.0 / 3.0), q0[1] * (1.0 / 3.0))
    n2r = q1[0] * (1.0 / 3.0)
    m0 = (None, d * (0.5 * n2r))
    m1 = (0.5 + 0.5 * (c * n2r), 0.5 * n0i)
    m2 = (0.5 * n1[0], 0.5 * n1[1])
    q0 = (1.0 - d * m2[1], d * m2[0])
    q1 = (1.0 + c * m2[0], m0[1] + c * m2[1])
    q2 = m1
    for _ in range(3):
        q12 = cmul(q1, q2)
        q22 = csquare(q2)
        q00 = csquare(q0)
        q11 = csquare(q1)
        q01 = cmul(q0, q1)
        q02 = cmul(q0, q2)
        d2 = 2.0 * d
        q0 = (q00[0] - d2 * q12[1], q00[1] + d2 * q12[0])
        q1 = (
            2.0 * (q01[0] + c * q12[0]) - d * q22[1],
            2.0 * (q01[1] + c * q12[1]) + d * q22[0],
        )
        q2 = (q11[0] + 2.0 * q02[0] + c * q22[0], q11[1] + 2.0 * q02[1] + c * q22[1])
    u, v = q1
    s, t = q2
    result = [[None] * 3 for _ in range(3)]
    for at, (theta, m) in enumerate(
        ((t0, -(s0 + na + nb)), (t1, -(s1 + na + ne)), (t2, -(s2 + nb + ne)))
    ):
        result[at][at] = (q0[0] - v * theta + s * m, q0[1] + u * theta + t * m)
    y01 = (t2 * a[1] - (b[0] * e[0] + b[1] * e[1]), -t2 * a[0] - (b[1] * e[0] - b[0] * e[1]))
    y02 = (t1 * b[1] + ae[0], -t1 * b[0] + ae[1])
    y12 = (t0 * e[1] - (a[0] * b[0] + a[1] * b[1]), -t0 * e[0] - (a[0] * b[1] - a[1] * b[0]))
    for (i, j), xx, yy in zip(PAIRS, (a, b, e), (y01, y02, y12)):
        ur, vi, ui, vr = u * xx[0], v * xx[1], u * xx[1], v * xx[0]
        sr, ti, si, tr = s * yy[0], t * yy[1], s * yy[1], t * yy[0]
        result[i][j] = ((ur - vi) + (sr - ti), (ui + vr) + (si + tr))
        result[j][i] = ((sr + ti) - (ur + vi), (tr - si) + (ui - vr))
    return result


def project(rows):
    third = (rows[0][0][1] + rows[1][1][1] + rows[2][2][1]) * (1.0 / 3.0)
    out = [rows[0][0][1] - third, rows[1][1][1] - third]
    for i, j in PAIRS:
        out.append(0.5 * (rows[i][j][0] - rows[j][i][0]))
        out.append(0.5 * (rows[i][j][1] + rows[j][i][1]))
    return out


def lane_of(shape):
    return lax.broadcasted_iota(jnp.int32, shape, 1)


def halves(x):
    high = x.astype(BF16)
    low = (x - high.astype(F32)).astype(BF16)
    return high, low


def dot(x, y):
    return jnp.dot(x, y, preferred_element_type=F32)


def pick_ahead(swapped):
    half = swapped.shape[1] // 2
    return jnp.where(
        lane_of(swapped.shape) < half, swapped, pltpu.roll(swapped, swapped.shape[0] - 1, axis=0)
    )


def pick_behind(swapped):
    half = swapped.shape[1] // 2
    return jnp.where(lane_of(swapped.shape) >= half, swapped, pltpu.roll(swapped, 1, axis=0))


def left_transform(stacked, table_ref):
    high, low = halves(stacked)
    depth, width = stacked.shape
    at = 2 * table_ref.shape[1]
    both = dot(
        table_ref[at : at + 2 * depth, : 3 * depth], jnp.concatenate([high, high, low], axis=0)
    )
    even = lane_of((depth, width)) % (2 * depth) < depth
    return jnp.where(even, both[:depth], both[depth:])


def right_transform(high_ref, low_ref, table_ref, out_ref):
    size = table_ref.shape[1]
    high = high_ref[...]
    first = table_ref[:size]
    out_ref[...] = dot(high, first) + dot(low_ref[...], first) + dot(high, table_ref[size : 2 * size])


def forward_transform(d_ref, table_ref, high_ref, low_ref, spec_ref, out_ref):
    slots, _, half, lanes = d_ref.shape
    parts = out_ref.shape[0] // 4
    rows = half // parts
    for slot in range(slots):
        stacked = jnp.concatenate(
            [
                jnp.concatenate([d_ref[slot, 2 * f], d_ref[slot, 2 * f + 1]], axis=0)
                for f in range(4)
            ],
            axis=1,
        )
        y = left_transform(stacked, table_ref)
        for f in range(4):
            re = y[:half, f * lanes : (f + 1) * lanes]
            im = y[half:, f * lanes : (f + 1) * lanes]
            high, low = halves(jnp.concatenate([re, im], axis=1))
            at = (slot * 4 + f) * half
            high_ref[at : at + half, :] = high
            low_ref[at : at + half, :] = low
    right_transform(high_ref, low_ref, table_ref, spec_ref)
    for slot in range(slots):
        for f in range(4):
            for part in range(parts):
                at = (slot * 4 + f) * half + part * rows
                for c in range(2):
                    to = (slot * 2 + c) * rows
                    out_ref[f * parts + part, to : to + rows, :] = spec_ref[
                        at : at + rows, c * lanes : (c + 1) * lanes
                    ]


def inverse_transform(in_ref, table_ref, high_ref, low_ref, spec_ref, x_ref):
    _, slots, half, lanes = x_ref.shape
    parts = in_ref.shape[0] // 4
    rows = half // parts
    for slot in range(slots):
        for f in range(4):
            columns = []
            for c in range(2):
                to = (slot * 2 + c) * rows
                pieces = [in_ref[f * parts + part, to : to + rows, :] for part in range(parts)]
                columns.append(jnp.concatenate(pieces, axis=0))
            high, low = halves(jnp.concatenate(columns, axis=1))
            at = (slot * 4 + f) * half
            high_ref[at : at + half, :] = high
            low_ref[at : at + half, :] = low
    right_transform(high_ref, low_ref, table_ref, spec_ref)
    for slot in range(slots):
        stacks = []
        for f in range(4):
            at = (slot * 4 + f) * half
            stacks.append(
                jnp.concatenate([spec_ref[at : at + half, :lanes], spec_ref[at : at + half, lanes:]], axis=0)
            )
        y = left_transform(jnp.concatenate(stacks, axis=1), table_ref)
        for f in range(4):
            x_ref[2 * f, slot] = y[:half, f * lanes : (f + 1) * lanes]
            x_ref[2 * f + 1, slot] = y[half:, f * lanes : (f + 1) * lanes]


def site_rows(plane, chunk, planes):
    return pl.ds(chunk * (8 * planes) + plane, 8, stride=planes)


def load_link(links_ref, direction, rows):
    base = direction * 18
    return [
        [(links_ref[base + 3 * i + j, rows, :], links_ref[base + 9 + 3 * i + j, rows, :]) for j in range(3)]
        for i in range(3)
    ]


def load_gauge(ref, plane, rows):
    return [
        [(ref[3 * i + j, plane, rows, :], ref[9 + 3 * i + j, plane, rows, :]) for j in range(3)]
        for i in range(3)
    ]


def store_gauge(ref, plane, rows, matrix):
    for i in range(3):
        for j in range(3):
            ref[3 * i + j, plane, rows, :] = matrix[i][j][0]
            ref[9 + 3 * i + j, plane, rows, :] = matrix[i][j][1]


def chunk_loop(planes, chunks, step):
    def run(index, carry):
        step(index // chunks, index % chunks)
        return carry

    lax.fori_loop(0, planes * chunks, run, 0)


def aligned(chunk):
    return pl.ds(pl.multiple_of(chunk * 8, 8), 8)


def shift_gauge(g_ref, shift, stack_ref, moved_ref, y_ref):
    planes, half, lanes = y_ref.shape[1:]
    for comp in range(18):
        for plane in range(planes):
            at = (comp * planes + plane) * half
            stack_ref[at : at + half, :] = jnp.concatenate(halves(g_ref[comp, plane]), axis=1)
    moved_ref[...] = dot(stack_ref[...], shift)
    for comp in range(18):
        for plane in range(planes):
            at = (comp * planes + plane) * half
            y_ref[comp, plane] = pick_ahead(moved_ref[at : at + half, :lanes])


def load_ahead(direction, g_ref, y_ref, moved_ref, plane, chunk):
    rows = aligned(chunk)
    if direction == 0:
        return load_gauge(g_ref, plane + 1, rows)
    if direction == 1:
        return load_gauge(y_ref, plane, rows)
    planes, half, lanes = y_ref.shape[1:]

    def at(comp):
        return moved_ref[pl.ds(pl.multiple_of((comp * planes + plane) * half + chunk * 8, 8), 8), lanes:]

    return [[(at(3 * i + j), at(9 + 3 * i + j)) for j in range(3)] for i in range(3)]


def divergence(v_ref, shift_ref, stack_ref, moved_ref, d_ref):
    _, comps, planes, half, lanes = v_ref.shape
    size = comps * planes * half
    for direction in (1, 2):
        for comp in range(comps):
            for plane in range(planes):
                at = (direction - 1) * size + (comp * planes + plane) * half
                stack_ref[at : at + half, :] = jnp.concatenate(
                    halves(v_ref[direction, comp, plane]), axis=1
                )
    first = shift_ref.shape[0] - 2 * lanes
    moved_ref[:size, :lanes] = dot(stack_ref[:size], shift_ref[first:, :lanes])
    moved_ref[size : 2 * size, :lanes] = dot(stack_ref[size : 2 * size], shift_ref[first:, lanes:])
    for comp in range(comps):
        before = None
        for plane in range(planes):
            at = (comp * planes + plane) * half
            vx = v_ref[0, comp, plane]
            total = (pick_behind(moved_ref[at : at + half, :lanes]) - v_ref[1, comp, plane]) + (
                moved_ref[size + at : size + at + half, :lanes] - v_ref[2, comp, plane]
            )
            total = total - vx
            if before is not None:
                total = total + before
            before = vx
            d_ref[plane, comp] = total
        d_ref[planes, comp] = before


def cut_kernel(split, source_any, *rest):
    cut_refs = rest[: split - 1]
    held_ref, sems = rest[split - 1 :]
    per = held_ref.shape[2]
    reads, writes = [], []
    for shift, cut in enumerate(cut_refs, 1):
        rows = pl.ds(share_start(shift, split, per), per)
        reads.append(
            pltpu.make_async_copy(source_any.at[:, rows, :], held_ref.at[shift - 1], sems.at[0, shift - 1])
        )
        writes.append(pltpu.make_async_copy(held_ref.at[shift - 1], cut, sems.at[1, shift - 1]))
    for copy in reads:
        copy.start()
    for read, write in zip(reads, writes):
        read.wait()
        write.start()
    for write in writes:
        write.wait()


def start_kernel(links_any, table_any, out_ref, links_ref, table_ref, v_ref, d_ref, stack_ref, moved_ref, high_ref, low_ref, spec_ref, sems):
    _, _, planes, half, _ = v_ref.shape
    copies = [
        pltpu.make_async_copy(
            links_any.at[pl.ds(18 * direction, 18)], links_ref.at[pl.ds(18 * direction, 18)], sems.at[direction]
        )
        for direction in range(3)
    ]
    copies.append(pltpu.make_async_copy(table_any, table_ref, sems.at[3]))
    for copy in copies:
        copy.start()
    for direction in range(3):
        copies[direction].wait()

        def step(plane, chunk, direction=direction):
            rows = site_rows(plane, chunk, planes)
            for comp, value in enumerate(project(load_link(links_ref, direction, rows))):
                v_ref[direction, comp, plane, aligned(chunk), :] = value

        chunk_loop(planes, half // 8, step)
    copies[3].wait()
    divergence(v_ref, table_ref, stack_ref, moved_ref, d_ref)
    forward_transform(d_ref, table_ref, high_ref, low_ref, spec_ref, out_ref)


def convolve_kernel(planes, in_ref, table_ref, out_ref):
    count = in_ref.shape[0]
    parts, offsets, rows, _ = table_ref.shape
    across = planes * count
    part = lax.axis_index("space") % parts
    step = min(8, rows)

    def run(index, carry):
        c = index // (rows // step)
        chunk = index % (rows // step)

        def at(slot):
            return pl.ds((slot * 2 + c) * rows + chunk * step, step)

        table = [table_ref[part, k, pl.ds(chunk * step, step), :] for k in range(offsets)]
        data = []
        for x in range(across):
            owner, plane = divmod(x, planes)
            value = in_ref[owner, at(plane), :]
            if plane == 0:
                value = value + in_ref[(owner - 1) % count, at(planes), :]
            data.append(value)
        for x in range(across):
            owner, plane = divmod(x, planes)
            total = table[0] * data[x] + table[offsets - 1] * data[(x + across // 2) % across]
            for k in range(1, offsets - 1):
                total = total + table[k] * (data[(x + k) % across] + data[(x - k) % across])
            out_ref[owner, at(plane), :] = total
            if plane == 0:
                out_ref[(owner - 1) % count, at(planes), :] = total
        return carry

    lax.fori_loop(0, 2 * (rows // step), run, 0)


def flatten_shares(x_ref, flat_ref, planes):
    half = x_ref.shape[2]
    if flat_ref.shape[1] > planes * half:
        flat_ref[...] = jnp.zeros_like(flat_ref)
    for comp in range(8):
        for plane in range(planes):
            flat_ref[comp, pl.ds(plane, half, stride=planes), :] = x_ref[comp, plane]


def share_start(shift, count, per):
    return pl.multiple_of((lax.axis_index("tm") + shift) % count * per, 8)


def middle_kernel(shares, in_ref, links_ref, inverse_ref, forward_ref, *rest):
    out_ref, x_any = rest[:2]
    share_refs = rest[2 : 2 + shares]
    x_ref, g_ref, y_ref, v_ref, d_ref, stack_ref, moved_ref, high_ref, low_ref, spec_ref, flat_ref, sems = rest[2 + shares :]
    _, slots, half, _ = x_ref.shape
    planes = slots - 1
    per = share_refs[0].shape[1]
    inverse_transform(in_ref, inverse_ref, high_ref, low_ref, spec_ref, x_ref)
    flatten_shares(x_ref, flat_ref, planes)
    copies = [
        pltpu.make_async_copy(
            flat_ref.at[:, pl.ds(share_start(shift, shares, per), per), :], share_refs[shift], sems.at[shift]
        )
        for shift in range(shares)
    ]
    copies.append(pltpu.make_async_copy(x_ref, x_any, sems.at[shares]))
    for copy in copies:
        copy.start()

    def raise_step(plane, chunk):
        rows = aligned(chunk)
        store_gauge(g_ref, plane, rows, exponential([x_ref[k, plane, rows, :] for k in range(8)]))

    chunk_loop(slots, half // 8, raise_step)
    lanes = x_ref.shape[3]
    shift_gauge(g_ref, inverse_ref[inverse_ref.shape[0] - 2 * lanes :], stack_ref, moved_ref, y_ref)

    def rotate_step(plane, chunk):
        rows = aligned(chunk)
        gauge = load_gauge(g_ref, plane, rows)
        link_rows = site_rows(plane, chunk, planes)
        for direction in range(3):
            link = load_link(links_ref, direction, link_rows)
            ahead = load_ahead(direction, g_ref, y_ref, moved_ref, plane, chunk)
            turned = [row_times_dagger(row_times(gauge[i], link), ahead) for i in range(3)]
            for comp, value in enumerate(project(turned)):
                v_ref[direction, comp, plane, rows, :] = value

    chunk_loop(planes, half // 8, rotate_step)
    divergence(v_ref, forward_ref, stack_ref, moved_ref, d_ref)
    forward_transform(d_ref, forward_ref, high_ref, low_ref, spec_ref, out_ref)
    for copy in copies:
        copy.wait()


def last_transform_kernel(in_ref, inverse_ref, x_ref, *rest):
    share_refs = rest[:-5]
    high_ref, low_ref, spec_ref, flat_ref, sems = rest[-5:]
    per = share_refs[0].shape[1]
    inverse_transform(in_ref, inverse_ref, high_ref, low_ref, spec_ref, x_ref)
    flatten_shares(x_ref, flat_ref, x_ref.shape[1] - 1)
    copies = [
        pltpu.make_async_copy(flat_ref.at[:, to * per : (to + 1) * per, :], share_ref, sems.at[to])
        for to, share_ref in enumerate(share_refs)
    ]
    for copy in copies:
        copy.start()
    for copy in copies:
        copy.wait()


def total_of(first, second):
    earlier = exponential(first)
    later = exponential(second)
    return [row_times(later[i], earlier) for i in range(3)]


def finish_kernel(links_any, first_any, table_any, second_ref, out_any, g_ref, y_ref, stack_ref, moved_ref, links_ref, first_ref, shift_ref, out_ref, sems):
    _, slots, half, lanes = first_ref.shape
    planes = slots - 1
    chunks = half // 8
    copies = [
        pltpu.make_async_copy(first_any, first_ref, sems.at[0]),
        pltpu.make_async_copy(links_any, links_ref, sems.at[1]),
        pltpu.make_async_copy(
            table_any.at[pl.ds(table_any.shape[0] - 2 * lanes, 2 * lanes)], shift_ref, sems.at[2]
        ),
    ]
    for copy in copies:
        copy.start()
    copies[0].wait()

    def raise_step(plane, chunk):
        rows = aligned(chunk)
        store_gauge(
            g_ref,
            plane,
            rows,
            total_of(
                [first_ref[k, plane, rows, :] for k in range(8)],
                [second_ref[k, plane, rows, :] for k in range(8)],
            ),
        )

    chunk_loop(slots, half // 8, raise_step)
    copies[2].wait()
    shift_gauge(g_ref, shift_ref[...], stack_ref, moved_ref, y_ref)
    copies[1].wait()

    def piece(chunk):
        rows = pl.ds(pl.multiple_of(chunk * (8 * planes), 8), 8 * planes)
        return pltpu.make_async_copy(out_ref.at[:, rows, :], out_any.at[:, rows, :], sems.at[3 + chunk])

    def rotate_step(chunk, plane):
        rows = aligned(chunk)
        gauge = load_gauge(g_ref, plane, rows)
        link_rows = site_rows(plane, chunk, planes)
        for direction in range(3):
            link = load_link(links_ref, direction, link_rows)
            ahead = load_ahead(direction, g_ref, y_ref, moved_ref, plane, chunk)
            for i in range(3):
                row = row_times_dagger(row_times(gauge[i], link), ahead)
                for j in range(3):
                    out_ref[direction * 18 + 3 * i + j, link_rows, :] = row[j][0]
                    out_ref[direction * 18 + 9 + 3 * i + j, link_rows, :] = row[j][1]

        @pl.when(plane == planes - 1)
        def _():
            piece(chunk).start()

    chunk_loop(chunks, planes, rotate_step)

    for chunk in range(chunks):
        piece(chunk).wait()


def lane_sums(rows):
    ones = jnp.ones((8, rows.shape[1]), BF16)
    total = None
    rest = rows
    for _ in range(3):
        piece = rest.astype(BF16)
        rest = rest - piece.astype(F32)
        part = lax.dot_general(ones, piece, (((1,), (1,)), ((), ())), preferred_element_type=F32)
        total = part if total is None else total + part
    return total


def sink_kernel(times, split, sink_ref, src_time_ref, src_site_ref, first_any, second_ref, source_ref, own_early_any, *rest):
    early = (own_early_any,) + rest[: times - 1]
    own = rest[times - 1 : times - 1 + split]
    late = rest[times - 1 + split : 2 * times - 2 + split]
    partners_any = rest[2 * times - 2 + split : 2 * times - 3 + 2 * split]
    out_ref, partner_ref, x_ref, gauge_ref, sum_ref, before_ref, anchor_ref, sems = rest[2 * times - 3 + 2 * split :]
    per = early[0].shape[1]
    pairs = source_ref.shape[0] // 2
    groups = pairs // 3
    _, slots, half, lanes = second_ref.shape
    planes = slots - 1
    mine = lax.axis_index("tm")
    sink = sink_ref[0]
    column = src_site_ref[0] % (half * lanes)
    plane = src_site_ref[0] // (half * lanes) - lax.axis_index("space") * planes
    present = (src_time_ref[0] == mine) & (plane >= 0) & (plane < planes)
    safe = jnp.clip(plane, 0, planes - 1)
    row = column // lanes
    block = pl.ds(pl.multiple_of(row // 8 * 8, 8), 8)
    before = pltpu.make_async_copy(first_any.at[:, safe, block, :], before_ref, sems.at[0])
    fetches = [pltpu.make_async_copy(early[0], x_ref.at[k], sems.at[1 + k]) for k in range(2)]
    partners = [
        pltpu.make_async_copy(partner, partner_ref.at[k], sems.at[3 + k])
        for k, partner in enumerate(partners_any)
    ]

    def fetch(condition, value, to):
        @pl.when(condition)
        def _():
            pltpu.make_async_copy(value, x_ref.at[to], sems.at[1 + to]).start()

    for shift in range(times):
        fetch((mine - sink) % times == shift, early[shift], 0)
    for at in range(split):
        fetch((mine == sink) & (mine % split == at), own[at], 1)
    for at in range(times - 1):
        fetch((mine != sink) & (jnp.where(mine > sink, mine - 1, mine) == at), late[at], 1)
    for copy in partners:
        copy.start()
    before.start()
    sum_ref[...] = jnp.zeros_like(sum_ref)
    for copy in fetches:
        copy.wait()
    chunks = per // 8
    for chunk in range(chunks):
        rows = slice(chunk * 8, chunk * 8 + 8)
        gauge = total_of([x_ref[0, k, rows, :] for k in range(8)], [x_ref[1, k, rows, :] for k in range(8)])
        for i in range(3):
            for j in range(3):
                gauge_ref[3 * i + j, rows, :] = gauge[i][j][0]
                gauge_ref[9 + 3 * i + j, rows, :] = gauge[i][j][1]
    for shift in range(split):
        if shift:
            partners[shift - 1].wait()
        block_ref = partner_ref.at[shift - 1] if shift else source_ref
        offset = 0 if shift else share_start(0, split, per)
        base = (mine - mine % split + (mine - shift) % split) * pairs

        def run(group, carry, block_ref=block_ref, offset=offset, base=base):
            sums = [None] * 3
            for chunk in range(chunks):
                rows = slice(chunk * 8, chunk * 8 + 8)
                own_rows = pl.ds(pl.multiple_of(offset + chunk * 8, 8), 8)
                column = [
                    (block_ref[3 * group + c, own_rows, :], block_ref[pairs + 3 * group + c, own_rows, :])
                    for c in range(3)
                ]
                for a in range(3):
                    for c in range(3):
                        part = cmul(
                            (gauge_ref[3 * a + c, rows, :], gauge_ref[9 + 3 * a + c, rows, :]), column[c]
                        )
                        sums[a] = part if sums[a] is None else (sums[a][0] + part[0], sums[a][1] + part[1])
            for a in range(3):
                to = pl.ds(pl.multiple_of((base + 3 * group + a) * 8, 8), 8)
                sum_ref[0, to, :] = sums[a][0]
                sum_ref[1, to, :] = sums[a][1]
            return carry

        lax.fori_loop(0, groups, run, 0, unroll=2 if groups % 2 == 0 else 1)
    before.wait()
    total = total_of([before_ref[k] for k in range(8)], [second_ref[k, safe, block, :] for k in range(8)])
    wide = (8, lanes)
    keep = (lane_of(wide) == jnp.where(present, column % lanes, -1)) & (
        lax.broadcasted_iota(jnp.int32, wide, 0) == row % 8
    )
    anchor_ref[...] = jnp.zeros_like(anchor_ref)
    for k in range(18):
        value = total[k % 9 // 3][k % 3][k // 9]
        anchor_ref[k : k + 1, :] = jnp.sum(jnp.where(keep, value, 0.0), axis=0, keepdims=True)
    whole = SC * SC
    width = -(-(whole + 24) // lanes) * lanes
    pieces = []
    for part in range(2):
        total = sum_ref[part, pl.ds(0, whole, stride=8), :]
        for k in range(1, 8):
            total = total + sum_ref[part, pl.ds(k, whole, stride=8), :]
        extra = anchor_ref[...] if part == 0 else jnp.zeros((24, lanes), F32)
        pieces += [total, extra, jnp.zeros((width - whole - 24, lanes), F32)]
    sums = lane_sums(jnp.concatenate(pieces, axis=0))
    block = jnp.concatenate(
        [sums[0:1, k * lanes : (k + 1) * lanes] for k in range(2 * width // lanes)], axis=0
    )

    def spread(index, carry):
        out_ref[index] = block
        return carry

    lax.fori_loop(0, out_ref.shape[0], spread, 0)


def wall_kernel(scale, in_ref, out_ref):
    whole = SC * SC
    total = jnp.sum(in_ref[...], axis=0)
    half = total.shape[0] // 2
    re = jnp.concatenate([total[k : k + 1] for k in range(half)], axis=1)
    im = jnp.concatenate([total[half + k : half + k + 1] for k in range(half)], axis=1)
    width = re.shape[1]
    colour = lane_of((1, width)) // SC % 3
    out_re = jnp.zeros((1, width), F32)
    out_im = jnp.zeros((1, width), F32)
    for b in range(3):
        for c in range(3):
            at = whole + 3 * b + c
            ar = re[:, at : at + 1]
            ai = re[:, at + 9 : at + 10]
            amount = (SC * (b - c)) % width
            wr = pltpu.roll(re, amount, axis=1) if amount else re
            wi = pltpu.roll(im, amount, axis=1) if amount else im
            here = colour == b
            out_re = out_re + jnp.where(here, wr * ar + wi * ai, 0.0)
            out_im = out_im + jnp.where(here, wi * ar - wr * ai, 0.0)
    out_ref[0:1, :] = out_re[:, :whole] * scale
    out_ref[1:2, :] = out_im[:, :whole] * scale


def shape(*dims):
    return jax.ShapeDtypeStruct(dims, F32)


SMEM_SPEC = pl.BlockSpec(memory_space=pltpu.SMEM)
VMEM_SPEC = pl.BlockSpec(memory_space=pltpu.VMEM)
ANY_SPEC = pl.BlockSpec(memory_space=pl.ANY)
HBM_SPEC = pl.BlockSpec(memory_space=pltpu.HBM)


def call(kernel, outs, out_specs, inputs, in_specs, scratch):
    inputs = [
        pltpu.with_memory_space_constraint(x, pltpu.HBM) if spec is HBM_SPEC else x
        for x, spec in zip(inputs, in_specs)
    ]
    outs = [
        pltpu.HBM(out.shape, out.dtype) if spec is HBM_SPEC else out
        for out, spec in zip(outs, out_specs)
    ]
    return pl.pallas_call(
        kernel,
        out_shape=outs,
        in_specs=in_specs,
        out_specs=out_specs,
        scratch_shapes=scratch,
        compiler_params=pltpu.CompilerParams(vmem_limit_bytes=20 * 1024 * 1024),
    )(*inputs)


def body(links, propagator, sink_time, src_time, src_site):
    count = lax.axis_size("space")
    times = lax.axis_size("tm")
    planes = links.shape[5]
    side = math.isqrt(links.shape[6])
    half, lanes = side // 2, 2 * side
    across = planes * count
    slots = planes + 1
    parts = count // 4
    rows = half // parts
    sites = planes * half
    split = 2 if times % 2 == 0 else 1
    per = 8 * -(-sites // (8 * split))
    pairs = propagator.shape[1]

    forward = jnp.asarray(transform_table(side, False))
    inverse = jnp.asarray(transform_table(side, True))
    table = jnp.asarray(filter_table(side, across, parts))

    def interleave(array, lead):
        return array.reshape(lead, planes, half, lanes).transpose(0, 2, 1, 3).reshape(lead, sites, lanes)

    lattice = interleave(links, 54)

    def forwarded(value, shift):
        return lax.ppermute(value, "tm", [(i, (i + shift) % times) for i in range(times)])

    def within(i, shift):
        return i - i % split + (i + shift) % split

    spectrum_shape = shape(count, slots * 2 * rows, lanes)
    transform_scratch = [
        VMEM((4 * slots * half, 2 * lanes), BF16),
        VMEM((4 * slots * half, 2 * lanes), BF16),
        VMEM((4 * slots * half, 2 * lanes), F32),
    ]
    divergence_scratch = [
        VMEM((3, 8, planes, half, lanes), F32),
        VMEM((slots, 8, half, lanes), F32),
    ]
    gauge_scratch = [
        VMEM((18, slots, half, lanes), F32),
        VMEM((18, planes, half, lanes), F32),
    ]
    shift_scratch = [
        VMEM((18 * planes * half, 2 * lanes), BF16),
        VMEM((18 * planes * half, 2 * lanes), F32),
    ]
    flat_scratch = [VMEM((8, per * split, lanes), F32)]
    algebra_shape = shape(8, slots, half, lanes)
    share_shapes = [shape(8, per, lanes)] * split

    def turn(spectrum):
        return lax.all_to_all(spectrum, "space", 0, 0, tiled=True)

    def convolve(spectrum):
        (out,) = call(
            functools.partial(convolve_kernel, planes),
            [spectrum_shape],
            [VMEM_SPEC],
            [spectrum, table],
            [VMEM_SPEC] * 2,
            [],
        )
        return out

    source = interleave(propagator, 2 * pairs)
    if per * split > sites:
        source = jnp.pad(source, ((0, 0), (0, per * split - sites), (0, 0)))
    scalars = [sink_time % times, src_time % times, jnp.maximum(src_site, 0)]
    (spectrum,) = call(
        start_kernel,
        [spectrum_shape],
        [VMEM_SPEC],
        [lattice, forward],
        [HBM_SPEC] * 2,
        [VMEM(lattice.shape, F32), VMEM(forward.shape, BF16)]
        + divergence_scratch
        + shift_scratch
        + transform_scratch
        + [pltpu.SemaphoreType.DMA((4,))],
    )
    spectrum, uncut = lax.optimization_barrier((spectrum, source))
    cuts = call(
        functools.partial(cut_kernel, split),
        [shape(2 * pairs, per, lanes)] * (split - 1),
        [HBM_SPEC] * (split - 1),
        [uncut],
        [HBM_SPEC],
        [VMEM((split - 1, 2 * pairs, per, lanes), F32), pltpu.SemaphoreType.DMA((2, split - 1))],
    )
    sources = [
        lax.ppermute(block, "tm", [(i, within(i, shift)) for i in range(times)])
        for shift, block in enumerate(cuts, 1)
    ]
    spectrum = turn(spectrum)
    spectrum = convolve(spectrum)
    spectrum = turn(spectrum)
    spectrum, first, *early = call(
        functools.partial(middle_kernel, split),
        [spectrum_shape, algebra_shape] + share_shapes,
        [VMEM_SPEC] + [HBM_SPEC] * (1 + split),
        [spectrum, lattice, inverse, forward],
        [VMEM_SPEC] * 4,
        [VMEM(algebra_shape.shape, F32)]
        + gauge_scratch
        + divergence_scratch
        + shift_scratch
        + transform_scratch
        + flat_scratch
        + [pltpu.SemaphoreType.DMA((split + 1,))],
    )
    first_shares = [forwarded(early[shift % split], shift) for shift in range(1, times)]
    spectrum = turn(spectrum)
    spectrum = convolve(spectrum)
    spectrum = turn(spectrum)
    second, *shares = call(
        last_transform_kernel,
        [algebra_shape] + share_shapes,
        [VMEM_SPEC] + [HBM_SPEC] * split,
        [spectrum, inverse],
        [VMEM_SPEC] * 2,
        transform_scratch + flat_scratch + [pltpu.SemaphoreType.DMA((split,))],
    )

    def sent_from(source_index):
        def send(*blocks):
            return tuple(
                lax.ppermute(blocks[to % split], "tm", [(source_index, to)])
                for to in range(times)
                if to != source_index
            )

        return send

    second_shares = lax.switch(sink_time[0] % times, [sent_from(k) for k in range(times)], *shares)
    (fixed,) = call(
        finish_kernel,
        [shape(54, sites, lanes)],
        [HBM_SPEC],
        [lattice, first, inverse, second],
        [HBM_SPEC] * 3 + [VMEM_SPEC],
        gauge_scratch
        + shift_scratch
        + [
            VMEM(lattice.shape, F32),
            VMEM(algebra_shape.shape, F32),
            VMEM((2 * lanes, 2 * lanes), BF16),
            VMEM(lattice.shape, F32),
            pltpu.SemaphoreType.DMA((3 + half // 8,)),
        ],
    )
    width = -(-(SC * SC + 24) // lanes)
    devices = count * times
    (payload,) = call(
        functools.partial(sink_kernel, times, split),
        [shape(devices, 2 * width, lanes)],
        [VMEM_SPEC],
        scalars + [first, second, source, early[0]] + first_shares + shares + list(second_shares) + sources,
        [SMEM_SPEC] * 3
        + [HBM_SPEC]
        + [VMEM_SPEC] * 2
        + [HBM_SPEC]
        + [ANY_SPEC] * (times - 1)
        + [HBM_SPEC] * (times - 2 + 2 * split),
        [
            VMEM((max(1, split - 1), 2 * pairs, per, lanes), F32),
            VMEM((2, 8, per, lanes), F32),
            VMEM((18, per, lanes), F32),
            VMEM((2, SC * SC * 8, lanes), F32),
            VMEM((8, 8, lanes), F32),
            VMEM((24, lanes), F32),
            pltpu.SemaphoreType.DMA((2 + split,)),
        ],
    )
    gathered = lax.all_to_all(payload, ("space", "tm"), 0, 0, tiled=True)
    scale = float(across * side * side) ** (-0.5)
    (wall,) = call(functools.partial(wall_kernel, scale), [shape(2, SC * SC)], [VMEM_SPEC], [gathered], [VMEM_SPEC], [])
    fixed = fixed.reshape(54, half, planes, lanes).transpose(0, 2, 1, 3).reshape(links.shape)
    return fixed, wall


def solution(mesh):
    placed = (
        P("tm", None, None, None, None, "space", None),
        P(None, "tm", "space", None),
        P(),
        P(),
        P(),
    )
    return jax.shard_map(
        body,
        mesh=mesh,
        in_specs=placed,
        out_specs=(P("tm", None, None, None, None, "space", None), P()),
        check_vma=False,
    )
```

```python
import functools
import math
from typing import NamedTuple

import jax
import jax.numpy as jnp
import numpy as np
from jax import lax
from jax.experimental import pallas as pl
from jax.experimental.pallas import tpu as pltpu
from jax.sharding import PartitionSpec as P


SC = 12
STEP_SIZE = 0.08
PEAK_SQUARE = 12.0
F32 = jnp.float32
BF16 = jnp.bfloat16
VMEM = pltpu.VMEM
PAIRS = ((0, 1), (0, 2), (1, 2))


def split_table(table):
    high = table.astype(jnp.bfloat16)
    low = (table - high.astype(np.float64)).astype(jnp.bfloat16)
    return high, low


def as_real(real, imag):
    return np.block([[real, imag], [-imag, real]])


@functools.lru_cache(None)
def transform_table(side, inverse):
    half = side // 2
    sign = 1.0 if inverse else -1.0
    k = np.arange(half)
    twist = np.exp(1j * sign * 2.0 * np.pi * k / side)
    even = np.exp(1j * sign * 2.0 * np.pi * np.outer(k, k) / half)
    odd = even * (twist[None, :] if inverse else twist[:, None])
    left = np.concatenate([as_real(m.real, -m.imag) for m in (even, odd)], axis=0)
    high, low = split_table(left)
    fill = np.zeros((left.shape[0], 4 * side - 3 * side), high.dtype)
    left = np.concatenate([high, low, high, fill], axis=1)
    z = np.arange(side)
    depth_phase = sign * 2.0 * np.pi * np.outer(z, z) / side
    parity = np.array([[1.0, 1.0], [1.0, -1.0]])
    right = as_real(np.kron(parity, np.cos(depth_phase)), np.kron(parity, np.sin(depth_phase)))
    high, low = split_table(right)
    lanes = np.arange(2 * side)
    from_depth = lanes - lanes % side + (lanes + (1 if inverse else -1)) % side
    moves = [np.eye(2 * side)[:, (lanes + side) % (2 * side)], np.eye(2 * side)[:, from_depth]]
    shift = np.concatenate(moves, axis=1)
    shift = np.concatenate([shift, shift], axis=0).astype(high.dtype)
    return np.concatenate([high, low, left, shift], axis=0)


@functools.lru_cache(None)
def filter_table(side, across, blocks):
    half = side // 2
    squares = 4.0 * np.sin(np.pi * np.arange(side) / side) ** 2
    squares_across = 4.0 * np.sin(np.pi * np.arange(across) / across) ** 2
    column = (squares[:, None] + squares[None, :]).reshape(2, half, side)
    column = np.swapaxes(column, 0, 1).reshape(half, 2 * side)
    momentum = squares_across[:, None, None] + column[None]
    weight = np.where(momentum > 0.0, PEAK_SQUARE / np.where(momentum > 0.0, momentum, 1.0), 0.0)
    offsets = np.arange(across // 2 + 1)
    phase = np.cos(2.0 * np.pi * np.outer(offsets, np.arange(across)) / across)
    table = np.einsum("dk,krl->drl", phase, weight) / (across * side * side)
    table = table * (STEP_SIZE / 16.0)
    table = table.reshape(len(offsets), blocks, half // blocks, 2 * side)
    return np.ascontiguousarray(np.swapaxes(table, 0, 1)).astype(np.float32)


def cmul(x, y):
    return x[0] * y[0] - x[1] * y[1], x[0] * y[1] + x[1] * y[0]


def csquare(x):
    return x[0] * x[0] - x[1] * x[1], 2.0 * (x[0] * x[1])


def row_times(row, matrix):
    out = []
    for b in range(3):
        re = row[0][0] * matrix[0][b][0] - row[0][1] * matrix[0][b][1]
        im = row[0][0] * matrix[0][b][1] + row[0][1] * matrix[0][b][0]
        for k in (1, 2):
            re = re + row[k][0] * matrix[k][b][0] - row[k][1] * matrix[k][b][1]
            im = im + row[k][0] * matrix[k][b][1] + row[k][1] * matrix[k][b][0]
        out.append((re, im))
    return out


def row_times_dagger(row, matrix):
    out = []
    for b in range(3):
        re = row[0][0] * matrix[b][0][0] + row[0][1] * matrix[b][0][1]
        im = row[0][1] * matrix[b][0][0] - row[0][0] * matrix[b][0][1]
        for k in (1, 2):
            re = re + row[k][0] * matrix[b][k][0] + row[k][1] * matrix[b][k][1]
            im = im + row[k][1] * matrix[b][k][0] - row[k][0] * matrix[b][k][1]
        out.append((re, im))
    return out


def exponential(x):
    t0, t1 = x[0], x[1]
    a, b, e = (x[2], x[3]), (x[4], x[5]), (x[6], x[7])
    t2 = -(t0 + t1)
    na = a[0] * a[0] + a[1] * a[1]
    nb = b[0] * b[0] + b[1] * b[1]
    ne = e[0] * e[0] + e[1] * e[1]
    s0, s1, s2 = t0 * t0, t1 * t1, t2 * t2
    ae = cmul(a, e)
    c = -(0.5 * (s0 + s1 + s2) + (na + nb + ne))
    cross = ae[1] * b[0] - ae[0] * b[1]
    d = t0 * ne + t1 * nb + t2 * na - t0 * t1 * t2 - 2.0 * cross
    c30 = c * (1.0 / 30.0)
    q0 = (None, d * (1.0 / 120.0))
    q1 = ((1.0 + c30) * 0.25, None)
    q2r = 1.0 / 20.0
    n0i = d * (q2r / 3.0)
    n1 = ((1.0 + c * q2r) * (1.0 / 3.0), q0[1] * (1.0 / 3.0))
    n2r = q1[0] * (1.0 / 3.0)
    m0 = (None, d * (0.5 * n2r))
    m1 = (0.5 + 0.5 * (c * n2r), 0.5 * n0i)
    m2 = (0.5 * n1[0], 0.5 * n1[1])
    q0 = (1.0 - d * m2[1], d * m2[0])
    q1 = (1.0 + c * m2[0], m0[1] + c * m2[1])
    q2 = m1
    for _ in range(3):
        q12 = cmul(q1, q2)
        q22 = csquare(q2)
        q00 = csquare(q0)
        q11 = csquare(q1)
        q01 = cmul(q0, q1)
        q02 = cmul(q0, q2)
        d2 = 2.0 * d
        q0 = (q00[0] - d2 * q12[1], q00[1] + d2 * q12[0])
        q1 = (
            2.0 * (q01[0] + c * q12[0]) - d * q22[1],
            2.0 * (q01[1] + c * q12[1]) + d * q22[0],
        )
        q2 = (q11[0] + 2.0 * q02[0] + c * q22[0], q11[1] + 2.0 * q02[1] + c * q22[1])
    u, v = q1
    s, t = q2
    result = [[None] * 3 for _ in range(3)]
    for at, (theta, m) in enumerate(
        ((t0, -(s0 + na + nb)), (t1, -(s1 + na + ne)), (t2, -(s2 + nb + ne)))
    ):
        result[at][at] = (q0[0] - v * theta + s * m, q0[1] + u * theta + t * m)
    y01 = (t2 * a[1] - (b[0] * e[0] + b[1] * e[1]), -t2 * a[0] - (b[1] * e[0] - b[0] * e[1]))
    y02 = (t1 * b[1] + ae[0], -t1 * b[0] + ae[1])
    y12 = (t0 * e[1] - (a[0] * b[0] + a[1] * b[1]), -t0 * e[0] - (a[0] * b[1] - a[1] * b[0]))
    for (i, j), xx, yy in zip(PAIRS, (a, b, e), (y01, y02, y12)):
        ur, vi, ui, vr = u * xx[0], v * xx[1], u * xx[1], v * xx[0]
        sr, ti, si, tr = s * yy[0], t * yy[1], s * yy[1], t * yy[0]
        result[i][j] = ((ur - vi) + (sr - ti), (ui + vr) + (si + tr))
        result[j][i] = ((sr + ti) - (ur + vi), (tr - si) + (ui - vr))
    return result


def project(rows):
    third = (rows[0][0][1] + rows[1][1][1] + rows[2][2][1]) * (1.0 / 3.0)
    out = [rows[0][0][1] - third, rows[1][1][1] - third]
    for i, j in PAIRS:
        out.append(0.5 * (rows[i][j][0] - rows[j][i][0]))
        out.append(0.5 * (rows[i][j][1] + rows[j][i][1]))
    return out


def lane_of(shape):
    return lax.broadcasted_iota(jnp.int32, shape, 1)


def halves(x):
    high = x.astype(BF16)
    low = (x - high.astype(F32)).astype(BF16)
    return high, low


def dot(x, y):
    return jnp.dot(x, y, preferred_element_type=F32)


def pick_ahead(swapped):
    half = swapped.shape[1] // 2
    return jnp.where(
        lane_of(swapped.shape) < half, swapped, pltpu.roll(swapped, swapped.shape[0] - 1, axis=0)
    )


def pick_behind(swapped):
    half = swapped.shape[1] // 2
    return jnp.where(lane_of(swapped.shape) >= half, swapped, pltpu.roll(swapped, 1, axis=0))


def left_transform(stacked, table_ref):
    high, low = halves(stacked)
    depth, width = stacked.shape
    at = 2 * table_ref.shape[1]
    both = dot(
        table_ref[at : at + 2 * depth, : 3 * depth], jnp.concatenate([high, high, low], axis=0)
    )
    even = lane_of((depth, width)) % (2 * depth) < depth
    return jnp.where(even, both[:depth], both[depth:])


def right_transform(high_ref, low_ref, table_ref, out_ref):
    size = table_ref.shape[1]
    high = high_ref[...]
    first = table_ref[:size]
    out_ref[...] = dot(high, first) + dot(low_ref[...], first) + dot(high, table_ref[size : 2 * size])


def forward_transform(d_ref, table_ref, high_ref, low_ref, spec_ref, out_ref, out_any, sems):
    slots, _, half, lanes = d_ref.shape
    parts = out_ref.shape[1] // 4
    rows = half // parts
    size = 4 * half
    for slot in range(slots):
        stacked = jnp.concatenate(
            [
                jnp.concatenate([d_ref[slot, 2 * f], d_ref[slot, 2 * f + 1]], axis=0)
                for f in range(4)
            ],
            axis=1,
        )
        y = left_transform(stacked, table_ref)
        for f in range(4):
            re = y[:half, f * lanes : (f + 1) * lanes]
            im = y[half:, f * lanes : (f + 1) * lanes]
            high, low = halves(jnp.concatenate([re, im], axis=1))
            at = (slot * 4 + f) * half
            high_ref[at : at + half, :] = high
            low_ref[at : at + half, :] = low
    copies = []
    for slot in range(slots):
        rows_of = pl.ds(slot * size, size)
        right_transform(high_ref.at[rows_of], low_ref.at[rows_of], table_ref, spec_ref.at[rows_of])
        for f in range(4):
            for part in range(parts):
                at = (slot * 4 + f) * half + part * rows
                for c in range(2):
                    out_ref[slot, f * parts + part, c * rows : (c + 1) * rows, :] = spec_ref[
                        at : at + rows, c * lanes : (c + 1) * lanes
                    ]
        copies.append(
            pltpu.make_async_copy(
                out_ref.at[slot], out_any.at[:, pl.ds(slot * 2 * rows, 2 * rows), :], sems.at[slot]
            )
        )
        copies[-1].start()
    return copies


def inverse_transform(in_ref, table_ref, high_ref, low_ref, spec_ref, x_ref):
    _, slots, half, lanes = x_ref.shape
    parts = in_ref.shape[0] // 4
    rows = half // parts
    for slot in range(slots):
        for f in range(4):
            columns = []
            for c in range(2):
                to = (slot * 2 + c) * rows
                pieces = [in_ref[f * parts + part, to : to + rows, :] for part in range(parts)]
                columns.append(jnp.concatenate(pieces, axis=0))
            high, low = halves(jnp.concatenate(columns, axis=1))
            at = (slot * 4 + f) * half
            high_ref[at : at + half, :] = high
            low_ref[at : at + half, :] = low
    right_transform(high_ref, low_ref, table_ref, spec_ref)
    for slot in range(slots):
        stacks = []
        for f in range(4):
            at = (slot * 4 + f) * half
            stacks.append(
                jnp.concatenate([spec_ref[at : at + half, :lanes], spec_ref[at : at + half, lanes:]], axis=0)
            )
        y = left_transform(jnp.concatenate(stacks, axis=1), table_ref)
        for f in range(4):
            x_ref[2 * f, slot] = y[:half, f * lanes : (f + 1) * lanes]
            x_ref[2 * f + 1, slot] = y[half:, f * lanes : (f + 1) * lanes]


def site_rows(plane, chunk, planes):
    return pl.ds(chunk * (8 * planes) + plane, 8, stride=planes)


def load_link(links_ref, direction, rows):
    base = direction * 18
    return [
        [(links_ref[base + 3 * i + j, rows, :], links_ref[base + 9 + 3 * i + j, rows, :]) for j in range(3)]
        for i in range(3)
    ]


def load_gauge(ref, plane, rows):
    return [
        [(ref[3 * i + j, plane, rows, :], ref[9 + 3 * i + j, plane, rows, :]) for j in range(3)]
        for i in range(3)
    ]


def store_gauge(ref, plane, rows, matrix):
    for i in range(3):
        for j in range(3):
            ref[3 * i + j, plane, rows, :] = matrix[i][j][0]
            ref[9 + 3 * i + j, plane, rows, :] = matrix[i][j][1]


def chunk_loop(planes, chunks, step):
    def run(index, carry):
        step(index // chunks, index % chunks)
        return carry

    lax.fori_loop(0, planes * chunks, run, 0)


def aligned(chunk):
    return pl.ds(pl.multiple_of(chunk * 8, 8), 8)


def shift_gauge(g_ref, shift, stack_ref, moved_ref, y_ref):
    planes, half, lanes = y_ref.shape[1:]
    for comp in range(18):
        for plane in range(planes):
            at = (comp * planes + plane) * half
            stack_ref[at : at + half, :] = jnp.concatenate(halves(g_ref[comp, plane]), axis=1)
    moved_ref[...] = dot(stack_ref[...], shift)
    for comp in range(18):
        for plane in range(planes):
            at = (comp * planes + plane) * half
            y_ref[comp, plane] = pick_ahead(moved_ref[at : at + half, :lanes])


def load_ahead(direction, g_ref, y_ref, moved_ref, plane, chunk):
    rows = aligned(chunk)
    if direction == 0:
        return load_gauge(g_ref, plane + 1, rows)
    if direction == 1:
        return load_gauge(y_ref, plane, rows)
    planes, half, lanes = y_ref.shape[1:]

    def at(comp):
        return moved_ref[pl.ds(pl.multiple_of((comp * planes + plane) * half + chunk * 8, 8), 8), lanes:]

    return [[(at(3 * i + j), at(9 + 3 * i + j)) for j in range(3)] for i in range(3)]


def divergence(v_ref, shift_ref, stack_ref, moved_ref, d_ref):
    _, comps, planes, half, lanes = v_ref.shape
    size = comps * planes * half
    for direction in (1, 2):
        for comp in range(comps):
            for plane in range(planes):
                at = (direction - 1) * size + (comp * planes + plane) * half
                stack_ref[at : at + half, :] = jnp.concatenate(
                    halves(v_ref[direction, comp, plane]), axis=1
                )
    first = shift_ref.shape[0] - 2 * lanes
    moved_ref[:size, :lanes] = dot(stack_ref[:size], shift_ref[first:, :lanes])
    moved_ref[size : 2 * size, :lanes] = dot(stack_ref[size : 2 * size], shift_ref[first:, lanes:])
    for comp in range(comps):
        before = None
        for plane in range(planes):
            at = (comp * planes + plane) * half
            vx = v_ref[0, comp, plane]
            total = (pick_behind(moved_ref[at : at + half, :lanes]) - v_ref[1, comp, plane]) + (
                moved_ref[size + at : size + at + half, :lanes] - v_ref[2, comp, plane]
            )
            total = total - vx
            if before is not None:
                total = total + before
            before = vx
            d_ref[plane, comp] = total
        d_ref[planes, comp] = before


class Split(NamedTuple):
    times: int
    group: int
    wide: int
    near: int

    @property
    def rows(self):
        return self.wide + self.near

    @property
    def offset(self):
        return self.times * self.wide

    @property
    def total(self):
        return self.offset + self.group * self.near

    @property
    def peers(self):
        groups = self.times // self.group
        steps = [(g, m) for g in range(groups) for m in range(self.group)]
        return steps[1:]

    def block(self, step):
        return self.wide if step[0] else self.rows

    def moved(self, device, step, back=False):
        sign = -1 if back else 1
        groups = self.times // self.group
        home = (device // self.group + sign * step[0]) % groups
        return home * self.group + (device % self.group + sign * step[1]) % self.group

    def starts(self, device):
        wide = device * self.wide
        near = self.offset + device % self.group * self.near
        if isinstance(device, int):
            return wide, near
        return pl.multiple_of(wide, 8), pl.multiple_of(near, 8)


def start_kernel(split, links_any, table_any, source_any, out_any, *rest):
    peers = split.peers
    cut_refs, held_refs = rest[: len(peers)], rest[len(peers) : 2 * len(peers)]
    links_ref, table_ref, v_ref, d_ref, stack_ref, moved_ref, high_ref, low_ref, spec_ref, out_ref, sems, cut_sems, out_sems = rest[
        2 * len(peers) :
    ]
    _, _, planes, half, _ = v_ref.shape
    mine = lax.axis_index("tm")
    copies = [
        pltpu.make_async_copy(
            links_any.at[pl.ds(18 * direction, 18)], links_ref.at[pl.ds(18 * direction, 18)], sems.at[direction]
        )
        for direction in range(3)
    ]
    copies.append(pltpu.make_async_copy(table_any, table_ref, sems.at[3]))
    reads, writes = [], []
    for k, (step, cut, held) in enumerate(zip(peers, cut_refs, held_refs)):
        wide, near = split.starts(split.moved(mine, step))
        pieces = [(wide, 0, split.wide)] if step[0] else [(wide, 0, split.wide), (near, split.wide, split.near)]
        for part, (start, to, size) in enumerate(pieces):
            reads.append(
                pltpu.make_async_copy(
                    source_any.at[:, pl.ds(start, size), :], held.at[:, pl.ds(to, size), :], cut_sems.at[part, k]
                )
            )
        writes.append(pltpu.make_async_copy(held, cut, cut_sems.at[2, k]))
    for copy in copies + reads:
        copy.start()
    for direction in range(3):
        copies[direction].wait()

        def step(plane, chunk, direction=direction):
            rows = site_rows(plane, chunk, planes)
            for comp, value in enumerate(project(load_link(links_ref, direction, rows))):
                v_ref[direction, comp, plane, aligned(chunk), :] = value

        chunk_loop(planes, half // 8, step)
    for copy in reads:
        copy.wait()
    for copy in writes:
        copy.start()
    copies[3].wait()
    divergence(v_ref, table_ref, stack_ref, moved_ref, d_ref)
    outs = forward_transform(d_ref, table_ref, high_ref, low_ref, spec_ref, out_ref, out_any, out_sems)
    for copy in writes + outs:
        copy.wait()


def convolve_kernel(planes, in_ref, table_ref, out_ref):
    count = in_ref.shape[0]
    parts, offsets, rows, _ = table_ref.shape
    across = planes * count
    part = lax.axis_index("space") % parts
    step = min(8, rows)

    def run(index, carry):
        c = index // (rows // step)
        chunk = index % (rows // step)

        def at(slot):
            return pl.ds((slot * 2 + c) * rows + chunk * step, step)

        table = [table_ref[part, k, pl.ds(chunk * step, step), :] for k in range(offsets)]
        data = []
        for x in range(across):
            owner, plane = divmod(x, planes)
            value = in_ref[owner, at(plane), :]
            if plane == 0:
                value = value + in_ref[(owner - 1) % count, at(planes), :]
            data.append(value)
        for x in range(across):
            owner, plane = divmod(x, planes)
            total = table[0] * data[x] + table[offsets - 1] * data[(x + across // 2) % across]
            for k in range(1, offsets - 1):
                total = total + table[k] * (data[(x + k) % across] + data[(x - k) % across])
            out_ref[owner, at(plane), :] = total
            if plane == 0:
                out_ref[(owner - 1) % count, at(planes), :] = total
        return carry

    lax.fori_loop(0, 2 * (rows // step), run, 0)


def flatten_shares(x_ref, flat_ref, planes, split):
    half = x_ref.shape[2]
    first = half // 2
    if flat_ref.shape[1] > planes * half:
        flat_ref[...] = jnp.zeros_like(flat_ref)
    for comp in range(8):
        for plane in range(planes):
            value = x_ref[comp, plane]
            flat_ref[comp, pl.ds(plane, first, stride=planes), :] = value[:first]
            flat_ref[comp, pl.ds(split.offset + plane, half - first, stride=planes), :] = value[first:]


def share_copies(flat_ref, share_refs, split, devices, sems):
    copies = []
    for k, (share_ref, device) in enumerate(zip(share_refs, devices)):
        wide, near = split.starts(device)
        copies.append(
            pltpu.make_async_copy(
                flat_ref.at[:, pl.ds(wide, split.wide), :], share_ref.at[:, : split.wide, :], sems.at[0, k]
            )
        )
        copies.append(
            pltpu.make_async_copy(
                flat_ref.at[:, pl.ds(near, split.near), :], share_ref.at[:, split.wide :, :], sems.at[1, k]
            )
        )
    return copies


def middle_kernel(split, in_ref, links_ref, inverse_ref, forward_ref, *rest):
    out_any, x_any = rest[:2]
    share_refs = rest[2 : 2 + split.times]
    x_ref, g_ref, y_ref, v_ref, d_ref, stack_ref, moved_ref, high_ref, low_ref, spec_ref, flat_ref, out_ref, sems, share_sems, out_sems = rest[2 + split.times :]
    _, slots, half, _ = x_ref.shape
    planes = slots - 1
    inverse_transform(in_ref, inverse_ref, high_ref, low_ref, spec_ref, x_ref)
    flatten_shares(x_ref, flat_ref, planes, split)
    mine = lax.axis_index("tm")
    devices = [(mine + shift) % split.times for shift in range(split.times)]
    copies = share_copies(flat_ref, share_refs, split, devices, share_sems)
    copies.append(pltpu.make_async_copy(x_ref, x_any, sems))
    for copy in copies:
        copy.start()

    def raise_step(plane, chunk):
        rows = aligned(chunk)
        store_gauge(g_ref, plane, rows, exponential([x_ref[k, plane, rows, :] for k in range(8)]))

    chunk_loop(slots, half // 8, raise_step)
    lanes = x_ref.shape[3]
    shift_gauge(g_ref, inverse_ref[inverse_ref.shape[0] - 2 * lanes :], stack_ref, moved_ref, y_ref)

    def rotate_step(plane, chunk):
        rows = aligned(chunk)
        gauge = load_gauge(g_ref, plane, rows)
        link_rows = site_rows(plane, chunk, planes)
        for direction in range(3):
            link = load_link(links_ref, direction, link_rows)
            ahead = load_ahead(direction, g_ref, y_ref, moved_ref, plane, chunk)
            turned = [row_times_dagger(row_times(gauge[i], link), ahead) for i in range(3)]
            for comp, value in enumerate(project(turned)):
                v_ref[direction, comp, plane, rows, :] = value

    chunk_loop(planes, half // 8, rotate_step)
    divergence(v_ref, forward_ref, stack_ref, moved_ref, d_ref)
    copies += forward_transform(
        d_ref, forward_ref, high_ref, low_ref, spec_ref, out_ref, out_any, out_sems
    )
    for copy in copies:
        copy.wait()


def last_transform_kernel(split, in_ref, inverse_ref, x_ref, *rest):
    share_refs = rest[: split.times]
    high_ref, low_ref, spec_ref, flat_ref = rest[split.times :]
    inverse_transform(in_ref, inverse_ref, high_ref, low_ref, spec_ref, x_ref)
    flatten_shares(x_ref, flat_ref, x_ref.shape[1] - 1, split)
    for device, share_ref in enumerate(share_refs):
        wide, near = split.starts(device)
        share_ref[:, : split.wide, :] = flat_ref[:, wide : wide + split.wide, :]
        share_ref[:, split.wide :, :] = flat_ref[:, near : near + split.near, :]


def total_of(first, second):
    earlier = exponential(first)
    later = exponential(second)
    return [row_times(later[i], earlier) for i in range(3)]


def finish_kernel(links_any, first_any, table_any, second_ref, out_any, g_ref, y_ref, stack_ref, moved_ref, links_ref, first_ref, shift_ref, out_ref, sems):
    _, slots, half, lanes = first_ref.shape
    planes = slots - 1
    chunks = half // 8
    copies = [
        pltpu.make_async_copy(first_any, first_ref, sems.at[0]),
        pltpu.make_async_copy(links_any, links_ref, sems.at[1]),
        pltpu.make_async_copy(
            table_any.at[pl.ds(table_any.shape[0] - 2 * lanes, 2 * lanes)], shift_ref, sems.at[2]
        ),
    ]
    for copy in copies:
        copy.start()
    copies[0].wait()

    def raise_step(plane, chunk):
        rows = aligned(chunk)
        store_gauge(
            g_ref,
            plane,
            rows,
            total_of(
                [first_ref[k, plane, rows, :] for k in range(8)],
                [second_ref[k, plane, rows, :] for k in range(8)],
            ),
        )

    chunk_loop(slots, half // 8, raise_step)
    copies[2].wait()
    shift_gauge(g_ref, shift_ref[...], stack_ref, moved_ref, y_ref)
    copies[1].wait()

    def piece(chunk):
        rows = pl.ds(pl.multiple_of(chunk * (8 * planes), 8), 8 * planes)
        return pltpu.make_async_copy(out_ref.at[:, rows, :], out_any.at[:, rows, :], sems.at[3 + chunk])

    def rotate_step(chunk, plane):
        rows = aligned(chunk)
        gauge = load_gauge(g_ref, plane, rows)
        link_rows = site_rows(plane, chunk, planes)
        for direction in range(3):
            link = load_link(links_ref, direction, link_rows)
            ahead = load_ahead(direction, g_ref, y_ref, moved_ref, plane, chunk)
            for i in range(3):
                row = row_times_dagger(row_times(gauge[i], link), ahead)
                for j in range(3):
                    out_ref[direction * 18 + 3 * i + j, link_rows, :] = row[j][0]
                    out_ref[direction * 18 + 9 + 3 * i + j, link_rows, :] = row[j][1]

        @pl.when(plane == planes - 1)
        def _():
            piece(chunk).start()

    chunk_loop(chunks, planes, rotate_step)

    for chunk in range(chunks):
        piece(chunk).wait()


def lane_sums(rows):
    ones = jnp.ones((8, rows.shape[1]), BF16)
    total = None
    rest = rows
    for _ in range(3):
        piece = rest.astype(BF16)
        rest = rest - piece.astype(F32)
        part = lax.dot_general(ones, piece, (((1,), (1,)), ((), ())), preferred_element_type=F32)
        total = part if total is None else total + part
    return total


def load_rows(ref, rows):
    return [[(ref[3 * i + j, rows, :], ref[9 + 3 * i + j, rows, :]) for j in range(3)] for i in range(3)]


def sink_kernel(split, sink_ref, src_time_ref, src_site_ref, first_any, second_ref, source_ref, own_early_any, *rest):
    times, group, per = split.times, split.group, split.rows
    rest = list(rest)

    def take(count):
        taken = rest[:count]
        del rest[:count]
        return taken

    early = [own_early_any] + take(times - 1)
    own, late = take(times), take(times - 1)
    partners_any = take(times - 1)
    out_ref, near_ref, wide_ref, x_ref, gauge_ref, sum_ref, before_ref, anchor_ref, sems = rest
    pairs = source_ref.shape[0] // 2
    groups = pairs // 3
    _, slots, half, lanes = second_ref.shape
    planes = slots - 1
    mine = lax.axis_index("tm")
    sink = sink_ref[0]
    column = src_site_ref[0] % (half * lanes)
    plane = src_site_ref[0] // (half * lanes) - lax.axis_index("space") * planes
    present = (src_time_ref[0] == mine) & (plane >= 0) & (plane < planes)
    safe = jnp.clip(plane, 0, planes - 1)
    row = column // lanes
    block = pl.ds(pl.multiple_of(row // 8 * 8, 8), 8)
    before = pltpu.make_async_copy(first_any.at[:, safe, block, :], before_ref, sems.at[0])
    fetches = [pltpu.make_async_copy(early[0], x_ref.at[k], sems.at[1 + k]) for k in range(2)]
    held = [near_ref.at[k] for k in range(group - 1)] + [wide_ref.at[k] for k in range(times - group)]
    partners = [
        pltpu.make_async_copy(partner, to, sems.at[3 + k])
        for k, (partner, to) in enumerate(zip(partners_any, held))
    ]

    def fetch(condition, value, to):
        @pl.when(condition)
        def _():
            pltpu.make_async_copy(value, x_ref.at[to], sems.at[1 + to]).start()

    for shift in range(times):
        fetch((mine - sink) % times == shift, early[shift], 0)
    for at in range(times):
        fetch((mine == sink) & (mine == at), own[at], 1)
    for at in range(times - 1):
        fetch((mine != sink) & (jnp.where(mine > sink, mine - 1, mine) == at), late[at], 1)
    for copy in partners:
        copy.start()
    before.start()
    chunks = per // 8
    for number in range(2):
        fetches[number].wait()
        for chunk in range(chunks):
            rows = slice(chunk * 8, chunk * 8 + 8)
            turn = exponential([x_ref[number, k, rows, :] for k in range(8)])
            if number:
                turn = [row_times(turn[i], load_rows(gauge_ref, rows)) for i in range(3)]
            for i in range(3):
                for j in range(3):
                    gauge_ref[3 * i + j, rows, :] = turn[i][j][0]
                    gauge_ref[9 + 3 * i + j, rows, :] = turn[i][j][1]

    def accumulate(block_ref, offset, first, count, source_device, add):
        base = source_device * pairs

        def run(group_at, carry):
            sums = [None] * 3
            for chunk in range(count // 8):
                rows = slice(first + chunk * 8, first + chunk * 8 + 8)
                own_rows = pl.ds(pl.multiple_of(offset + chunk * 8, 8), 8)
                column = [
                    (
                        block_ref[3 * group_at + c, own_rows, :],
                        block_ref[pairs + 3 * group_at + c, own_rows, :],
                    )
                    for c in range(3)
                ]
                for a in range(3):
                    for c in range(3):
                        part = cmul(
                            (gauge_ref[3 * a + c, rows, :], gauge_ref[9 + 3 * a + c, rows, :]), column[c]
                        )
                        sums[a] = part if sums[a] is None else (sums[a][0] + part[0], sums[a][1] + part[1])
            for a in range(3):
                to = pl.ds(pl.multiple_of((base + 3 * group_at + a) * 8, 8), 8)
                re, im = sums[a]
                if add:
                    re, im = re + sum_ref[0, to, :], im + sum_ref[1, to, :]
                sum_ref[0, to, :] = re
                sum_ref[1, to, :] = im
            return carry

        lax.fori_loop(0, groups, run, 0, unroll=2 if groups % 2 == 0 else 1)

    wide_start, near_start = split.starts(mine)
    accumulate(source_ref, wide_start, 0, split.wide, mine, False)
    accumulate(source_ref, near_start, split.wide, split.near, mine, True)
    for k, step in enumerate(split.peers):
        partners[k].wait()
        owner = split.moved(mine, step, back=True)
        accumulate(held[k], 0, 0, split.block(step), owner, False)
    before.wait()
    total = total_of([before_ref[k] for k in range(8)], [second_ref[k, safe, block, :] for k in range(8)])
    wide = (8, lanes)
    keep = (lane_of(wide) == jnp.where(present, column % lanes, -1)) & (
        lax.broadcasted_iota(jnp.int32, wide, 0) == row % 8
    )
    anchor_ref[...] = jnp.zeros_like(anchor_ref)
    for k in range(18):
        value = total[k % 9 // 3][k % 3][k // 9]
        anchor_ref[k : k + 1, :] = jnp.sum(jnp.where(keep, value, 0.0), axis=0, keepdims=True)
    whole = SC * SC
    width = -(-(whole + 24) // lanes) * lanes
    pieces = []
    for part in range(2):
        total = sum_ref[part, pl.ds(0, whole, stride=8), :]
        for k in range(1, 8):
            total = total + sum_ref[part, pl.ds(k, whole, stride=8), :]
        extra = anchor_ref[...] if part == 0 else jnp.zeros((24, lanes), F32)
        pieces += [total, extra, jnp.zeros((width - whole - 24, lanes), F32)]
    sums = lane_sums(jnp.concatenate(pieces, axis=0))
    block = jnp.concatenate(
        [sums[0:1, k * lanes : (k + 1) * lanes] for k in range(2 * width // lanes)], axis=0
    )

    def spread(index, carry):
        out_ref[index] = block
        return carry

    lax.fori_loop(0, out_ref.shape[0], spread, 0)


def wall_kernel(scale, in_ref, out_ref):
    whole = SC * SC
    total = jnp.sum(in_ref[...], axis=0)
    half = total.shape[0] // 2
    re = jnp.concatenate([total[k : k + 1] for k in range(half)], axis=1)
    im = jnp.concatenate([total[half + k : half + k + 1] for k in range(half)], axis=1)
    width = re.shape[1]
    colour = lane_of((1, width)) // SC % 3
    out_re = jnp.zeros((1, width), F32)
    out_im = jnp.zeros((1, width), F32)
    for b in range(3):
        for c in range(3):
            at = whole + 3 * b + c
            ar = re[:, at : at + 1]
            ai = re[:, at + 9 : at + 10]
            amount = (SC * (b - c)) % width
            wr = pltpu.roll(re, amount, axis=1) if amount else re
            wi = pltpu.roll(im, amount, axis=1) if amount else im
            here = colour == b
            out_re = out_re + jnp.where(here, wr * ar + wi * ai, 0.0)
            out_im = out_im + jnp.where(here, wi * ar - wr * ai, 0.0)
    out_ref[0:1, :] = out_re[:, :whole] * scale
    out_ref[1:2, :] = out_im[:, :whole] * scale


def shape(*dims):
    return jax.ShapeDtypeStruct(dims, F32)


SMEM_SPEC = pl.BlockSpec(memory_space=pltpu.SMEM)
VMEM_SPEC = pl.BlockSpec(memory_space=pltpu.VMEM)
ANY_SPEC = pl.BlockSpec(memory_space=pl.ANY)
HBM_SPEC = pl.BlockSpec(memory_space=pltpu.HBM)


def call(kernel, outs, out_specs, inputs, in_specs, scratch):
    inputs = [
        pltpu.with_memory_space_constraint(x, pltpu.HBM) if spec is HBM_SPEC else x
        for x, spec in zip(inputs, in_specs)
    ]
    outs = [
        pltpu.HBM(out.shape, out.dtype) if spec is HBM_SPEC else out
        for out, spec in zip(outs, out_specs)
    ]
    return pl.pallas_call(
        kernel,
        out_shape=outs,
        in_specs=in_specs,
        out_specs=out_specs,
        scratch_shapes=scratch,
        compiler_params=pltpu.CompilerParams(vmem_limit_bytes=20 * 1024 * 1024),
    )(*inputs)


def body(links, propagator, sink_time, src_time, src_site):
    count = lax.axis_size("space")
    times = lax.axis_size("tm")
    planes = links.shape[5]
    side = math.isqrt(links.shape[6])
    half, lanes = side // 2, 2 * side
    across = planes * count
    slots = planes + 1
    parts = count // 4
    rows = half // parts
    sites = planes * half
    group = 2 if times % 2 == 0 else 1
    spread = sites // 2
    split = Split(times, group, 8 * -(-spread // (8 * times)), 8 * -(-(sites - spread) // (8 * group)))
    pairs = propagator.shape[1]

    forward = jnp.asarray(transform_table(side, False))
    inverse = jnp.asarray(transform_table(side, True))
    table = jnp.asarray(filter_table(side, across, parts))

    def interleave(array, lead):
        return array.reshape(lead, planes, half, lanes).transpose(0, 2, 1, 3).reshape(lead, sites, lanes)

    lattice = interleave(links, 54)

    def forwarded(value, shift):
        return lax.ppermute(value, "tm", [(i, (i + shift) % times) for i in range(times)])

    spectrum_shape = shape(count, slots * 2 * rows, lanes)
    transform_scratch = [
        VMEM((4 * slots * half, 2 * lanes), BF16),
        VMEM((4 * slots * half, 2 * lanes), BF16),
        VMEM((4 * slots * half, 2 * lanes), F32),
    ]
    divergence_scratch = [
        VMEM((3, 8, planes, half, lanes), F32),
        VMEM((slots, 8, half, lanes), F32),
    ]
    gauge_scratch = [
        VMEM((18, slots, half, lanes), F32),
        VMEM((18, planes, half, lanes), F32),
    ]
    shift_scratch = [
        VMEM((18 * planes * half, 2 * lanes), BF16),
        VMEM((18 * planes * half, 2 * lanes), F32),
    ]
    out_scratch = [VMEM((slots, count, 2 * rows, lanes), F32)]
    flat_scratch = [VMEM((8, split.total, lanes), F32)]
    algebra_shape = shape(8, slots, half, lanes)
    share_shapes = [shape(8, split.rows, lanes)] * times

    def turn(spectrum):
        return lax.all_to_all(spectrum, "space", 0, 0, tiled=True)

    def convolve(spectrum):
        (out,) = call(
            functools.partial(convolve_kernel, planes),
            [spectrum_shape],
            [VMEM_SPEC],
            [spectrum, table],
            [VMEM_SPEC] * 2,
            [],
        )
        return out

    source = interleave(propagator, 2 * pairs)
    if split.total > sites:
        fill = jnp.zeros((2 * pairs, split.offset - spread, lanes), F32)
        source = jnp.concatenate([source[:, :spread], fill, source[:, spread:]], axis=1)
    scalars = [sink_time % times, src_time % times, jnp.maximum(src_site, 0)]
    cut_shapes = [shape(2 * pairs, split.block(step), lanes) for step in split.peers]
    spectrum, *cuts = call(
        functools.partial(start_kernel, split),
        [spectrum_shape] + cut_shapes,
        [HBM_SPEC] * times,
        [lattice, forward, source],
        [HBM_SPEC] * 3,
        [VMEM(cut.shape, F32) for cut in cut_shapes]
        + [VMEM(lattice.shape, F32), VMEM(forward.shape, BF16)]
        + divergence_scratch
        + shift_scratch
        + transform_scratch
        + out_scratch
        + [
            pltpu.SemaphoreType.DMA((4,)),
            pltpu.SemaphoreType.DMA((3, times - 1)),
            pltpu.SemaphoreType.DMA((slots,)),
        ],
    )
    held_scratch = [
        VMEM((max(1, group - 1), 2 * pairs, split.rows, lanes), F32),
        VMEM((max(1, times - group), 2 * pairs, split.wide, lanes), F32),
    ]
    scalars = [sink_time % times, src_time % times, jnp.maximum(src_site, 0)]
    sources = [
        lax.ppermute(cut, "tm", [(i, split.moved(i, step)) for i in range(times)])
        for step, cut in zip(split.peers, cuts)
    ]

    spectrum = turn(spectrum)
    spectrum = convolve(spectrum)
    spectrum = turn(spectrum)
    spectrum, first, *early = call(
        functools.partial(middle_kernel, split),
        [spectrum_shape, algebra_shape] + share_shapes,
        [HBM_SPEC] * (2 + times),
        [spectrum, lattice, inverse, forward],
        [VMEM_SPEC] * 4,
        [VMEM(algebra_shape.shape, F32)]
        + gauge_scratch
        + divergence_scratch
        + shift_scratch
        + transform_scratch
        + flat_scratch
        + out_scratch
        + [
            pltpu.SemaphoreType.DMA,
            pltpu.SemaphoreType.DMA((2, times)),
            pltpu.SemaphoreType.DMA((slots,)),
        ],
    )
    first_shares = [forwarded(early[shift], shift) for shift in range(1, times)]
    spectrum = turn(spectrum)
    spectrum = convolve(spectrum)
    spectrum = turn(spectrum)
    second, *shares = call(
        functools.partial(last_transform_kernel, split),
        [algebra_shape] + share_shapes,
        [VMEM_SPEC] * (1 + times),
        [spectrum, inverse],
        [VMEM_SPEC] * 2,
        transform_scratch + flat_scratch,
    )

    def sent_from(source_index):
        def send(*blocks):
            return tuple(
                lax.ppermute(blocks[to], "tm", [(source_index, to)])
                for to in range(times)
                if to != source_index
            )

        return send

    second_shares = lax.switch(sink_time[0] % times, [sent_from(k) for k in range(times)], *shares)
    (fixed,) = call(
        finish_kernel,
        [shape(54, sites, lanes)],
        [HBM_SPEC],
        [lattice, first, inverse, second],
        [HBM_SPEC] * 3 + [VMEM_SPEC],
        gauge_scratch
        + shift_scratch
        + [
            VMEM(lattice.shape, F32),
            VMEM(algebra_shape.shape, F32),
            VMEM((2 * lanes, 2 * lanes), BF16),
            VMEM(lattice.shape, F32),
            pltpu.SemaphoreType.DMA((3 + half // 8,)),
        ],
    )
    width = -(-(SC * SC + 24) // lanes)
    devices = count * times
    (payload,) = call(
        functools.partial(sink_kernel, split),
        [shape(devices, 2 * width, lanes)],
        [VMEM_SPEC],
        scalars + [first, second, source, early[0]] + first_shares + shares + list(second_shares) + sources,
        [SMEM_SPEC] * 3
        + [HBM_SPEC]
        + [VMEM_SPEC] * 2
        + [HBM_SPEC]
        + [ANY_SPEC] * (2 * times - 1)
        + [HBM_SPEC] * (2 * times - 2),
        held_scratch
        + [
            VMEM((2, 8, split.rows, lanes), F32),
            VMEM((18, split.rows, lanes), F32),
            VMEM((2, SC * SC * 8, lanes), F32),
            VMEM((8, 8, lanes), F32),
            VMEM((24, lanes), F32),
            pltpu.SemaphoreType.DMA((2 + times,)),
        ],
    )
    gathered = lax.all_to_all(payload, ("space", "tm"), 0, 0, tiled=True)
    scale = float(across * side * side) ** (-0.5)
    (wall,) = call(functools.partial(wall_kernel, scale), [shape(2, SC * SC)], [VMEM_SPEC], [gathered], [VMEM_SPEC], [])
    fixed = fixed.reshape(54, half, planes, lanes).transpose(0, 2, 1, 3).reshape(links.shape)
    return fixed, wall


def solution(mesh):
    placed = (
        P("tm", None, None, None, None, "space", None),
        P(None, "tm", "space", None),
        P(),
        P(),
        P(),
    )
    return jax.shard_map(
        body,
        mesh=mesh,
        in_specs=placed,
        out_specs=(P("tm", None, None, None, None, "space", None), P()),
        check_vma=False,
    )
```

```python
import functools
import math
from typing import NamedTuple

import jax
import jax.numpy as jnp
import numpy as np
from jax import lax
from jax.experimental import pallas as pl
from jax.experimental.pallas import tpu as pltpu
from jax.sharding import PartitionSpec as P


SC = 12
STEP_SIZE = 0.08
PEAK_SQUARE = 12.0
F32 = jnp.float32
BF16 = jnp.bfloat16
VMEM = pltpu.VMEM
PAIRS = ((0, 1), (0, 2), (1, 2))


def split_table(table):
    high = table.astype(jnp.bfloat16)
    low = (table - high.astype(np.float64)).astype(jnp.bfloat16)
    return high, low


def as_real(real, imag):
    return np.block([[real, imag], [-imag, real]])


@functools.lru_cache(None)
def transform_table(side, inverse):
    half = side // 2
    sign = 1.0 if inverse else -1.0
    k = np.arange(half)
    twist = np.exp(1j * sign * 2.0 * np.pi * k / side)
    even = np.exp(1j * sign * 2.0 * np.pi * np.outer(k, k) / half)
    odd = even * (twist[None, :] if inverse else twist[:, None])
    left = np.concatenate([as_real(m.real, -m.imag) for m in (even, odd)], axis=0)
    high, low = split_table(left)
    fill = np.zeros((left.shape[0], 4 * side - 3 * side), high.dtype)
    left = np.concatenate([high, low, high, fill], axis=1)
    z = np.arange(side)
    depth_phase = sign * 2.0 * np.pi * np.outer(z, z) / side
    parity = np.array([[1.0, 1.0], [1.0, -1.0]])
    right = as_real(np.kron(parity, np.cos(depth_phase)), np.kron(parity, np.sin(depth_phase)))
    high, low = split_table(right)
    lanes = np.arange(2 * side)
    from_depth = lanes - lanes % side + (lanes + (1 if inverse else -1)) % side
    moves = [np.eye(2 * side)[:, (lanes + side) % (2 * side)], np.eye(2 * side)[:, from_depth]]
    shift = np.concatenate(moves, axis=1)
    shift = np.concatenate([shift, shift], axis=0).astype(high.dtype)
    return np.concatenate([high, low, left, shift], axis=0)


@functools.lru_cache(None)
def filter_table(side, across, blocks):
    half = side // 2
    squares = 4.0 * np.sin(np.pi * np.arange(side) / side) ** 2
    squares_across = 4.0 * np.sin(np.pi * np.arange(across) / across) ** 2
    column = (squares[:, None] + squares[None, :]).reshape(2, half, side)
    column = np.swapaxes(column, 0, 1).reshape(half, 2 * side)
    momentum = squares_across[:, None, None] + column[None]
    weight = np.where(momentum > 0.0, PEAK_SQUARE / np.where(momentum > 0.0, momentum, 1.0), 0.0)
    offsets = np.arange(across // 2 + 1)
    phase = np.cos(2.0 * np.pi * np.outer(offsets, np.arange(across)) / across)
    table = np.einsum("dk,krl->drl", phase, weight) / (across * side * side)
    table = table * (STEP_SIZE / 16.0)
    table = table.reshape(len(offsets), blocks, half // blocks, 2 * side)
    return np.ascontiguousarray(np.swapaxes(table, 0, 1)).astype(np.float32)


def cmul(x, y):
    return x[0] * y[0] - x[1] * y[1], x[0] * y[1] + x[1] * y[0]


def csquare(x):
    return x[0] * x[0] - x[1] * x[1], 2.0 * (x[0] * x[1])


def row_times(row, matrix):
    out = []
    for b in range(3):
        re = row[0][0] * matrix[0][b][0] - row[0][1] * matrix[0][b][1]
        im = row[0][0] * matrix[0][b][1] + row[0][1] * matrix[0][b][0]
        for k in (1, 2):
            re = re + row[k][0] * matrix[k][b][0] - row[k][1] * matrix[k][b][1]
            im = im + row[k][0] * matrix[k][b][1] + row[k][1] * matrix[k][b][0]
        out.append((re, im))
    return out


def row_times_dagger(row, matrix):
    out = []
    for b in range(3):
        re = row[0][0] * matrix[b][0][0] + row[0][1] * matrix[b][0][1]
        im = row[0][1] * matrix[b][0][0] - row[0][0] * matrix[b][0][1]
        for k in (1, 2):
            re = re + row[k][0] * matrix[b][k][0] + row[k][1] * matrix[b][k][1]
            im = im + row[k][1] * matrix[b][k][0] - row[k][0] * matrix[b][k][1]
        out.append((re, im))
    return out


def exponential(x):
    t0, t1 = x[0], x[1]
    a, b, e = (x[2], x[3]), (x[4], x[5]), (x[6], x[7])
    t2 = -(t0 + t1)
    na = a[0] * a[0] + a[1] * a[1]
    nb = b[0] * b[0] + b[1] * b[1]
    ne = e[0] * e[0] + e[1] * e[1]
    s0, s1, s2 = t0 * t0, t1 * t1, t2 * t2
    ae = cmul(a, e)
    c = -(0.5 * (s0 + s1 + s2) + (na + nb + ne))
    cross = ae[1] * b[0] - ae[0] * b[1]
    d = t0 * ne + t1 * nb + t2 * na - t0 * t1 * t2 - 2.0 * cross
    c30 = c * (1.0 / 30.0)
    q0 = (None, d * (1.0 / 120.0))
    q1 = ((1.0 + c30) * 0.25, None)
    q2r = 1.0 / 20.0
    n0i = d * (q2r / 3.0)
    n1 = ((1.0 + c * q2r) * (1.0 / 3.0), q0[1] * (1.0 / 3.0))
    n2r = q1[0] * (1.0 / 3.0)
    m0 = (None, d * (0.5 * n2r))
    m1 = (0.5 + 0.5 * (c * n2r), 0.5 * n0i)
    m2 = (0.5 * n1[0], 0.5 * n1[1])
    q0 = (1.0 - d * m2[1], d * m2[0])
    q1 = (1.0 + c * m2[0], m0[1] + c * m2[1])
    q2 = m1
    for _ in range(3):
        q12 = cmul(q1, q2)
        q22 = csquare(q2)
        q00 = csquare(q0)
        q11 = csquare(q1)
        q01 = cmul(q0, q1)
        q02 = cmul(q0, q2)
        d2 = 2.0 * d
        q0 = (q00[0] - d2 * q12[1], q00[1] + d2 * q12[0])
        q1 = (
            2.0 * (q01[0] + c * q12[0]) - d * q22[1],
            2.0 * (q01[1] + c * q12[1]) + d * q22[0],
        )
        q2 = (q11[0] + 2.0 * q02[0] + c * q22[0], q11[1] + 2.0 * q02[1] + c * q22[1])
    u, v = q1
    s, t = q2
    result = [[None] * 3 for _ in range(3)]
    for at, (theta, m) in enumerate(
        ((t0, -(s0 + na + nb)), (t1, -(s1 + na + ne)), (t2, -(s2 + nb + ne)))
    ):
        result[at][at] = (q0[0] - v * theta + s * m, q0[1] + u * theta + t * m)
    y01 = (t2 * a[1] - (b[0] * e[0] + b[1] * e[1]), -t2 * a[0] - (b[1] * e[0] - b[0] * e[1]))
    y02 = (t1 * b[1] + ae[0], -t1 * b[0] + ae[1])
    y12 = (t0 * e[1] - (a[0] * b[0] + a[1] * b[1]), -t0 * e[0] - (a[0] * b[1] - a[1] * b[0]))
    for (i, j), xx, yy in zip(PAIRS, (a, b, e), (y01, y02, y12)):
        ur, vi, ui, vr = u * xx[0], v * xx[1], u * xx[1], v * xx[0]
        sr, ti, si, tr = s * yy[0], t * yy[1], s * yy[1], t * yy[0]
        result[i][j] = ((ur - vi) + (sr - ti), (ui + vr) + (si + tr))
        result[j][i] = ((sr + ti) - (ur + vi), (tr - si) + (ui - vr))
    return result


def project(rows):
    third = (rows[0][0][1] + rows[1][1][1] + rows[2][2][1]) * (1.0 / 3.0)
    out = [rows[0][0][1] - third, rows[1][1][1] - third]
    for i, j in PAIRS:
        out.append(0.5 * (rows[i][j][0] - rows[j][i][0]))
        out.append(0.5 * (rows[i][j][1] + rows[j][i][1]))
    return out


def lane_of(shape):
    return lax.broadcasted_iota(jnp.int32, shape, 1)


def halves(x):
    high = x.astype(BF16)
    low = (x - high.astype(F32)).astype(BF16)
    return high, low


def dot(x, y):
    return jnp.dot(x, y, preferred_element_type=F32)


def pick_ahead(swapped):
    half = swapped.shape[1] // 2
    return jnp.where(
        lane_of(swapped.shape) < half, swapped, pltpu.roll(swapped, swapped.shape[0] - 1, axis=0)
    )


def pick_behind(swapped):
    half = swapped.shape[1] // 2
    return jnp.where(lane_of(swapped.shape) >= half, swapped, pltpu.roll(swapped, 1, axis=0))


def left_transform(stacked, table_ref):
    high, low = halves(stacked)
    depth, width = stacked.shape
    at = 2 * table_ref.shape[1]
    both = dot(
        table_ref[at : at + 2 * depth, : 3 * depth], jnp.concatenate([high, high, low], axis=0)
    )
    even = lane_of((depth, width)) % (2 * depth) < depth
    return jnp.where(even, both[:depth], both[depth:])


def right_transform(high_ref, low_ref, table_ref, out_ref):
    size = table_ref.shape[1]
    high = high_ref[...]
    first = table_ref[:size]
    out_ref[...] = dot(high, first) + dot(low_ref[...], first) + dot(high, table_ref[size : 2 * size])


def forward_transform(d_ref, table_ref, high_ref, low_ref, spec_ref, out_ref, out_any, sems):
    slots, _, half, lanes = d_ref.shape
    parts = out_ref.shape[1] // 4
    rows = half // parts
    size = 4 * half
    for slot in range(slots):
        stacked = jnp.concatenate(
            [
                jnp.concatenate([d_ref[slot, 2 * f], d_ref[slot, 2 * f + 1]], axis=0)
                for f in range(4)
            ],
            axis=1,
        )
        y = left_transform(stacked, table_ref)
        for f in range(4):
            re = y[:half, f * lanes : (f + 1) * lanes]
            im = y[half:, f * lanes : (f + 1) * lanes]
            high, low = halves(jnp.concatenate([re, im], axis=1))
            at = (slot * 4 + f) * half
            high_ref[at : at + half, :] = high
            low_ref[at : at + half, :] = low
    copies = []
    for slot in range(slots):
        rows_of = pl.ds(slot * size, size)
        right_transform(high_ref.at[rows_of], low_ref.at[rows_of], table_ref, spec_ref.at[rows_of])
        for f in range(4):
            for part in range(parts):
                at = (slot * 4 + f) * half + part * rows
                for c in range(2):
                    out_ref[slot, f * parts + part, c * rows : (c + 1) * rows, :] = spec_ref[
                        at : at + rows, c * lanes : (c + 1) * lanes
                    ]
        copies.append(
            pltpu.make_async_copy(
                out_ref.at[slot], out_any.at[:, pl.ds(slot * 2 * rows, 2 * rows), :], sems.at[slot]
            )
        )
        copies[-1].start()
    return copies


def inverse_transform(in_ref, table_ref, high_ref, low_ref, spec_ref, x_ref):
    _, slots, half, lanes = x_ref.shape
    parts = in_ref.shape[0] // 4
    rows = half // parts
    for slot in range(slots):
        for f in range(4):
            columns = []
            for c in range(2):
                to = (slot * 2 + c) * rows
                pieces = [in_ref[f * parts + part, to : to + rows, :] for part in range(parts)]
                columns.append(jnp.concatenate(pieces, axis=0))
            high, low = halves(jnp.concatenate(columns, axis=1))
            at = (slot * 4 + f) * half
            high_ref[at : at + half, :] = high
            low_ref[at : at + half, :] = low
    right_transform(high_ref, low_ref, table_ref, spec_ref)
    for slot in range(slots):
        stacks = []
        for f in range(4):
            at = (slot * 4 + f) * half
            stacks.append(
                jnp.concatenate([spec_ref[at : at + half, :lanes], spec_ref[at : at + half, lanes:]], axis=0)
            )
        y = left_transform(jnp.concatenate(stacks, axis=1), table_ref)
        for f in range(4):
            x_ref[2 * f, slot] = y[:half, f * lanes : (f + 1) * lanes]
            x_ref[2 * f + 1, slot] = y[half:, f * lanes : (f + 1) * lanes]


def site_rows(plane, chunk, planes):
    return pl.ds(chunk * (8 * planes) + plane, 8, stride=planes)


def load_link(links_ref, direction, rows):
    base = direction * 18
    return [
        [(links_ref[base + 3 * i + j, rows, :], links_ref[base + 9 + 3 * i + j, rows, :]) for j in range(3)]
        for i in range(3)
    ]


def load_gauge(ref, plane, rows):
    return [
        [(ref[3 * i + j, plane, rows, :], ref[9 + 3 * i + j, plane, rows, :]) for j in range(3)]
        for i in range(3)
    ]


def store_gauge(ref, plane, rows, matrix):
    for i in range(3):
        for j in range(3):
            ref[3 * i + j, plane, rows, :] = matrix[i][j][0]
            ref[9 + 3 * i + j, plane, rows, :] = matrix[i][j][1]


def chunk_loop(planes, chunks, step):
    def run(index, carry):
        step(index // chunks, index % chunks)
        return carry

    lax.fori_loop(0, planes * chunks, run, 0)


def aligned(chunk):
    return pl.ds(pl.multiple_of(chunk * 8, 8), 8)


def shift_gauge(g_ref, shift, stack_ref, moved_ref, y_ref):
    planes, half, lanes = y_ref.shape[1:]
    for comp in range(18):
        for plane in range(planes):
            at = (comp * planes + plane) * half
            stack_ref[at : at + half, :] = jnp.concatenate(halves(g_ref[comp, plane]), axis=1)
    moved_ref[...] = dot(stack_ref[...], shift)
    for comp in range(18):
        for plane in range(planes):
            at = (comp * planes + plane) * half
            y_ref[comp, plane] = pick_ahead(moved_ref[at : at + half, :lanes])


def load_ahead(direction, g_ref, y_ref, moved_ref, plane, chunk):
    rows = aligned(chunk)
    if direction == 0:
        return load_gauge(g_ref, plane + 1, rows)
    if direction == 1:
        return load_gauge(y_ref, plane, rows)
    planes, half, lanes = y_ref.shape[1:]

    def at(comp):
        return moved_ref[pl.ds(pl.multiple_of((comp * planes + plane) * half + chunk * 8, 8), 8), lanes:]

    return [[(at(3 * i + j), at(9 + 3 * i + j)) for j in range(3)] for i in range(3)]


def divergence(v_ref, shift_ref, stack_ref, moved_ref, rest_ref, d_ref):
    _, comps, planes, half, lanes = v_ref.shape
    size = comps * planes * half
    for direction in (1, 2):
        for comp in range(comps):
            for plane in range(planes):
                at = (direction - 1) * size + (comp * planes + plane) * half
                value = v_ref[direction, comp, plane]
                high, low = halves(value)
                stack_ref[at : at + half, :] = jnp.concatenate([high, low], axis=1)
                rest = (value - high.astype(F32)) - low.astype(F32)
                rest_ref[at : at + half, :] = rest.astype(BF16)
    first = shift_ref.shape[0] - 2 * lanes
    for k in range(2):
        part, columns = slice(k * size, (k + 1) * size), slice(k * lanes, (k + 1) * lanes)
        moved_ref[part, :lanes] = dot(stack_ref[part], shift_ref[first:, columns]) + dot(
            rest_ref[part], shift_ref[first + lanes :, columns]
        )
    for comp in range(comps):
        before = None
        for plane in range(planes):
            at = (comp * planes + plane) * half
            vx = v_ref[0, comp, plane]
            total = (pick_behind(moved_ref[at : at + half, :lanes]) - v_ref[1, comp, plane]) + (
                moved_ref[size + at : size + at + half, :lanes] - v_ref[2, comp, plane]
            )
            total = total - vx
            if before is not None:
                total = total + before
            before = vx
            d_ref[plane, comp] = total
        d_ref[planes, comp] = before


class Split(NamedTuple):
    times: int
    group: int
    wide: int
    near: int

    @property
    def rows(self):
        return self.wide + self.near

    @property
    def offset(self):
        return self.times * self.wide

    @property
    def total(self):
        return self.offset + self.group * self.near

    @property
    def peers(self):
        groups = self.times // self.group
        steps = [(g, m) for g in range(groups) for m in range(self.group)]
        return steps[1:]

    def block(self, step):
        return self.wide if step[0] else self.rows

    def moved(self, device, step, back=False):
        sign = -1 if back else 1
        groups = self.times // self.group
        home = (device // self.group + sign * step[0]) % groups
        return home * self.group + (device % self.group + sign * step[1]) % self.group

    def starts(self, device):
        wide = device * self.wide
        near = self.offset + device % self.group * self.near
        if isinstance(device, int):
            return wide, near
        return pl.multiple_of(wide, 8), pl.multiple_of(near, 8)


def start_kernel(split, links_any, table_any, source_any, out_any, *rest):
    peers = split.peers
    cut_refs, held_refs = rest[: len(peers)], rest[len(peers) : 2 * len(peers)]
    links_ref, table_ref, v_ref, d_ref, rest_ref, stack_ref, moved_ref, high_ref, low_ref, spec_ref, out_ref, sems, cut_sems, out_sems = rest[
        2 * len(peers) :
    ]
    _, _, planes, half, _ = v_ref.shape
    mine = lax.axis_index("tm")
    copies = [
        pltpu.make_async_copy(
            links_any.at[pl.ds(18 * direction, 18)], links_ref.at[pl.ds(18 * direction, 18)], sems.at[direction]
        )
        for direction in range(3)
    ]
    copies.append(pltpu.make_async_copy(table_any, table_ref, sems.at[3]))
    reads, writes = [], []
    for k, (step, cut, held) in enumerate(zip(peers, cut_refs, held_refs)):
        wide, near = split.starts(split.moved(mine, step))
        pieces = [(wide, 0, split.wide)] if step[0] else [(wide, 0, split.wide), (near, split.wide, split.near)]
        for part, (start, to, size) in enumerate(pieces):
            reads.append(
                pltpu.make_async_copy(
                    source_any.at[:, pl.ds(start, size), :], held.at[:, pl.ds(to, size), :], cut_sems.at[part, k]
                )
            )
        writes.append(pltpu.make_async_copy(held, cut, cut_sems.at[2, k]))
    for copy in copies + reads:
        copy.start()
    for direction in range(3):
        copies[direction].wait()

        def step(plane, chunk, direction=direction):
            rows = site_rows(plane, chunk, planes)
            for comp, value in enumerate(project(load_link(links_ref, direction, rows))):
                v_ref[direction, comp, plane, aligned(chunk), :] = value

        chunk_loop(planes, half // 8, step)
    for copy in reads:
        copy.wait()
    for copy in writes:
        copy.start()
    copies[3].wait()
    divergence(v_ref, table_ref, stack_ref, moved_ref, rest_ref, d_ref)
    outs = forward_transform(d_ref, table_ref, high_ref, low_ref, spec_ref, out_ref, out_any, out_sems)
    for copy in writes + outs:
        copy.wait()


def convolve_kernel(planes, in_ref, table_ref, out_ref):
    count = in_ref.shape[0]
    parts, offsets, rows, _ = table_ref.shape
    across = planes * count
    part = lax.axis_index("space") % parts
    step = min(8, rows)

    def run(index, carry):
        c = index // (rows // step)
        chunk = index % (rows // step)

        def at(slot):
            return pl.ds((slot * 2 + c) * rows + chunk * step, step)

        table = [table_ref[part, k, pl.ds(chunk * step, step), :] for k in range(offsets)]
        data = []
        for x in range(across):
            owner, plane = divmod(x, planes)
            value = in_ref[owner, at(plane), :]
            if plane == 0:
                value = value + in_ref[(owner - 1) % count, at(planes), :]
            data.append(value)
        for x in range(across):
            owner, plane = divmod(x, planes)
            total = table[0] * data[x] + table[offsets - 1] * data[(x + across // 2) % across]
            for k in range(1, offsets - 1):
                total = total + table[k] * (data[(x + k) % across] + data[(x - k) % across])
            out_ref[owner, at(plane), :] = total
            if plane == 0:
                out_ref[(owner - 1) % count, at(planes), :] = total
        return carry

    lax.fori_loop(0, 2 * (rows // step), run, 0)


def flatten_shares(x_ref, flat_ref, planes, split):
    half = x_ref.shape[2]
    first = half // 2
    if flat_ref.shape[1] > planes * half:
        flat_ref[...] = jnp.zeros_like(flat_ref)
    for comp in range(8):
        for plane in range(planes):
            value = x_ref[comp, plane]
            flat_ref[comp, pl.ds(plane, first, stride=planes), :] = value[:first]
            flat_ref[comp, pl.ds(split.offset + plane, half - first, stride=planes), :] = value[first:]


def share_copies(flat_ref, share_refs, split, devices, sems):
    copies = []
    for k, (share_ref, device) in enumerate(zip(share_refs, devices)):
        wide, near = split.starts(device)
        copies.append(
            pltpu.make_async_copy(
                flat_ref.at[:, pl.ds(wide, split.wide), :], share_ref.at[:, : split.wide, :], sems.at[0, k]
            )
        )
        copies.append(
            pltpu.make_async_copy(
                flat_ref.at[:, pl.ds(near, split.near), :], share_ref.at[:, split.wide :, :], sems.at[1, k]
            )
        )
    return copies


def middle_kernel(split, in_ref, links_ref, inverse_ref, forward_ref, *rest):
    out_any, x_any = rest[:2]
    share_refs = rest[2 : 2 + split.times]
    x_ref, g_ref, y_ref, v_ref, d_ref, rest_ref, stack_ref, moved_ref, high_ref, low_ref, spec_ref, flat_ref, out_ref, sems, share_sems, out_sems = rest[2 + split.times :]
    _, slots, half, _ = x_ref.shape
    planes = slots - 1
    inverse_transform(in_ref, inverse_ref, high_ref, low_ref, spec_ref, x_ref)
    flatten_shares(x_ref, flat_ref, planes, split)
    mine = lax.axis_index("tm")
    devices = [(mine + shift) % split.times for shift in range(split.times)]
    copies = share_copies(flat_ref, share_refs, split, devices, share_sems)
    copies.append(pltpu.make_async_copy(x_ref, x_any, sems))
    for copy in copies:
        copy.start()

    def raise_step(plane, chunk):
        rows = aligned(chunk)
        store_gauge(g_ref, plane, rows, exponential([x_ref[k, plane, rows, :] for k in range(8)]))

    chunk_loop(slots, half // 8, raise_step)
    lanes = x_ref.shape[3]
    shift_gauge(g_ref, inverse_ref[inverse_ref.shape[0] - 2 * lanes :], stack_ref, moved_ref, y_ref)

    def rotate_step(plane, chunk):
        rows = aligned(chunk)
        gauge = load_gauge(g_ref, plane, rows)
        link_rows = site_rows(plane, chunk, planes)
        for direction in range(3):
            link = load_link(links_ref, direction, link_rows)
            ahead = load_ahead(direction, g_ref, y_ref, moved_ref, plane, chunk)
            turned = [row_times_dagger(row_times(gauge[i], link), ahead) for i in range(3)]
            for comp, value in enumerate(project(turned)):
                v_ref[direction, comp, plane, rows, :] = value

    chunk_loop(planes, half // 8, rotate_step)
    divergence(v_ref, forward_ref, stack_ref, moved_ref, rest_ref, d_ref)
    copies += forward_transform(
        d_ref, forward_ref, high_ref, low_ref, spec_ref, out_ref, out_any, out_sems
    )
    for copy in copies:
        copy.wait()


def last_transform_kernel(split, in_ref, inverse_ref, x_ref, *rest):
    share_refs = rest[: split.times]
    high_ref, low_ref, spec_ref, flat_ref = rest[split.times :]
    inverse_transform(in_ref, inverse_ref, high_ref, low_ref, spec_ref, x_ref)
    flatten_shares(x_ref, flat_ref, x_ref.shape[1] - 1, split)
    for device, share_ref in enumerate(share_refs):
        wide, near = split.starts(device)
        share_ref[:, : split.wide, :] = flat_ref[:, wide : wide + split.wide, :]
        share_ref[:, split.wide :, :] = flat_ref[:, near : near + split.near, :]


def total_of(first, second):
    earlier = exponential(first)
    later = exponential(second)
    return [row_times(later[i], earlier) for i in range(3)]


def finish_kernel(links_any, first_any, table_any, second_ref, out_any, g_ref, y_ref, stack_ref, moved_ref, links_ref, first_ref, shift_ref, out_ref, sems):
    _, slots, half, lanes = first_ref.shape
    planes = slots - 1
    chunks = half // 8
    copies = [
        pltpu.make_async_copy(first_any, first_ref, sems.at[0]),
        pltpu.make_async_copy(links_any, links_ref, sems.at[1]),
        pltpu.make_async_copy(
            table_any.at[pl.ds(table_any.shape[0] - 2 * lanes, 2 * lanes)], shift_ref, sems.at[2]
        ),
    ]
    for copy in copies:
        copy.start()
    copies[0].wait()

    def raise_step(plane, chunk):
        rows = aligned(chunk)
        store_gauge(
            g_ref,
            plane,
            rows,
            total_of(
                [first_ref[k, plane, rows, :] for k in range(8)],
                [second_ref[k, plane, rows, :] for k in range(8)],
            ),
        )

    chunk_loop(slots, half // 8, raise_step)
    copies[2].wait()
    shift_gauge(g_ref, shift_ref[...], stack_ref, moved_ref, y_ref)
    copies[1].wait()

    def piece(chunk):
        rows = pl.ds(pl.multiple_of(chunk * (8 * planes), 8), 8 * planes)
        return pltpu.make_async_copy(out_ref.at[:, rows, :], out_any.at[:, rows, :], sems.at[3 + chunk])

    def rotate_step(chunk, plane):
        rows = aligned(chunk)
        gauge = load_gauge(g_ref, plane, rows)
        link_rows = site_rows(plane, chunk, planes)
        for direction in range(3):
            link = load_link(links_ref, direction, link_rows)
            ahead = load_ahead(direction, g_ref, y_ref, moved_ref, plane, chunk)
            for i in range(3):
                row = row_times_dagger(row_times(gauge[i], link), ahead)
                for j in range(3):
                    out_ref[direction * 18 + 3 * i + j, link_rows, :] = row[j][0]
                    out_ref[direction * 18 + 9 + 3 * i + j, link_rows, :] = row[j][1]

        @pl.when(plane == planes - 1)
        def _():
            piece(chunk).start()

    chunk_loop(chunks, planes, rotate_step)

    for chunk in range(chunks):
        piece(chunk).wait()


def lane_sums(rows):
    ones = jnp.ones((8, rows.shape[1]), BF16)
    total = None
    rest = rows
    for _ in range(3):
        piece = rest.astype(BF16)
        rest = rest - piece.astype(F32)
        part = lax.dot_general(ones, piece, (((1,), (1,)), ((), ())), preferred_element_type=F32)
        total = part if total is None else total + part
    return total


def load_rows(ref, rows):
    return [[(ref[3 * i + j, rows, :], ref[9 + 3 * i + j, rows, :]) for j in range(3)] for i in range(3)]


def sink_kernel(split, sink_ref, src_time_ref, src_site_ref, first_any, second_ref, source_ref, own_early_any, *rest):
    times, group, per = split.times, split.group, split.rows
    rest = list(rest)

    def take(count):
        taken = rest[:count]
        del rest[:count]
        return taken

    early = [own_early_any] + take(times - 1)
    own, late = take(times), take(times - 1)
    partners_any = take(times - 1)
    out_ref, near_ref, wide_ref, x_ref, gauge_ref, sum_ref, before_ref, anchor_ref, sems = rest
    pairs = source_ref.shape[0] // 2
    groups = pairs // 3
    _, slots, half, lanes = second_ref.shape
    planes = slots - 1
    mine = lax.axis_index("tm")
    sink = sink_ref[0]
    column = src_site_ref[0] % (half * lanes)
    plane = src_site_ref[0] // (half * lanes) - lax.axis_index("space") * planes
    present = (src_time_ref[0] == mine) & (plane >= 0) & (plane < planes)
    safe = jnp.clip(plane, 0, planes - 1)
    row = column // lanes
    block = pl.ds(pl.multiple_of(row // 8 * 8, 8), 8)
    before = pltpu.make_async_copy(first_any.at[:, safe, block, :], before_ref, sems.at[0])
    fetches = [pltpu.make_async_copy(early[0], x_ref.at[k], sems.at[1 + k]) for k in range(2)]
    held = [near_ref.at[k] for k in range(group - 1)] + [wide_ref.at[k] for k in range(times - group)]
    partners = [
        pltpu.make_async_copy(partner, to, sems.at[3 + k])
        for k, (partner, to) in enumerate(zip(partners_any, held))
    ]

    def fetch(condition, value, to):
        @pl.when(condition)
        def _():
            pltpu.make_async_copy(value, x_ref.at[to], sems.at[1 + to]).start()

    for shift in range(times):
        fetch((mine - sink) % times == shift, early[shift], 0)
    for at in range(times):
        fetch((mine == sink) & (mine == at), own[at], 1)
    for at in range(times - 1):
        fetch((mine != sink) & (jnp.where(mine > sink, mine - 1, mine) == at), late[at], 1)
    for copy in partners:
        copy.start()
    before.start()
    chunks = per // 8
    for number in range(2):
        fetches[number].wait()
        for chunk in range(chunks):
            rows = slice(chunk * 8, chunk * 8 + 8)
            turn = exponential([x_ref[number, k, rows, :] for k in range(8)])
            if number:
                turn = [row_times(turn[i], load_rows(gauge_ref, rows)) for i in range(3)]
            for i in range(3):
                for j in range(3):
                    gauge_ref[3 * i + j, rows, :] = turn[i][j][0]
                    gauge_ref[9 + 3 * i + j, rows, :] = turn[i][j][1]

    def accumulate(block_ref, offset, first, count, source_device, add):
        base = source_device * pairs

        def run(group_at, carry):
            sums = [None] * 3
            for chunk in range(count // 8):
                rows = slice(first + chunk * 8, first + chunk * 8 + 8)
                own_rows = pl.ds(pl.multiple_of(offset + chunk * 8, 8), 8)
                column = [
                    (
                        block_ref[3 * group_at + c, own_rows, :],
                        block_ref[pairs + 3 * group_at + c, own_rows, :],
                    )
                    for c in range(3)
                ]
                for a in range(3):
                    for c in range(3):
                        part = cmul(
                            (gauge_ref[3 * a + c, rows, :], gauge_ref[9 + 3 * a + c, rows, :]), column[c]
                        )
                        sums[a] = part if sums[a] is None else (sums[a][0] + part[0], sums[a][1] + part[1])
            for a in range(3):
                to = pl.ds(pl.multiple_of((base + 3 * group_at + a) * 8, 8), 8)
                re, im = sums[a]
                if add:
                    re, im = re + sum_ref[0, to, :], im + sum_ref[1, to, :]
                sum_ref[0, to, :] = re
                sum_ref[1, to, :] = im
            return carry

        lax.fori_loop(0, groups, run, 0, unroll=2 if groups % 2 == 0 else 1)

    wide_start, near_start = split.starts(mine)
    accumulate(source_ref, wide_start, 0, split.wide, mine, False)
    accumulate(source_ref, near_start, split.wide, split.near, mine, True)
    for k, step in enumerate(split.peers):
        partners[k].wait()
        owner = split.moved(mine, step, back=True)
        accumulate(held[k], 0, 0, split.block(step), owner, False)
    before.wait()
    total = total_of([before_ref[k] for k in range(8)], [second_ref[k, safe, block, :] for k in range(8)])
    wide = (8, lanes)
    keep = (lane_of(wide) == jnp.where(present, column % lanes, -1)) & (
        lax.broadcasted_iota(jnp.int32, wide, 0) == row % 8
    )
    anchor_ref[...] = jnp.zeros_like(anchor_ref)
    for k in range(18):
        value = total[k % 9 // 3][k % 3][k // 9]
        anchor_ref[k : k + 1, :] = jnp.sum(jnp.where(keep, value, 0.0), axis=0, keepdims=True)
    whole = SC * SC
    width = -(-(whole + 24) // lanes) * lanes
    pieces = []
    for part in range(2):
        total = sum_ref[part, pl.ds(0, whole, stride=8), :]
        for k in range(1, 8):
            total = total + sum_ref[part, pl.ds(k, whole, stride=8), :]
        extra = anchor_ref[...] if part == 0 else jnp.zeros((24, lanes), F32)
        pieces += [total, extra, jnp.zeros((width - whole - 24, lanes), F32)]
    sums = lane_sums(jnp.concatenate(pieces, axis=0))
    block = jnp.concatenate(
        [sums[0:1, k * lanes : (k + 1) * lanes] for k in range(2 * width // lanes)], axis=0
    )

    def spread(index, carry):
        out_ref[index] = block
        return carry

    lax.fori_loop(0, out_ref.shape[0], spread, 0)


def wall_kernel(scale, in_ref, out_ref):
    whole = SC * SC
    total = jnp.sum(in_ref[...], axis=0)
    half = total.shape[0] // 2
    re = jnp.concatenate([total[k : k + 1] for k in range(half)], axis=1)
    im = jnp.concatenate([total[half + k : half + k + 1] for k in range(half)], axis=1)
    width = re.shape[1]
    colour = lane_of((1, width)) // SC % 3
    out_re = jnp.zeros((1, width), F32)
    out_im = jnp.zeros((1, width), F32)
    for b in range(3):
        for c in range(3):
            at = whole + 3 * b + c
            ar = re[:, at : at + 1]
            ai = re[:, at + 9 : at + 10]
            amount = (SC * (b - c)) % width
            wr = pltpu.roll(re, amount, axis=1) if amount else re
            wi = pltpu.roll(im, amount, axis=1) if amount else im
            here = colour == b
            out_re = out_re + jnp.where(here, wr * ar + wi * ai, 0.0)
            out_im = out_im + jnp.where(here, wi * ar - wr * ai, 0.0)
    out_ref[0:1, :] = out_re[:, :whole] * scale
    out_ref[1:2, :] = out_im[:, :whole] * scale


def shape(*dims):
    return jax.ShapeDtypeStruct(dims, F32)


SMEM_SPEC = pl.BlockSpec(memory_space=pltpu.SMEM)
VMEM_SPEC = pl.BlockSpec(memory_space=pltpu.VMEM)
ANY_SPEC = pl.BlockSpec(memory_space=pl.ANY)
HBM_SPEC = pl.BlockSpec(memory_space=pltpu.HBM)


def call(kernel, outs, out_specs, inputs, in_specs, scratch):
    inputs = [
        pltpu.with_memory_space_constraint(x, pltpu.HBM) if spec is HBM_SPEC else x
        for x, spec in zip(inputs, in_specs)
    ]
    outs = [
        pltpu.HBM(out.shape, out.dtype) if spec is HBM_SPEC else out
        for out, spec in zip(outs, out_specs)
    ]
    return pl.pallas_call(
        kernel,
        out_shape=outs,
        in_specs=in_specs,
        out_specs=out_specs,
        scratch_shapes=scratch,
        compiler_params=pltpu.CompilerParams(vmem_limit_bytes=20 * 1024 * 1024),
    )(*inputs)


def body(links, propagator, sink_time, src_time, src_site):
    count = lax.axis_size("space")
    times = lax.axis_size("tm")
    planes = links.shape[5]
    side = math.isqrt(links.shape[6])
    half, lanes = side // 2, 2 * side
    across = planes * count
    slots = planes + 1
    parts = count // 4
    rows = half // parts
    sites = planes * half
    group = 2 if times % 2 == 0 else 1
    spread = sites // 2
    split = Split(times, group, 8 * -(-spread // (8 * times)), 8 * -(-(sites - spread) // (8 * group)))
    pairs = propagator.shape[1]

    forward = jnp.asarray(transform_table(side, False))
    inverse = jnp.asarray(transform_table(side, True))
    table = jnp.asarray(filter_table(side, across, parts))

    def interleave(array, lead):
        return array.reshape(lead, planes, half, lanes).transpose(0, 2, 1, 3).reshape(lead, sites, lanes)

    lattice = interleave(links, 54)

    def forwarded(value, shift):
        return lax.ppermute(value, "tm", [(i, (i + shift) % times) for i in range(times)])

    spectrum_shape = shape(count, slots * 2 * rows, lanes)
    transform_scratch = [
        VMEM((4 * slots * half, 2 * lanes), BF16),
        VMEM((4 * slots * half, 2 * lanes), BF16),
        VMEM((4 * slots * half, 2 * lanes), F32),
    ]
    divergence_scratch = [
        VMEM((3, 8, planes, half, lanes), F32),
        VMEM((slots, 8, half, lanes), F32),
        VMEM((16 * planes * half, lanes), BF16),
    ]
    gauge_scratch = [
        VMEM((18, slots, half, lanes), F32),
        VMEM((18, planes, half, lanes), F32),
    ]
    shift_scratch = [
        VMEM((18 * planes * half, 2 * lanes), BF16),
        VMEM((18 * planes * half, 2 * lanes), F32),
    ]
    out_scratch = [VMEM((slots, count, 2 * rows, lanes), F32)]
    flat_scratch = [VMEM((8, split.total, lanes), F32)]
    algebra_shape = shape(8, slots, half, lanes)
    share_shapes = [shape(8, split.rows, lanes)] * times

    def turn(spectrum):
        return lax.all_to_all(spectrum, "space", 0, 0, tiled=True)

    def convolve(spectrum):
        (out,) = call(
            functools.partial(convolve_kernel, planes),
            [spectrum_shape],
            [VMEM_SPEC],
            [spectrum, table],
            [VMEM_SPEC] * 2,
            [],
        )
        return out

    source = interleave(propagator, 2 * pairs)
    if split.total > sites:
        fill = jnp.zeros((2 * pairs, split.offset - spread, lanes), F32)
        source = jnp.concatenate([source[:, :spread], fill, source[:, spread:]], axis=1)
    scalars = [sink_time % times, src_time % times, jnp.maximum(src_site, 0)]
    cut_shapes = [shape(2 * pairs, split.block(step), lanes) for step in split.peers]
    spectrum, *cuts = call(
        functools.partial(start_kernel, split),
        [spectrum_shape] + cut_shapes,
        [HBM_SPEC] * times,
        [lattice, forward, source],
        [HBM_SPEC] * 3,
        [VMEM(cut.shape, F32) for cut in cut_shapes]
        + [VMEM(lattice.shape, F32), VMEM(forward.shape, BF16)]
        + divergence_scratch
        + shift_scratch
        + transform_scratch
        + out_scratch
        + [
            pltpu.SemaphoreType.DMA((4,)),
            pltpu.SemaphoreType.DMA((3, times - 1)),
            pltpu.SemaphoreType.DMA((slots,)),
        ],
    )
    held_scratch = [
        VMEM((max(1, group - 1), 2 * pairs, split.rows, lanes), F32),
        VMEM((max(1, times - group), 2 * pairs, split.wide, lanes), F32),
    ]
    scalars = [sink_time % times, src_time % times, jnp.maximum(src_site, 0)]
    sources = [
        lax.ppermute(cut, "tm", [(i, split.moved(i, step)) for i in range(times)])
        for step, cut in zip(split.peers, cuts)
    ]

    spectrum = turn(spectrum)
    spectrum = convolve(spectrum)
    spectrum = turn(spectrum)
    spectrum, first, *early = call(
        functools.partial(middle_kernel, split),
        [spectrum_shape, algebra_shape] + share_shapes,
        [HBM_SPEC] * (2 + times),
        [spectrum, lattice, inverse, forward],
        [VMEM_SPEC] * 4,
        [VMEM(algebra_shape.shape, F32)]
        + gauge_scratch
        + divergence_scratch
        + shift_scratch
        + transform_scratch
        + flat_scratch
        + out_scratch
        + [
            pltpu.SemaphoreType.DMA,
            pltpu.SemaphoreType.DMA((2, times)),
            pltpu.SemaphoreType.DMA((slots,)),
        ],
    )
    first_shares = [forwarded(early[shift], shift) for shift in range(1, times)]
    spectrum = turn(spectrum)
    spectrum = convolve(spectrum)
    spectrum = turn(spectrum)
    second, *shares = call(
        functools.partial(last_transform_kernel, split),
        [algebra_shape] + share_shapes,
        [VMEM_SPEC] * (1 + times),
        [spectrum, inverse],
        [VMEM_SPEC] * 2,
        transform_scratch + flat_scratch,
    )

    def sent_from(source_index):
        def send(*blocks):
            return tuple(
                lax.ppermute(blocks[to], "tm", [(source_index, to)])
                for to in range(times)
                if to != source_index
            )

        return send

    second_shares = lax.switch(sink_time[0] % times, [sent_from(k) for k in range(times)], *shares)
    (fixed,) = call(
        finish_kernel,
        [shape(54, sites, lanes)],
        [HBM_SPEC],
        [lattice, first, inverse, second],
        [HBM_SPEC] * 3 + [VMEM_SPEC],
        gauge_scratch
        + shift_scratch
        + [
            VMEM(lattice.shape, F32),
            VMEM(algebra_shape.shape, F32),
            VMEM((2 * lanes, 2 * lanes), BF16),
            VMEM(lattice.shape, F32),
            pltpu.SemaphoreType.DMA((3 + half // 8,)),
        ],
    )
    width = -(-(SC * SC + 24) // lanes)
    devices = count * times
    (payload,) = call(
        functools.partial(sink_kernel, split),
        [shape(devices, 2 * width, lanes)],
        [VMEM_SPEC],
        scalars + [first, second, source, early[0]] + first_shares + shares + list(second_shares) + sources,
        [SMEM_SPEC] * 3
        + [HBM_SPEC]
        + [VMEM_SPEC] * 2
        + [HBM_SPEC]
        + [ANY_SPEC] * (2 * times - 1)
        + [HBM_SPEC] * (2 * times - 2),
        held_scratch
        + [
            VMEM((2, 8, split.rows, lanes), F32),
            VMEM((18, split.rows, lanes), F32),
            VMEM((2, SC * SC * 8, lanes), F32),
            VMEM((8, 8, lanes), F32),
            VMEM((24, lanes), F32),
            pltpu.SemaphoreType.DMA((2 + times,)),
        ],
    )
    gathered = lax.all_to_all(payload, ("space", "tm"), 0, 0, tiled=True)
    scale = float(across * side * side) ** (-0.5)
    (wall,) = call(functools.partial(wall_kernel, scale), [shape(2, SC * SC)], [VMEM_SPEC], [gathered], [VMEM_SPEC], [])
    fixed = fixed.reshape(54, half, planes, lanes).transpose(0, 2, 1, 3).reshape(links.shape)
    return fixed, wall


def solution(mesh):
    placed = (
        P("tm", None, None, None, None, "space", None),
        P(None, "tm", "space", None),
        P(),
        P(),
        P(),
    )
    return jax.shard_map(
        body,
        mesh=mesh,
        in_specs=placed,
        out_specs=(P("tm", None, None, None, None, "space", None), P()),
        check_vma=False,
    )
```

```python
import functools
import math
from typing import NamedTuple

import jax
import jax.numpy as jnp
import numpy as np
from jax import lax
from jax.experimental import pallas as pl
from jax.experimental.pallas import tpu as pltpu
from jax.sharding import PartitionSpec as P


SC = 12
STEP_SIZE = 0.08
PEAK_SQUARE = 12.0
F32 = jnp.float32
BF16 = jnp.bfloat16
VMEM = pltpu.VMEM
PAIRS = ((0, 1), (0, 2), (1, 2))


def split_table(table):
    high = table.astype(jnp.bfloat16)
    low = (table - high.astype(np.float64)).astype(jnp.bfloat16)
    return high, low


def as_real(real, imag):
    return np.block([[real, imag], [-imag, real]])


@functools.lru_cache(None)
def transform_table(side, inverse):
    half = side // 2
    sign = 1.0 if inverse else -1.0
    k = np.arange(half)
    twist = np.exp(1j * sign * 2.0 * np.pi * k / side)
    even = np.exp(1j * sign * 2.0 * np.pi * np.outer(k, k) / half)
    odd = even * (twist[None, :] if inverse else twist[:, None])
    left = np.concatenate([as_real(m.real, -m.imag) for m in (even, odd)], axis=0)
    high, low = split_table(left)
    fill = np.zeros((left.shape[0], 4 * side - 3 * side), high.dtype)
    left = np.concatenate([high, low, high, fill], axis=1)
    z = np.arange(side)
    depth_phase = sign * 2.0 * np.pi * np.outer(z, z) / side
    parity = np.array([[1.0, 1.0], [1.0, -1.0]])
    right = as_real(np.kron(parity, np.cos(depth_phase)), np.kron(parity, np.sin(depth_phase)))
    high, low = split_table(right)
    lanes = np.arange(2 * side)
    from_depth = lanes - lanes % side + (lanes + (1 if inverse else -1)) % side
    moves = [np.eye(2 * side)[:, (lanes + side) % (2 * side)], np.eye(2 * side)[:, from_depth]]
    shift = np.concatenate(moves, axis=1)
    shift = np.concatenate([shift, shift], axis=0).astype(high.dtype)
    return np.concatenate([high, low, left, shift], axis=0)


@functools.lru_cache(None)
def filter_table(side, across, blocks):
    half = side // 2
    squares = 4.0 * np.sin(np.pi * np.arange(side) / side) ** 2
    squares_across = 4.0 * np.sin(np.pi * np.arange(across) / across) ** 2
    column = (squares[:, None] + squares[None, :]).reshape(2, half, side)
    column = np.swapaxes(column, 0, 1).reshape(half, 2 * side)
    momentum = squares_across[:, None, None] + column[None]
    weight = np.where(momentum > 0.0, PEAK_SQUARE / np.where(momentum > 0.0, momentum, 1.0), 0.0)
    offsets = np.arange(across // 2 + 1)
    phase = np.cos(2.0 * np.pi * np.outer(offsets, np.arange(across)) / across)
    table = np.einsum("dk,krl->drl", phase, weight) / (across * side * side)
    table = table * (STEP_SIZE / 16.0)
    table = table.reshape(len(offsets), blocks, half // blocks, 2 * side)
    return np.ascontiguousarray(np.swapaxes(table, 0, 1)).astype(np.float32)


def cmul(x, y):
    return x[0] * y[0] - x[1] * y[1], x[0] * y[1] + x[1] * y[0]


def csquare(x):
    return x[0] * x[0] - x[1] * x[1], 2.0 * (x[0] * x[1])


def row_times(row, matrix):
    out = []
    for b in range(3):
        re = row[0][0] * matrix[0][b][0] - row[0][1] * matrix[0][b][1]
        im = row[0][0] * matrix[0][b][1] + row[0][1] * matrix[0][b][0]
        for k in (1, 2):
            re = re + row[k][0] * matrix[k][b][0] - row[k][1] * matrix[k][b][1]
            im = im + row[k][0] * matrix[k][b][1] + row[k][1] * matrix[k][b][0]
        out.append((re, im))
    return out


def row_times_dagger(row, matrix):
    out = []
    for b in range(3):
        re = row[0][0] * matrix[b][0][0] + row[0][1] * matrix[b][0][1]
        im = row[0][1] * matrix[b][0][0] - row[0][0] * matrix[b][0][1]
        for k in (1, 2):
            re = re + row[k][0] * matrix[b][k][0] + row[k][1] * matrix[b][k][1]
            im = im + row[k][1] * matrix[b][k][0] - row[k][0] * matrix[b][k][1]
        out.append((re, im))
    return out


def exponential(x):
    t0, t1 = x[0], x[1]
    a, b, e = (x[2], x[3]), (x[4], x[5]), (x[6], x[7])
    t2 = -(t0 + t1)
    na = a[0] * a[0] + a[1] * a[1]
    nb = b[0] * b[0] + b[1] * b[1]
    ne = e[0] * e[0] + e[1] * e[1]
    s0, s1, s2 = t0 * t0, t1 * t1, t2 * t2
    ae = cmul(a, e)
    c = -(0.5 * (s0 + s1 + s2) + (na + nb + ne))
    cross = ae[1] * b[0] - ae[0] * b[1]
    d = t0 * ne + t1 * nb + t2 * na - t0 * t1 * t2 - 2.0 * cross
    c30 = c * (1.0 / 30.0)
    q0 = (None, d * (1.0 / 120.0))
    q1 = ((1.0 + c30) * 0.25, None)
    q2r = 1.0 / 20.0
    n0i = d * (q2r / 3.0)
    n1 = ((1.0 + c * q2r) * (1.0 / 3.0), q0[1] * (1.0 / 3.0))
    n2r = q1[0] * (1.0 / 3.0)
    m0 = (None, d * (0.5 * n2r))
    m1 = (0.5 + 0.5 * (c * n2r), 0.5 * n0i)
    m2 = (0.5 * n1[0], 0.5 * n1[1])
    q0 = (1.0 - d * m2[1], d * m2[0])
    q1 = (1.0 + c * m2[0], m0[1] + c * m2[1])
    q2 = m1
    for _ in range(3):
        q12 = cmul(q1, q2)
        q22 = csquare(q2)
        q00 = csquare(q0)
        q11 = csquare(q1)
        q01 = cmul(q0, q1)
        q02 = cmul(q0, q2)
        d2 = 2.0 * d
        q0 = (q00[0] - d2 * q12[1], q00[1] + d2 * q12[0])
        q1 = (
            2.0 * (q01[0] + c * q12[0]) - d * q22[1],
            2.0 * (q01[1] + c * q12[1]) + d * q22[0],
        )
        q2 = (q11[0] + 2.0 * q02[0] + c * q22[0], q11[1] + 2.0 * q02[1] + c * q22[1])
    u, v = q1
    s, t = q2
    result = [[None] * 3 for _ in range(3)]
    for at, (theta, m) in enumerate(
        ((t0, -(s0 + na + nb)), (t1, -(s1 + na + ne)), (t2, -(s2 + nb + ne)))
    ):
        result[at][at] = (q0[0] - v * theta + s * m, q0[1] + u * theta + t * m)
    y01 = (t2 * a[1] - (b[0] * e[0] + b[1] * e[1]), -t2 * a[0] - (b[1] * e[0] - b[0] * e[1]))
    y02 = (t1 * b[1] + ae[0], -t1 * b[0] + ae[1])
    y12 = (t0 * e[1] - (a[0] * b[0] + a[1] * b[1]), -t0 * e[0] - (a[0] * b[1] - a[1] * b[0]))
    for (i, j), xx, yy in zip(PAIRS, (a, b, e), (y01, y02, y12)):
        ur, vi, ui, vr = u * xx[0], v * xx[1], u * xx[1], v * xx[0]
        sr, ti, si, tr = s * yy[0], t * yy[1], s * yy[1], t * yy[0]
        result[i][j] = ((ur - vi) + (sr - ti), (ui + vr) + (si + tr))
        result[j][i] = ((sr + ti) - (ur + vi), (tr - si) + (ui - vr))
    return result


def project(rows):
    third = (rows[0][0][1] + rows[1][1][1] + rows[2][2][1]) * (1.0 / 3.0)
    out = [rows[0][0][1] - third, rows[1][1][1] - third]
    for i, j in PAIRS:
        out.append(0.5 * (rows[i][j][0] - rows[j][i][0]))
        out.append(0.5 * (rows[i][j][1] + rows[j][i][1]))
    return out


def lane_of(shape):
    return lax.broadcasted_iota(jnp.int32, shape, 1)


def halves(x):
    high = x.astype(BF16)
    low = (x - high.astype(F32)).astype(BF16)
    return high, low


def dot(x, y):
    return jnp.dot(x, y, preferred_element_type=F32)


def pick_ahead(swapped):
    half = swapped.shape[1] // 2
    return jnp.where(
        lane_of(swapped.shape) < half, swapped, pltpu.roll(swapped, swapped.shape[0] - 1, axis=0)
    )


def pick_behind(swapped):
    half = swapped.shape[1] // 2
    return jnp.where(lane_of(swapped.shape) >= half, swapped, pltpu.roll(swapped, 1, axis=0))


def left_transform(stacked, table_ref):
    high, low = halves(stacked)
    depth, width = stacked.shape
    at = 2 * table_ref.shape[1]
    both = dot(
        table_ref[at : at + 2 * depth, : 3 * depth], jnp.concatenate([high, high, low], axis=0)
    )
    even = lane_of((depth, width)) % (2 * depth) < depth
    return jnp.where(even, both[:depth], both[depth:])


def right_transform(high_ref, low_ref, table_ref, out_ref):
    size = table_ref.shape[1]
    high = high_ref[...]
    first = table_ref[:size]
    out_ref[...] = dot(high, first) + dot(low_ref[...], first) + dot(high, table_ref[size : 2 * size])


def forward_transform(d_ref, table_ref, high_ref, low_ref, spec_ref, out_ref, out_any, sems):
    slots, _, half, lanes = d_ref.shape
    parts = out_ref.shape[1] // 4
    rows = half // parts
    size = 4 * half
    for slot in range(slots):
        stacked = jnp.concatenate(
            [
                jnp.concatenate([d_ref[slot, 2 * f], d_ref[slot, 2 * f + 1]], axis=0)
                for f in range(4)
            ],
            axis=1,
        )
        y = left_transform(stacked, table_ref)
        for f in range(4):
            re = y[:half, f * lanes : (f + 1) * lanes]
            im = y[half:, f * lanes : (f + 1) * lanes]
            high, low = halves(jnp.concatenate([re, im], axis=1))
            at = (slot * 4 + f) * half
            high_ref[at : at + half, :] = high
            low_ref[at : at + half, :] = low
    copies = []
    for slot in range(slots):
        rows_of = pl.ds(slot * size, size)
        right_transform(high_ref.at[rows_of], low_ref.at[rows_of], table_ref, spec_ref.at[rows_of])
        for f in range(4):
            for part in range(parts):
                at = (slot * 4 + f) * half + part * rows
                for c in range(2):
                    out_ref[slot, f * parts + part, c * rows : (c + 1) * rows, :] = spec_ref[
                        at : at + rows, c * lanes : (c + 1) * lanes
                    ]
        copies.append(
            pltpu.make_async_copy(
                out_ref.at[slot], out_any.at[:, pl.ds(slot * 2 * rows, 2 * rows), :], sems.at[slot]
            )
        )
        copies[-1].start()
    return copies


def inverse_transform(in_ref, table_ref, high_ref, low_ref, spec_ref, x_ref):
    _, slots, half, lanes = x_ref.shape
    parts = in_ref.shape[0] // 4
    rows = half // parts
    for slot in range(slots):
        for f in range(4):
            columns = []
            for c in range(2):
                to = (slot * 2 + c) * rows
                pieces = [in_ref[f * parts + part, to : to + rows, :] for part in range(parts)]
                columns.append(jnp.concatenate(pieces, axis=0))
            high, low = halves(jnp.concatenate(columns, axis=1))
            at = (slot * 4 + f) * half
            high_ref[at : at + half, :] = high
            low_ref[at : at + half, :] = low
    right_transform(high_ref, low_ref, table_ref, spec_ref)
    for slot in range(slots):
        stacks = []
        for f in range(4):
            at = (slot * 4 + f) * half
            stacks.append(
                jnp.concatenate([spec_ref[at : at + half, :lanes], spec_ref[at : at + half, lanes:]], axis=0)
            )
        y = left_transform(jnp.concatenate(stacks, axis=1), table_ref)
        for f in range(4):
            x_ref[2 * f, slot] = y[:half, f * lanes : (f + 1) * lanes]
            x_ref[2 * f + 1, slot] = y[half:, f * lanes : (f + 1) * lanes]


def site_rows(plane, chunk, planes):
    return pl.ds(chunk * (8 * planes) + plane, 8, stride=planes)


def load_link(links_ref, direction, rows):
    base = direction * 18
    return [
        [(links_ref[base + 3 * i + j, rows, :], links_ref[base + 9 + 3 * i + j, rows, :]) for j in range(3)]
        for i in range(3)
    ]


def load_gauge(ref, plane, rows):
    return [
        [(ref[3 * i + j, plane, rows, :], ref[9 + 3 * i + j, plane, rows, :]) for j in range(3)]
        for i in range(3)
    ]


def store_gauge(ref, plane, rows, matrix):
    for i in range(3):
        for j in range(3):
            ref[3 * i + j, plane, rows, :] = matrix[i][j][0]
            ref[9 + 3 * i + j, plane, rows, :] = matrix[i][j][1]


def chunk_loop(planes, chunks, step, unroll=1):
    def run(index, carry):
        step(index // chunks, index % chunks)
        return carry

    lax.fori_loop(0, planes * chunks, run, 0, unroll=unroll if planes * chunks % unroll == 0 else 1)


def aligned(chunk):
    return pl.ds(pl.multiple_of(chunk * 8, 8), 8)


def shift_gauge(g_ref, shift, stack_ref, moved_ref, y_ref):
    planes, half, lanes = y_ref.shape[1:]
    for comp in range(18):
        for plane in range(planes):
            at = (comp * planes + plane) * half
            stack_ref[at : at + half, :] = jnp.concatenate(halves(g_ref[comp, plane]), axis=1)
    moved_ref[...] = dot(stack_ref[...], shift)
    for comp in range(18):
        for plane in range(planes):
            at = (comp * planes + plane) * half
            y_ref[comp, plane] = pick_ahead(moved_ref[at : at + half, :lanes])


def load_ahead(direction, g_ref, y_ref, moved_ref, plane, chunk):
    rows = aligned(chunk)
    if direction == 0:
        return load_gauge(g_ref, plane + 1, rows)
    if direction == 1:
        return load_gauge(y_ref, plane, rows)
    planes, half, lanes = y_ref.shape[1:]

    def at(comp):
        return moved_ref[pl.ds(pl.multiple_of((comp * planes + plane) * half + chunk * 8, 8), 8), lanes:]

    return [[(at(3 * i + j), at(9 + 3 * i + j)) for j in range(3)] for i in range(3)]


def divergence(v_ref, shift_ref, stack_ref, moved_ref, rest_ref, d_ref):
    _, comps, planes, half, lanes = v_ref.shape
    size = comps * planes * half
    for direction in (1, 2):
        for comp in range(comps):
            for plane in range(planes):
                at = (direction - 1) * size + (comp * planes + plane) * half
                value = v_ref[direction, comp, plane]
                high, low = halves(value)
                stack_ref[at : at + half, :] = jnp.concatenate([high, low], axis=1)
                rest = (value - high.astype(F32)) - low.astype(F32)
                rest_ref[at : at + half, :] = rest.astype(BF16)
    first = shift_ref.shape[0] - 2 * lanes
    for k in range(2):
        part, columns = slice(k * size, (k + 1) * size), slice(k * lanes, (k + 1) * lanes)
        moved_ref[part, :lanes] = dot(stack_ref[part], shift_ref[first:, columns]) + dot(
            rest_ref[part], shift_ref[first + lanes :, columns]
        )
    for comp in range(comps):
        before = None
        for plane in range(planes):
            at = (comp * planes + plane) * half
            vx = v_ref[0, comp, plane]
            total = (pick_behind(moved_ref[at : at + half, :lanes]) - v_ref[1, comp, plane]) + (
                moved_ref[size + at : size + at + half, :lanes] - v_ref[2, comp, plane]
            )
            total = total - vx
            if before is not None:
                total = total + before
            before = vx
            d_ref[plane, comp] = total
        d_ref[planes, comp] = before


class Split(NamedTuple):
    times: int
    group: int
    wide: int
    near: int

    @property
    def rows(self):
        return self.wide + self.near

    @property
    def offset(self):
        return self.times * self.wide

    @property
    def total(self):
        return self.offset + self.group * self.near

    @property
    def peers(self):
        groups = self.times // self.group
        steps = [(g, m) for g in range(groups) for m in range(self.group)]
        return steps[1:]

    def block(self, step):
        return self.wide if step[0] else self.rows

    def moved(self, device, step, back=False):
        sign = -1 if back else 1
        groups = self.times // self.group
        home = (device // self.group + sign * step[0]) % groups
        return home * self.group + (device % self.group + sign * step[1]) % self.group

    def starts(self, device):
        wide = device * self.wide
        near = self.offset + device % self.group * self.near
        if isinstance(device, int):
            return wide, near
        return pl.multiple_of(wide, 8), pl.multiple_of(near, 8)


def start_kernel(split, links_any, table_any, source_any, out_any, *rest):
    peers = split.peers
    cut_refs, held_refs = rest[: len(peers)], rest[len(peers) : 2 * len(peers)]
    links_ref, table_ref, v_ref, d_ref, rest_ref, stack_ref, moved_ref, high_ref, low_ref, spec_ref, out_ref, sems, cut_sems, out_sems = rest[
        2 * len(peers) :
    ]
    _, _, planes, half, _ = v_ref.shape
    mine = lax.axis_index("tm")
    copies = [
        pltpu.make_async_copy(
            links_any.at[pl.ds(18 * direction, 18)], links_ref.at[pl.ds(18 * direction, 18)], sems.at[direction]
        )
        for direction in range(3)
    ]
    copies.append(pltpu.make_async_copy(table_any, table_ref, sems.at[3]))
    reads, writes = [], []
    for k, (step, cut, held) in enumerate(zip(peers, cut_refs, held_refs)):
        wide, near = split.starts(split.moved(mine, step))
        pieces = [(wide, 0, split.wide)] if step[0] else [(wide, 0, split.wide), (near, split.wide, split.near)]
        for part, (start, to, size) in enumerate(pieces):
            reads.append(
                pltpu.make_async_copy(
                    source_any.at[:, pl.ds(start, size), :], held.at[:, pl.ds(to, size), :], cut_sems.at[part, k]
                )
            )
        writes.append(pltpu.make_async_copy(held, cut, cut_sems.at[2, k]))
    for copy in copies + reads:
        copy.start()
    for direction in range(3):
        copies[direction].wait()

        def step(plane, chunk, direction=direction):
            rows = site_rows(plane, chunk, planes)
            for comp, value in enumerate(project(load_link(links_ref, direction, rows))):
                v_ref[direction, comp, plane, aligned(chunk), :] = value

        chunk_loop(planes, half // 8, step, 4)
    for copy in reads:
        copy.wait()
    for copy in writes:
        copy.start()
    copies[3].wait()
    divergence(v_ref, table_ref, stack_ref, moved_ref, rest_ref, d_ref)
    outs = forward_transform(d_ref, table_ref, high_ref, low_ref, spec_ref, out_ref, out_any, out_sems)
    for copy in writes + outs:
        copy.wait()


def convolve_kernel(planes, in_ref, table_ref, out_ref):
    count = in_ref.shape[0]
    parts, offsets, rows, _ = table_ref.shape
    across = planes * count
    part = lax.axis_index("space") % parts
    step = min(8, rows)

    def run(index, carry):
        c = index // (rows // step)
        chunk = index % (rows // step)

        def at(slot):
            return pl.ds((slot * 2 + c) * rows + chunk * step, step)

        table = [table_ref[part, k, pl.ds(chunk * step, step), :] for k in range(offsets)]
        data = []
        for x in range(across):
            owner, plane = divmod(x, planes)
            value = in_ref[owner, at(plane), :]
            if plane == 0:
                value = value + in_ref[(owner - 1) % count, at(planes), :]
            data.append(value)
        for x in range(across):
            owner, plane = divmod(x, planes)
            total = table[0] * data[x] + table[offsets - 1] * data[(x + across // 2) % across]
            for k in range(1, offsets - 1):
                total = total + table[k] * (data[(x + k) % across] + data[(x - k) % across])
            out_ref[owner, at(plane), :] = total
            if plane == 0:
                out_ref[(owner - 1) % count, at(planes), :] = total
        return carry

    lax.fori_loop(0, 2 * (rows // step), run, 0)


def flatten_shares(x_ref, flat_ref, planes, split):
    half = x_ref.shape[2]
    first = half // 2
    if flat_ref.shape[1] > planes * half:
        flat_ref[...] = jnp.zeros_like(flat_ref)
    for comp in range(8):
        for plane in range(planes):
            value = x_ref[comp, plane]
            flat_ref[comp, pl.ds(plane, first, stride=planes), :] = value[:first]
            flat_ref[comp, pl.ds(split.offset + plane, half - first, stride=planes), :] = value[first:]


def share_copies(flat_ref, share_refs, split, devices, sems):
    copies = []
    for k, (share_ref, device) in enumerate(zip(share_refs, devices)):
        wide, near = split.starts(device)
        copies.append(
            pltpu.make_async_copy(
                flat_ref.at[:, pl.ds(wide, split.wide), :], share_ref.at[:, : split.wide, :], sems.at[0, k]
            )
        )
        copies.append(
            pltpu.make_async_copy(
                flat_ref.at[:, pl.ds(near, split.near), :], share_ref.at[:, split.wide :, :], sems.at[1, k]
            )
        )
    return copies


def middle_kernel(split, in_ref, links_ref, inverse_ref, forward_ref, *rest):
    out_any, x_any = rest[:2]
    share_refs = rest[2 : 2 + split.times]
    x_ref, g_ref, y_ref, v_ref, d_ref, rest_ref, stack_ref, moved_ref, high_ref, low_ref, spec_ref, flat_ref, out_ref, sems, share_sems, out_sems = rest[2 + split.times :]
    _, slots, half, _ = x_ref.shape
    planes = slots - 1
    inverse_transform(in_ref, inverse_ref, high_ref, low_ref, spec_ref, x_ref)
    flatten_shares(x_ref, flat_ref, planes, split)
    mine = lax.axis_index("tm")
    devices = [(mine + shift) % split.times for shift in range(split.times)]
    copies = share_copies(flat_ref, share_refs, split, devices, share_sems)
    copies.append(pltpu.make_async_copy(x_ref, x_any, sems))
    for copy in copies:
        copy.start()

    def raise_step(plane, chunk):
        rows = aligned(chunk)
        store_gauge(g_ref, plane, rows, exponential([x_ref[k, plane, rows, :] for k in range(8)]))

    chunk_loop(slots, half // 8, raise_step, 2)
    lanes = x_ref.shape[3]
    shift_gauge(g_ref, inverse_ref[inverse_ref.shape[0] - 2 * lanes :], stack_ref, moved_ref, y_ref)

    def rotate_step(plane, chunk):
        rows = aligned(chunk)
        gauge = load_gauge(g_ref, plane, rows)
        link_rows = site_rows(plane, chunk, planes)
        for direction in range(3):
            link = load_link(links_ref, direction, link_rows)
            ahead = load_ahead(direction, g_ref, y_ref, moved_ref, plane, chunk)
            turned = [row_times_dagger(row_times(gauge[i], link), ahead) for i in range(3)]
            for comp, value in enumerate(project(turned)):
                v_ref[direction, comp, plane, rows, :] = value

    chunk_loop(planes, half // 8, rotate_step)
    divergence(v_ref, forward_ref, stack_ref, moved_ref, rest_ref, d_ref)
    copies += forward_transform(
        d_ref, forward_ref, high_ref, low_ref, spec_ref, out_ref, out_any, out_sems
    )
    for copy in copies:
        copy.wait()


def last_transform_kernel(split, in_ref, inverse_ref, x_ref, *rest):
    share_refs = rest[: split.times]
    high_ref, low_ref, spec_ref, flat_ref = rest[split.times :]
    inverse_transform(in_ref, inverse_ref, high_ref, low_ref, spec_ref, x_ref)
    flatten_shares(x_ref, flat_ref, x_ref.shape[1] - 1, split)
    for device, share_ref in enumerate(share_refs):
        wide, near = split.starts(device)
        share_ref[:, : split.wide, :] = flat_ref[:, wide : wide + split.wide, :]
        share_ref[:, split.wide :, :] = flat_ref[:, near : near + split.near, :]


def total_of(first, second):
    earlier = exponential(first)
    later = exponential(second)
    return [row_times(later[i], earlier) for i in range(3)]


def finish_kernel(links_any, first_any, table_any, second_ref, out_any, g_ref, y_ref, stack_ref, moved_ref, links_ref, first_ref, shift_ref, out_ref, sems):
    _, slots, half, lanes = first_ref.shape
    planes = slots - 1
    chunks = half // 8
    copies = [
        pltpu.make_async_copy(first_any, first_ref, sems.at[0]),
        pltpu.make_async_copy(links_any, links_ref, sems.at[1]),
        pltpu.make_async_copy(
            table_any.at[pl.ds(table_any.shape[0] - 2 * lanes, 2 * lanes)], shift_ref, sems.at[2]
        ),
    ]
    for copy in copies:
        copy.start()
    copies[0].wait()

    def raise_step(plane, chunk):
        rows = aligned(chunk)
        store_gauge(
            g_ref,
            plane,
            rows,
            total_of(
                [first_ref[k, plane, rows, :] for k in range(8)],
                [second_ref[k, plane, rows, :] for k in range(8)],
            ),
        )

    chunk_loop(slots, half // 8, raise_step)
    copies[2].wait()
    shift_gauge(g_ref, shift_ref[...], stack_ref, moved_ref, y_ref)
    copies[1].wait()

    def piece(chunk):
        rows = pl.ds(pl.multiple_of(chunk * (8 * planes), 8), 8 * planes)
        return pltpu.make_async_copy(out_ref.at[:, rows, :], out_any.at[:, rows, :], sems.at[3 + chunk])

    def rotate_step(chunk, plane):
        rows = aligned(chunk)
        gauge = load_gauge(g_ref, plane, rows)
        link_rows = site_rows(plane, chunk, planes)
        for direction in range(3):
            link = load_link(links_ref, direction, link_rows)
            ahead = load_ahead(direction, g_ref, y_ref, moved_ref, plane, chunk)
            for i in range(3):
                row = row_times_dagger(row_times(gauge[i], link), ahead)
                for j in range(3):
                    out_ref[direction * 18 + 3 * i + j, link_rows, :] = row[j][0]
                    out_ref[direction * 18 + 9 + 3 * i + j, link_rows, :] = row[j][1]

        @pl.when(plane == planes - 1)
        def _():
            piece(chunk).start()

    chunk_loop(chunks, planes, rotate_step)

    for chunk in range(chunks):
        piece(chunk).wait()


def lane_sums(rows):
    ones = jnp.ones((8, rows.shape[1]), BF16)
    total = None
    rest = rows
    for _ in range(3):
        piece = rest.astype(BF16)
        rest = rest - piece.astype(F32)
        part = lax.dot_general(ones, piece, (((1,), (1,)), ((), ())), preferred_element_type=F32)
        total = part if total is None else total + part
    return total


def load_rows(ref, rows):
    return [[(ref[3 * i + j, rows, :], ref[9 + 3 * i + j, rows, :]) for j in range(3)] for i in range(3)]


def sink_kernel(split, sink_ref, src_time_ref, src_site_ref, first_any, second_ref, source_ref, own_early_any, *rest):
    times, group, per = split.times, split.group, split.rows
    rest = list(rest)

    def take(count):
        taken = rest[:count]
        del rest[:count]
        return taken

    early = [own_early_any] + take(times - 1)
    own, late = take(times), take(times - 1)
    partners_any = take(times - 1)
    out_ref, near_ref, wide_ref, x_ref, gauge_ref, sum_ref, before_ref, anchor_ref, sems = rest
    pairs = source_ref.shape[0] // 2
    groups = pairs // 3
    _, slots, half, lanes = second_ref.shape
    planes = slots - 1
    mine = lax.axis_index("tm")
    sink = sink_ref[0]
    column = src_site_ref[0] % (half * lanes)
    plane = src_site_ref[0] // (half * lanes) - lax.axis_index("space") * planes
    present = (src_time_ref[0] == mine) & (plane >= 0) & (plane < planes)
    safe = jnp.clip(plane, 0, planes - 1)
    row = column // lanes
    block = pl.ds(pl.multiple_of(row // 8 * 8, 8), 8)
    before = pltpu.make_async_copy(first_any.at[:, safe, block, :], before_ref, sems.at[0])
    fetches = [pltpu.make_async_copy(early[0], x_ref.at[k], sems.at[1 + k]) for k in range(2)]
    held = [near_ref.at[k] for k in range(group - 1)] + [wide_ref.at[k] for k in range(times - group)]
    partners = [
        pltpu.make_async_copy(partner, to, sems.at[3 + k])
        for k, (partner, to) in enumerate(zip(partners_any, held))
    ]

    def fetch(condition, value, to):
        @pl.when(condition)
        def _():
            pltpu.make_async_copy(value, x_ref.at[to], sems.at[1 + to]).start()

    for shift in range(times):
        fetch((mine - sink) % times == shift, early[shift], 0)
    for at in range(times):
        fetch((mine == sink) & (mine == at), own[at], 1)
    for at in range(times - 1):
        fetch((mine != sink) & (jnp.where(mine > sink, mine - 1, mine) == at), late[at], 1)
    for copy in partners:
        copy.start()
    before.start()
    chunks = per // 8
    for number in range(2):
        fetches[number].wait()
        for chunk in range(chunks):
            rows = slice(chunk * 8, chunk * 8 + 8)
            turn = exponential([x_ref[number, k, rows, :] for k in range(8)])
            if number:
                turn = [row_times(turn[i], load_rows(gauge_ref, rows)) for i in range(3)]
            for i in range(3):
                for j in range(3):
                    gauge_ref[3 * i + j, rows, :] = turn[i][j][0]
                    gauge_ref[9 + 3 * i + j, rows, :] = turn[i][j][1]

    def accumulate(block_ref, offset, first, count, source_device, add):
        base = source_device * pairs

        def run(group_at, carry):
            sums = [None] * 3
            for chunk in range(count // 8):
                rows = slice(first + chunk * 8, first + chunk * 8 + 8)
                own_rows = pl.ds(pl.multiple_of(offset + chunk * 8, 8), 8)
                column = [
                    (
                        block_ref[3 * group_at + c, own_rows, :],
                        block_ref[pairs + 3 * group_at + c, own_rows, :],
                    )
                    for c in range(3)
                ]
                for a in range(3):
                    for c in range(3):
                        part = cmul(
                            (gauge_ref[3 * a + c, rows, :], gauge_ref[9 + 3 * a + c, rows, :]), column[c]
                        )
                        sums[a] = part if sums[a] is None else (sums[a][0] + part[0], sums[a][1] + part[1])
            for a in range(3):
                to = pl.ds(pl.multiple_of((base + 3 * group_at + a) * 8, 8), 8)
                re, im = sums[a]
                if add:
                    re, im = re + sum_ref[0, to, :], im + sum_ref[1, to, :]
                sum_ref[0, to, :] = re
                sum_ref[1, to, :] = im
            return carry

        lax.fori_loop(0, groups, run, 0, unroll=4 if groups % 4 == 0 else 1)

    wide_start, near_start = split.starts(mine)
    accumulate(source_ref, wide_start, 0, split.wide, mine, False)
    accumulate(source_ref, near_start, split.wide, split.near, mine, True)
    for k, step in enumerate(split.peers):
        partners[k].wait()
        owner = split.moved(mine, step, back=True)
        accumulate(held[k], 0, 0, split.block(step), owner, False)
    before.wait()
    total = total_of([before_ref[k] for k in range(8)], [second_ref[k, safe, block, :] for k in range(8)])
    wide = (8, lanes)
    keep = (lane_of(wide) == jnp.where(present, column % lanes, -1)) & (
        lax.broadcasted_iota(jnp.int32, wide, 0) == row % 8
    )
    anchor_ref[...] = jnp.zeros_like(anchor_ref)
    for k in range(18):
        value = total[k % 9 // 3][k % 3][k // 9]
        anchor_ref[k : k + 1, :] = jnp.sum(jnp.where(keep, value, 0.0), axis=0, keepdims=True)
    whole = SC * SC
    width = -(-(whole + 24) // lanes) * lanes
    pieces = []
    for part in range(2):
        total = sum_ref[part, pl.ds(0, whole, stride=8), :]
        for k in range(1, 8):
            total = total + sum_ref[part, pl.ds(k, whole, stride=8), :]
        extra = anchor_ref[...] if part == 0 else jnp.zeros((24, lanes), F32)
        pieces += [total, extra, jnp.zeros((width - whole - 24, lanes), F32)]
    sums = lane_sums(jnp.concatenate(pieces, axis=0))
    block = jnp.concatenate(
        [sums[0:1, k * lanes : (k + 1) * lanes] for k in range(2 * width // lanes)], axis=0
    )

    def spread(index, carry):
        out_ref[index] = block
        return carry

    lax.fori_loop(0, out_ref.shape[0], spread, 0)


def wall_kernel(scale, in_ref, out_ref):
    whole = SC * SC
    total = jnp.sum(in_ref[...], axis=0)
    half = total.shape[0] // 2
    re = jnp.concatenate([total[k : k + 1] for k in range(half)], axis=1)
    im = jnp.concatenate([total[half + k : half + k + 1] for k in range(half)], axis=1)
    width = re.shape[1]
    colour = lane_of((1, width)) // SC % 3
    out_re = jnp.zeros((1, width), F32)
    out_im = jnp.zeros((1, width), F32)
    for b in range(3):
        for c in range(3):
            at = whole + 3 * b + c
            ar = re[:, at : at + 1]
            ai = re[:, at + 9 : at + 10]
            amount = (SC * (b - c)) % width
            wr = pltpu.roll(re, amount, axis=1) if amount else re
            wi = pltpu.roll(im, amount, axis=1) if amount else im
            here = colour == b
            out_re = out_re + jnp.where(here, wr * ar + wi * ai, 0.0)
            out_im = out_im + jnp.where(here, wi * ar - wr * ai, 0.0)
    out_ref[0:1, :] = out_re[:, :whole] * scale
    out_ref[1:2, :] = out_im[:, :whole] * scale


def shape(*dims):
    return jax.ShapeDtypeStruct(dims, F32)


SMEM_SPEC = pl.BlockSpec(memory_space=pltpu.SMEM)
VMEM_SPEC = pl.BlockSpec(memory_space=pltpu.VMEM)
ANY_SPEC = pl.BlockSpec(memory_space=pl.ANY)
HBM_SPEC = pl.BlockSpec(memory_space=pltpu.HBM)


def call(kernel, outs, out_specs, inputs, in_specs, scratch):
    inputs = [
        pltpu.with_memory_space_constraint(x, pltpu.HBM) if spec is HBM_SPEC else x
        for x, spec in zip(inputs, in_specs)
    ]
    outs = [
        pltpu.HBM(out.shape, out.dtype) if spec is HBM_SPEC else out
        for out, spec in zip(outs, out_specs)
    ]
    return pl.pallas_call(
        kernel,
        out_shape=outs,
        in_specs=in_specs,
        out_specs=out_specs,
        scratch_shapes=scratch,
        compiler_params=pltpu.CompilerParams(vmem_limit_bytes=20 * 1024 * 1024),
    )(*inputs)


def body(links, propagator, sink_time, src_time, src_site):
    count = lax.axis_size("space")
    times = lax.axis_size("tm")
    planes = links.shape[5]
    side = math.isqrt(links.shape[6])
    half, lanes = side // 2, 2 * side
    across = planes * count
    slots = planes + 1
    parts = count // 4
    rows = half // parts
    sites = planes * half
    group = 2 if times % 2 == 0 else 1
    spread = sites // 2
    split = Split(times, group, 8 * -(-spread // (8 * times)), 8 * -(-(sites - spread) // (8 * group)))
    pairs = propagator.shape[1]

    forward = jnp.asarray(transform_table(side, False))
    inverse = jnp.asarray(transform_table(side, True))
    table = jnp.asarray(filter_table(side, across, parts))

    def interleave(array, lead):
        return array.reshape(lead, planes, half, lanes).transpose(0, 2, 1, 3).reshape(lead, sites, lanes)

    lattice = interleave(links, 54)

    def forwarded(value, shift):
        return lax.ppermute(value, "tm", [(i, (i + shift) % times) for i in range(times)])

    spectrum_shape = shape(count, slots * 2 * rows, lanes)
    transform_scratch = [
        VMEM((4 * slots * half, 2 * lanes), BF16),
        VMEM((4 * slots * half, 2 * lanes), BF16),
        VMEM((4 * slots * half, 2 * lanes), F32),
    ]
    divergence_scratch = [
        VMEM((3, 8, planes, half, lanes), F32),
        VMEM((slots, 8, half, lanes), F32),
        VMEM((16 * planes * half, lanes), BF16),
    ]
    gauge_scratch = [
        VMEM((18, slots, half, lanes), F32),
        VMEM((18, planes, half, lanes), F32),
    ]
    shift_scratch = [
        VMEM((18 * planes * half, 2 * lanes), BF16),
        VMEM((18 * planes * half, 2 * lanes), F32),
    ]
    out_scratch = [VMEM((slots, count, 2 * rows, lanes), F32)]
    flat_scratch = [VMEM((8, split.total, lanes), F32)]
    algebra_shape = shape(8, slots, half, lanes)
    share_shapes = [shape(8, split.rows, lanes)] * times

    def turn(spectrum):
        return lax.all_to_all(spectrum, "space", 0, 0, tiled=True)

    def convolve(spectrum):
        (out,) = call(
            functools.partial(convolve_kernel, planes),
            [spectrum_shape],
            [VMEM_SPEC],
            [spectrum, table],
            [VMEM_SPEC] * 2,
            [],
        )
        return out

    source = interleave(propagator, 2 * pairs)
    if split.total > sites:
        fill = jnp.zeros((2 * pairs, split.offset - spread, lanes), F32)
        source = jnp.concatenate([source[:, :spread], fill, source[:, spread:]], axis=1)
    scalars = [sink_time % times, src_time % times, jnp.maximum(src_site, 0)]
    cut_shapes = [shape(2 * pairs, split.block(step), lanes) for step in split.peers]
    spectrum, *cuts = call(
        functools.partial(start_kernel, split),
        [spectrum_shape] + cut_shapes,
        [HBM_SPEC] * times,
        [lattice, forward, source],
        [HBM_SPEC] * 3,
        [VMEM(cut.shape, F32) for cut in cut_shapes]
        + [VMEM(lattice.shape, F32), VMEM(forward.shape, BF16)]
        + divergence_scratch
        + shift_scratch
        + transform_scratch
        + out_scratch
        + [
            pltpu.SemaphoreType.DMA((4,)),
            pltpu.SemaphoreType.DMA((3, times - 1)),
            pltpu.SemaphoreType.DMA((slots,)),
        ],
    )
    held_scratch = [
        VMEM((max(1, group - 1), 2 * pairs, split.rows, lanes), F32),
        VMEM((max(1, times - group), 2 * pairs, split.wide, lanes), F32),
    ]
    scalars = [sink_time % times, src_time % times, jnp.maximum(src_site, 0)]
    sources = [
        lax.ppermute(cut, "tm", [(i, split.moved(i, step)) for i in range(times)])
        for step, cut in zip(split.peers, cuts)
    ]

    spectrum = turn(spectrum)
    spectrum = convolve(spectrum)
    spectrum = turn(spectrum)
    spectrum, first, *early = call(
        functools.partial(middle_kernel, split),
        [spectrum_shape, algebra_shape] + share_shapes,
        [HBM_SPEC] * (2 + times),
        [spectrum, lattice, inverse, forward],
        [VMEM_SPEC] * 4,
        [VMEM(algebra_shape.shape, F32)]
        + gauge_scratch
        + divergence_scratch
        + shift_scratch
        + transform_scratch
        + flat_scratch
        + out_scratch
        + [
            pltpu.SemaphoreType.DMA,
            pltpu.SemaphoreType.DMA((2, times)),
            pltpu.SemaphoreType.DMA((slots,)),
        ],
    )
    first_shares = [forwarded(early[shift], shift) for shift in range(1, times)]
    spectrum = turn(spectrum)
    spectrum = convolve(spectrum)
    spectrum = turn(spectrum)
    second, *shares = call(
        functools.partial(last_transform_kernel, split),
        [algebra_shape] + share_shapes,
        [VMEM_SPEC] * (1 + times),
        [spectrum, inverse],
        [VMEM_SPEC] * 2,
        transform_scratch + flat_scratch,
    )

    def sent_from(source_index):
        def send(*blocks):
            return tuple(
                lax.ppermute(blocks[to], "tm", [(source_index, to)])
                for to in range(times)
                if to != source_index
            )

        return send

    second_shares = lax.switch(sink_time[0] % times, [sent_from(k) for k in range(times)], *shares)
    (fixed,) = call(
        finish_kernel,
        [shape(54, sites, lanes)],
        [HBM_SPEC],
        [lattice, first, inverse, second],
        [HBM_SPEC] * 3 + [VMEM_SPEC],
        gauge_scratch
        + shift_scratch
        + [
            VMEM(lattice.shape, F32),
            VMEM(algebra_shape.shape, F32),
            VMEM((2 * lanes, 2 * lanes), BF16),
            VMEM(lattice.shape, F32),
            pltpu.SemaphoreType.DMA((3 + half // 8,)),
        ],
    )
    width = -(-(SC * SC + 24) // lanes)
    devices = count * times
    (payload,) = call(
        functools.partial(sink_kernel, split),
        [shape(devices, 2 * width, lanes)],
        [VMEM_SPEC],
        scalars + [first, second, source, early[0]] + first_shares + shares + list(second_shares) + sources,
        [SMEM_SPEC] * 3
        + [HBM_SPEC]
        + [VMEM_SPEC] * 2
        + [HBM_SPEC]
        + [ANY_SPEC] * (2 * times - 1)
        + [HBM_SPEC] * (2 * times - 2),
        held_scratch
        + [
            VMEM((2, 8, split.rows, lanes), F32),
            VMEM((18, split.rows, lanes), F32),
            VMEM((2, SC * SC * 8, lanes), F32),
            VMEM((8, 8, lanes), F32),
            VMEM((24, lanes), F32),
            pltpu.SemaphoreType.DMA((2 + times,)),
        ],
    )
    gathered = lax.all_to_all(payload, ("space", "tm"), 0, 0, tiled=True)
    scale = float(across * side * side) ** (-0.5)
    (wall,) = call(functools.partial(wall_kernel, scale), [shape(2, SC * SC)], [VMEM_SPEC], [gathered], [VMEM_SPEC], [])
    fixed = fixed.reshape(54, half, planes, lanes).transpose(0, 2, 1, 3).reshape(links.shape)
    return fixed, wall


def solution(mesh):
    placed = (
        P("tm", None, None, None, None, "space", None),
        P(None, "tm", "space", None),
        P(),
        P(),
        P(),
    )
    return jax.shard_map(
        body,
        mesh=mesh,
        in_specs=placed,
        out_specs=(P("tm", None, None, None, None, "space", None), P()),
        check_vma=False,
    )
```
